32 devices in a mesh: dp: 1 (over z), ep: 32 (over y, x, core).
Axes of the slice: x: 4, y: 4, z: 1, core: 2. Of those that a mesh axis runs over, the one named last changes fastest.
The devices are a block of a 4x4x8 slice.
Arguments:
- x_tokens: bfloat16 [8192, 512], P(('dp', 'ep'))
- expert_ids: int32 [8192, 8], P(('dp', 'ep'))
- grad_y: bfloat16 [8192, 512], P(('dp', 'ep'))
- w_q: bfloat16 [512, 512], P('ep')
- w_k: bfloat16 [512, 512], P('ep')
- w_v: bfloat16 [512, 512], P('ep')
- w_o: bfloat16 [512, 512], P('ep')
- w_router: float32 [512, 64], replicated
- w_gate: bfloat16 [64, 512, 256], P('ep')
- w_up: bfloat16 [64, 512, 256], P('ep')
- w_down: bfloat16 [64, 256, 512], P('ep')
Outputs:
- output 1: bfloat16 [8192, 512], P(('dp', 'ep'))
- output 2: bfloat16 [8192, 512], P(('dp', 'ep'))
- output 3: bfloat16 [64, 512, 256], P(('dp', 'ep'))
- output 4: bfloat16 [64, 512, 256], P(('dp', 'ep'))
- output 5: bfloat16 [64, 256, 512], P(('dp', 'ep'))
All inputs are finite; a program needn't handle non-finite values.
Results may differ from the reference program's by a relative error of at most 0.0199931.
Values are sent between devices in bfloat16 or wider.
A program may use at most 768 MiB of HBM per device.

```python
import jax
import jax.numpy as jnp
from jax import lax

GROUP = 32
TOKENS = 256
SEQ = 256
D = 512
FF = 256
EXPERTS = 64
TOP = 8
HEADS = 8
HEAD = 64
NORM_EPS = 1e-6
AVG_LOAD = TOKENS * TOP // EXPERTS
CAP = AVG_LOAD + AVG_LOAD // 2
ROWS = GROUP * TOKENS
EXPERT_ROWS = GROUP * CAP


def draw_routing(rng_key):
    perm_key, shift_key, token_key = jax.random.split(rng_key, 3)
    half_load = AVG_LOAD // 2
    load_shift = jax.random.randint(shift_key, (EXPERTS // 2,), 0, half_load + 1)
    load_shift = load_shift.at[0].set(half_load)
    expert_loads = jnp.stack([AVG_LOAD + load_shift, AVG_LOAD - load_shift], axis=1).reshape(-1)
    bounds = jnp.cumsum(expert_loads)
    positions = jnp.arange(TOKENS)[:, None] + TOKENS * jnp.arange(TOP)[None, :]
    sorted_ids = jnp.searchsorted(bounds, positions, side='right')
    expert_perm = jax.random.permutation(perm_key, EXPERTS)
    token_perm = jax.random.permutation(token_key, TOKENS)
    return expert_perm[sorted_ids][token_perm].astype(jnp.int32)


def draw_normal(rng_key, arr_shape, std_scale):
    return (jax.random.normal(rng_key, arr_shape, jnp.float32) * std_scale).astype(jnp.bfloat16)


def setup_inputs(seed: int = 0, part: int = 0) -> dict:
    base_key = jax.random.key(seed)
    part_keys = jax.random.split(jax.random.fold_in(base_key, part), 3)
    w_keys = jax.random.split(base_key, 8)
    attn_width = HEADS * HEAD
    route_keys = jax.random.split(part_keys[2], GROUP)
    return {
        'x_tokens': draw_normal(part_keys[0], (ROWS, D), 1.0),
        'expert_ids': jax.vmap(draw_routing)(route_keys).reshape(ROWS, TOP),
        'grad_y': draw_normal(part_keys[1], (ROWS, D), 1.0),
        'w_q': draw_normal(w_keys[0], (D, attn_width), D ** -0.5),
        'w_k': draw_normal(w_keys[1], (D, attn_width), D ** -0.5),
        'w_v': draw_normal(w_keys[2], (D, attn_width), D ** -0.5),
        'w_o': draw_normal(w_keys[3], (attn_width, D), 3.0 * attn_width ** -0.5),
        'w_router': jax.random.normal(w_keys[4], (D, EXPERTS), jnp.float32) * D ** -0.5,
        'w_gate': draw_normal(w_keys[5], (EXPERTS, D, FF), D ** -0.5),
        'w_up': draw_normal(w_keys[6], (EXPERTS, D, FF), D ** -0.5),
        'w_down': draw_normal(w_keys[7], (EXPERTS, FF, D), 3.0 * FF ** -0.5),
    }


def rms_norm(values):
    wide_vals = values.astype(jnp.float32)
    return wide_vals * lax.rsqrt(jnp.mean(wide_vals * wide_vals, axis=-1, keepdims=True) + NORM_EPS)


def attend_device(qkv_dev):
    q_dev, k_dev, v_dev = qkv_dev
    scores = jnp.einsum('bqhd,bkhd->bhqk', q_dev.astype(jnp.float32), k_dev.astype(jnp.float32)) * HEAD ** -0.5
    causal = jnp.arange(SEQ)[:, None] >= jnp.arange(SEQ)[None, :]
    attn_probs = jax.nn.softmax(jnp.where(causal, scores, -1e30), axis=-1).astype(jnp.bfloat16)
    attn_out = jnp.einsum('bhqk,bkhd->bqhd', attn_probs.astype(jnp.float32), v_dev.astype(jnp.float32))
    return attn_out.astype(jnp.bfloat16)


def layer_forward(x_tokens, expert_ids, w_q, w_k, w_v, w_o, w_router, w_gate, w_up, w_down):
    x_norm = rms_norm(x_tokens).astype(jnp.bfloat16)

    def project(weight):
        heads_flat = jnp.dot(x_norm, weight, preferred_element_type=jnp.float32).astype(jnp.bfloat16)
        return heads_flat.reshape(GROUP, TOKENS // SEQ, SEQ, HEADS, HEAD)

    heads_out = lax.map(jax.checkpoint(attend_device), (project(w_q), project(w_k), project(w_v)))
    attn_proj = jnp.dot(heads_out.reshape(ROWS, HEADS * HEAD), w_o, preferred_element_type=jnp.float32)
    hidden = (x_tokens.astype(jnp.float32) + attn_proj).astype(jnp.bfloat16)
    h_norm = rms_norm(hidden)
    u_wide = h_norm.astype(jnp.bfloat16).astype(jnp.float32)
    logits = jnp.dot(h_norm, w_router, preferred_element_type=jnp.float32)
    gate_probs = jax.nn.softmax(jnp.take_along_axis(logits, expert_ids, axis=1), axis=-1)
    flat_e = expert_ids.reshape(-1)
    sort_order = jnp.argsort(flat_e, stable=True)
    counts = jnp.bincount(flat_e, length=EXPERTS)
    starts = jnp.cumsum(counts) - counts
    slot_rank = jnp.arange(EXPERT_ROWS)
    row_valid = slot_rank[None, :] < counts[:, None]
    row_token = sort_order[jnp.minimum(starts[:, None] + slot_rank[None, :], ROWS * TOP - 1)] // TOP

    def expert_rows(operands):
        tok_ids, keep_row, gate_w, up_w, down_w = operands
        rows_in = jnp.where(keep_row[:, None], u_wide[tok_ids], 0.0).astype(jnp.bfloat16)
        a_gate = jnp.dot(rows_in, gate_w, preferred_element_type=jnp.float32)
        a_up = jnp.dot(rows_in, up_w, preferred_element_type=jnp.float32)
        mid_act = (jax.nn.silu(a_gate) * a_up).astype(jnp.bfloat16)
        return jnp.dot(mid_act, down_w, preferred_element_type=jnp.float32).astype(jnp.bfloat16)

    expert_out = lax.map(jax.checkpoint(expert_rows), (row_token, row_valid, w_gate, w_up, w_down))
    inverse = jnp.argsort(sort_order)
    slot_of = flat_e * EXPERT_ROWS + inverse - starts[flat_e]
    picked = expert_out.reshape(EXPERTS * EXPERT_ROWS, D)[slot_of].reshape(ROWS, TOP, D)
    mixed = jnp.sum(gate_probs[:, :, None] * picked.astype(jnp.float32), axis=1)
    return (hidden.astype(jnp.float32) + mixed).astype(jnp.bfloat16)


def reference(x_tokens, expert_ids, grad_y, w_q, w_k, w_v, w_o, w_router, w_gate, w_up, w_down):
    def layer_fn(x_in, gate_w, up_w, down_w):
        return layer_forward(x_in, expert_ids, w_q, w_k, w_v, w_o, w_router, gate_w, up_w, down_w)

    y_tokens, pullback = jax.vjp(layer_fn, x_tokens, w_gate, w_up, w_down)
    grad_x, grad_gate, grad_up, grad_down = pullback(grad_y)
    return (y_tokens, grad_x, grad_gate, grad_up, grad_down)
```

```python
import functools
import math

import jax
import jax.numpy as jnp
from jax import lax
from jax.experimental import pallas as pl
from jax.experimental.pallas import tpu as pltpu
from jax.sharding import PartitionSpec as P

NORM_EPS = 1e-6
SEQ_LEN = 256
HEAD_DIM = 64
AXIS = 'ep'
F32 = jnp.float32
BF16 = jnp.bfloat16


class Place:
    def __init__(self, group):
        self.group = group
        self.side = math.isqrt(group // 2)
        self.me = lax.axis_index(AXIS)
        self.core = lax.rem(self.me, 2)
        self.x = lax.rem(self.me // 2, self.side)
        self.y = self.me // (2 * self.side)

    def wrap(self, v):
        return lax.rem(v + self.side, self.side)

    def at(self, dy, dx, dc=0):
        return (self.wrap(self.y + dy) * self.side + self.wrap(self.x + dx)) * 2 + lax.rem(self.core + dc, 2)


def remote(src, dst, k, target, ssem, rsem):
    return pltpu.make_async_remote_copy(src_ref=src, dst_ref=dst, send_sem=ssem.at[k], recv_sem=rsem.at[k],
                                        device_id={AXIS: target}, device_id_type=pl.DeviceIdType.MESH)


def barrier(peers):
    sem = pltpu.get_barrier_semaphore()
    for peer in peers:
        pl.semaphore_signal(sem, inc=1, device_id={AXIS: peer}, device_id_type=pl.DeviceIdType.MESH)
    pl.semaphore_wait(sem, len(peers))


def torus_peers(pl_):
    return [pl_.at(0, 1), pl_.at(0, -1), pl_.at(1, 0), pl_.at(-1, 0), pl_.at(0, 2), pl_.at(2, 0), pl_.at(0, 0, 1)]


class Sems:
    def __init__(self, ssem, rsem):
        self.ssem, self.rsem, self.used, self.sent = ssem, rsem, 0, []

    def send(self, src, dst, target):
        k = self.used
        self.used += 1
        copy = remote(src, dst, k, target, self.ssem, self.rsem)
        copy.start()
        self.sent.append(copy)
        return k

    def wait(self, k, dst, anyone):
        remote(dst, dst, k, anyone, self.ssem, self.rsem).wait_recv()


def gather_steps(place, sems, own, region, relay):
    partner = place.at(0, 0, 1)

    def dev(h, a, b, dc=0):
        return place.at(b, a, dc) if h == 0 else place.at(a, b, dc)

    def src(h, a, b, lo, num):
        return own(lo, num) if (a, b) == (0, 0) else region(dev(h, a, b), lo, num)

    def send(h, a, b, lo, num, ta, tb):
        return sems.send(src(h, a, b, lo, num), region(dev(h, a, b), lo, num), dev(h, ta, tb))

    def wait(k, h, a, b, lo, num):
        sems.wait(k, region(dev(h, a, b), lo, num), partner)

    passed = []

    def pass_on(h, a, b, lo, num):
        k = sems.send(src(h, a, b, lo, num), region(dev(h, a, b), lo, num), partner)
        passed.append((k, h, a, b, lo, num))

    halves = ((0, 0, 2), (1, 2, 2))
    first, second, rel1, rel2 = {}, {}, {}, {}
    shifts = (1, -1) if relay else (1, -1, 2)

    def go_second(h, a, lo, num):
        for s in shifts:
            second[h, a, s] = send(h, a, 0, lo, num, a, s) if False else sems.send(
                src(h, a, 0, lo, num), region(dev(h, a, 0), lo, num), dev(h, 0, s))

    for h, lo, num in halves:
        for s in shifts:
            first[h, s] = sems.send(own(lo, num), region(place.me, lo, num), dev(h, s, 0))
    for h, lo, num in halves:
        go_second(h, 0, lo, num)
    for h, lo, num in halves:
        pass_on(h, 0, 0, lo, num)
    yield
    if not relay:
        for s in shifts:
            for h, lo, num in halves:
                wait(first[h, s], h, -s, 0, lo, num)
                go_second(h, -s, lo, num)
                pass_on(h, -s, 0, lo, num)
            yield
        for a in (0, -1, 1, -2):
            for s in shifts:
                for h, lo, num in halves:
                    wait(second[h, a, s], h, a, -s, lo, num)
                    pass_on(h, a, -s, lo, num)
            yield
    else:
        for s in shifts:
            for h, lo, num in halves:
                wait(first[h, s], h, -s, 0, lo, num)
                part = lo + (s == -1)
                rel1[h, s] = sems.send(src(h, -s, 0, part, 1), region(dev(h, -s, 0), part, 1), dev(h, s, 0))
                go_second(h, -s, lo, num)
                pass_on(h, -s, 0, lo, num)
            yield

        def relay2(h, lo, num, a, s):
            wait(second[h, a, s], h, a, -s, lo, num)
            part = lo + (s == -1)
            rel2[h, a, s] = sems.send(src(h, a, -s, part, 1), region(dev(h, a, -s), part, 1), dev(h, 0, s))
            pass_on(h, a, -s, lo, num)

        for h, lo, num in halves:
            for s in shifts:
                relay2(h, lo, num, 0, s)
        yield
        for h, lo, num in halves:
            for s in shifts:
                wait(rel1[h, s], h, -2 * s, 0, lo + (s == -1), 1)
            go_second(h, 2, lo, num)
            pass_on(h, 2, 0, lo, num)
        yield
        for a in (-1, 1, 2):
            for s in shifts:
                for h, lo, num in halves:
                    relay2(h, lo, num, a, s)
            yield
        for a in (0, -1, 1, 2):
            for h, lo, num in halves:
                for s in shifts:
                    wait(rel2[h, a, s], h, a, -2 * s, lo + (s == -1), 1)
                pass_on(h, a, 2, lo, num)
            yield
    for k, h, a, b, lo, num in passed:
        yy = dev(h, a, b, 1)
        sems.wait(k, region(yy, lo, num), partner)
    yield


def run_all(gens):
    gens = list(gens)
    while gens:
        alive = []
        for g in gens:
            try:
                next(g)
                alive.append(g)
            except StopIteration:
                pass
        gens = alive


def rows_region(ref, quarter):
    return lambda d, lo, num: ref.at[d, pl.ds(lo * quarter, num * quarter)]


def rows_own(ref, quarter):
    return lambda lo, num: ref.at[pl.ds(lo * quarter, num * quarter)]


def weights_kernel(group, w_ref, dy_ref, full_ref, dy_all_ref, ssem, rsem):
    place = Place(group)
    barrier(torus_peers(place))
    sems = Sems(ssem, rsem)
    depth = w_ref.shape[1]
    mine = pl.ds(pl.multiple_of(place.me * depth, depth), depth)
    full_ref[:, mine, :] = w_ref[...]
    dy_all_ref[place.me] = dy_ref[...]
    w_steps = gather_steps(
        place, sems, lambda lo, num: w_ref.at[pl.ds(lo, num)],
        lambda d, lo, num: full_ref.at[pl.ds(lo, num), pl.ds(pl.multiple_of(d * depth, depth), depth)], False)
    quarter = dy_ref.shape[0] // 4
    dy_steps = gather_steps(place, sems, rows_own(dy_ref, quarter), rows_region(dy_all_ref, quarter), True)
    run_all([w_steps, dy_steps])
    for copy in sems.sent:
        copy.wait_send()


def tokens_kernel(group, u_ref, meta_ref, u_all_ref, meta_all_ref, ssem, rsem):
    place = Place(group)
    barrier(torus_peers(place))
    sems = Sems(ssem, rsem)
    u_all_ref[place.me] = u_ref[...]
    meta_all_ref[place.me] = meta_ref[...]
    quarter = u_ref.shape[0] // 4
    m_steps = gather_steps(place, sems, lambda lo, num: meta_ref.at[pl.ds(lo, num)],
                           lambda d, lo, num: meta_all_ref.at[d, pl.ds(lo, num)], False)
    u_steps = gather_steps(place, sems, rows_own(u_ref, quarter), rows_region(u_all_ref, quarter), True)
    run_all([m_steps, u_steps])
    for copy in sems.sent:
        copy.wait_send()


def return_kernel(group, z_ref, du_ref, z_back_ref, du_back_ref, ssem, rsem):
    place = Place(group)
    side = place.side
    offs = [(dy, dx, dc) for dy in range(side) for dx in range(side) for dc in range(2)][1:]
    barrier([place.at(*o) for o in offs])
    sems = Sems(ssem, rsem)
    waits = []
    for out, back in ((z_ref, z_back_ref), (du_ref, du_back_ref)):
        back[place.me] = out[place.me]
        for i in range(len(offs)):
            dy, dx, dc = offs[(i * 12) % len(offs)]
            target = place.at(dy, dx, dc)
            k = sems.send(out.at[target], back.at[place.me], target)
            waits.append((k, back, place.at(-dy, -dx, dc)))
    for k, back, origin in waits:
        sems.wait(k, back.at[origin], origin)
    for copy in sems.sent:
        copy.wait_send()


def comm_call(kernel, group, outs, sems, cid, name):
    vmem = pl.BlockSpec(memory_space=pltpu.VMEM)
    return lambda *args: pl.pallas_call(
        functools.partial(kernel, group), out_shape=outs,
        in_specs=[vmem] * len(args), out_specs=[vmem] * len(outs),
        scratch_shapes=[pltpu.SemaphoreType.DMA((sems,)), pltpu.SemaphoreType.DMA((sems,))],
        compiler_params=pltpu.CompilerParams(collective_id=cid, has_side_effects=True, vmem_limit_bytes=60 << 20),
        name=name)(*args)


def rms_norm(values):
    wide_vals = values.astype(F32)
    return wide_vals * lax.rsqrt(jnp.mean(wide_vals * wide_vals, axis=-1, keepdims=True) + NORM_EPS)


def local_attention(q_heads, k_heads, v_heads):
    scores = jnp.einsum('bqhd,bkhd->bhqk', q_heads, k_heads, preferred_element_type=F32) * HEAD_DIM ** -0.5
    causal = jnp.arange(SEQ_LEN)[:, None] >= jnp.arange(SEQ_LEN)[None, :]
    attn_probs = jax.nn.softmax(jnp.where(causal, scores, -1e30), axis=-1).astype(BF16)
    return jnp.einsum('bhqk,bkhd->bqhd', attn_probs, v_heads, preferred_element_type=F32).astype(BF16)


def mm(a, b, dims):
    return lax.dot_general(a, b, dims, preferred_element_type=F32)


def solution(mesh):
    group = mesh.shape[AXIS]
    tok_spec = P(('dp', 'ep'), None)
    fsdp_spec = P('ep', None)
    expert_spec = P('ep', None, None)
    grad_spec = P(('dp', 'ep'), None, None)

    def device_step(x_tokens, expert_ids, grad_y, w_q, w_k, w_v, w_o, w_router, w_gate, w_up, w_down):
        toks, d_model = x_tokens.shape
        choices = expert_ids.shape[1]
        experts = w_router.shape[1]
        local = w_gate.shape[0]
        avg_load = toks * choices // experts
        cap = avg_load + avg_load // 2
        n_seq = toks // SEQ_LEN
        shape = jax.ShapeDtypeStruct
        depth = w_q.shape[0]

        w_own = jnp.stack([w_q, w_k, w_v, w_o])
        w_full, dy_all = comm_call(
            weights_kernel, group,
            [shape((4, group * depth, d_model), BF16), shape((group, toks, d_model), BF16)], 176, 1, 'gather_w')(w_own, grad_y)
        full_q, full_k, full_v, full_o = w_full[0], w_full[1], w_full[2], w_full[3]

        x_wide = x_tokens.astype(F32)
        x_norm, x_pullback = jax.vjp(rms_norm, x_wide)
        x_norm_b = x_norm.astype(BF16)

        def project(weight):
            heads_flat = jnp.dot(x_norm_b, weight, preferred_element_type=F32).astype(BF16)
            return heads_flat.reshape(n_seq, SEQ_LEN, -1, HEAD_DIM)

        attn_heads, attn_pullback = jax.vjp(local_attention, project(full_q), project(full_k), project(full_v))
        attn_proj = jnp.dot(attn_heads.reshape(toks, -1), full_o, preferred_element_type=F32)
        hidden = (x_wide + attn_proj).astype(BF16)
        h_norm, norm_pullback = jax.vjp(rms_norm, hidden.astype(F32))
        u_norm = h_norm.astype(BF16)
        logits = jnp.dot(h_norm, w_router, precision=lax.Precision.HIGHEST)

        lane_e = jnp.arange(experts)
        hit = expert_ids[:, :, None] == lane_e
        chosen = jnp.any(hit, axis=1)
        earlier = (jnp.arange(toks)[:, None] > jnp.arange(toks)[None, :]).astype(BF16)
        rank = jnp.dot(earlier, chosen.astype(BF16), preferred_element_type=F32)
        top = jnp.max(jnp.where(chosen, logits, -jnp.inf), axis=-1, keepdims=True)
        expd = jnp.where(chosen, jnp.exp(logits - top), 0.0)
        gates = expd / jnp.sum(expd, axis=-1, keepdims=True)
        gate_j = jnp.sum(jnp.where(hit, gates[:, None, :], 0.0), axis=-1)

        meta = jnp.concatenate([expert_ids.astype(F32).T, gate_j.T], axis=0).reshape(4, 4, toks)
        u_all, meta_all = comm_call(
            tokens_kernel, group,
            [shape((group, toks, d_model), BF16), shape((group, 4, 4, toks), F32)], 176, 2, 'gather_u')(u_norm, meta)
        meta_all = meta_all.reshape(group, 2, choices, toks)

        mine = lax.axis_index(AXIS) * local + jnp.arange(local)
        hits = meta_all[:, 0][:, None] == mine.astype(F32)[None, :, None, None]
        sel = jnp.any(hits, axis=2)
        gate_here = jnp.sum(jnp.where(hits, meta_all[:, 1][:, None], 0.0), axis=2)
        later = (jnp.arange(toks)[:, None] < jnp.arange(toks)[None, :]).astype(BF16)
        rank_here = mm(sel.astype(BF16), later, (((2,), (0,)), ((), ())))
        pick = sel[:, :, None, :] & (rank_here[:, :, None, :] == jnp.arange(cap, dtype=F32)[None, None, :, None])
        slot_gate = jnp.sum(jnp.where(pick, gate_here[:, :, None, :], 0.0), axis=-1).reshape(group, local * cap)
        pick_b = pick.astype(BF16).reshape(group, local * cap, toks)
        batched = (((2,), (1,)), ((0,), (0,)))
        recv_u = mm(pick_b, u_all, batched).astype(BF16).reshape(group, local, cap, d_model)
        raw_dy = mm(pick_b, dy_all, batched)
        recv_dy = (slot_gate[:, :, None] * raw_dy).astype(BF16).reshape(group, local, cap, d_model)

        a_gate = jnp.einsum('secd,edf->secf', recv_u, w_gate, preferred_element_type=F32)
        a_up = jnp.einsum('secd,edf->secf', recv_u, w_up, preferred_element_type=F32)
        mid_act = (jax.nn.silu(a_gate) * a_up).astype(BF16)
        expert_y = jnp.einsum('secf,efd->secd', mid_act, w_down, preferred_element_type=F32).astype(BF16)
        grad_down = jnp.einsum('secf,secd->efd', mid_act, recv_dy, preferred_element_type=F32).astype(BF16)
        grad_mid = jnp.einsum('secd,efd->secf', recv_dy, w_down, preferred_element_type=F32)
        sig_gate = jax.nn.sigmoid(a_gate)
        grad_agate = (grad_mid * a_up * sig_gate * (1.0 + a_gate * (1.0 - sig_gate))).astype(BF16)
        grad_aup = (grad_mid * a_gate * sig_gate).astype(BF16)
        grad_gate = jnp.einsum('secd,secf->edf', recv_u, grad_agate, preferred_element_type=F32).astype(BF16)
        grad_up = jnp.einsum('secd,secf->edf', recv_u, grad_aup, preferred_element_type=F32).astype(BF16)
        grad_recv = (jnp.einsum('secf,edf->secd', grad_agate, w_gate, preferred_element_type=F32)
                     + jnp.einsum('secf,edf->secd', grad_aup, w_up, preferred_element_type=F32)).astype(BF16)

        rows = shape((group, local * cap, d_model), BF16)
        back_z, back_u = comm_call(return_kernel, group, [rows, rows], 2 * group, 3, 'return_rows')(
            expert_y.reshape(rows.shape), grad_recv.reshape(rows.shape))
        back_z = back_z.reshape(-1, d_model)
        back_u = back_u.reshape(-1, d_model)

        slots = experts * cap
        column = jnp.arange(slots)
        spread = (lane_e[:, None] == (column // cap)[None, :]).astype(BF16)
        rank_x = jnp.dot(jnp.where(chosen, rank, -1.0).astype(BF16), spread, preferred_element_type=F32)
        place = rank_x == (column % cap).astype(F32)[None, :]
        gate_x = jnp.dot(gates, spread.astype(F32), precision=lax.Precision.HIGHEST)
        mixed = jnp.dot(jnp.where(place, gate_x, 0.0), back_z.astype(F32), precision=lax.Precision.HIGHEST)
        y_tokens = (hidden.astype(F32) + mixed).astype(BF16)

        dy_wide = grad_y.astype(F32)
        score = mm(grad_y, back_z, (((1,), (1,)), ((), ())))
        grad_gates = jnp.dot(jnp.where(place, score, 0.0), spread.astype(F32).T, precision=lax.Precision.HIGHEST)
        grad_logits = gates * (grad_gates - jnp.sum(gates * grad_gates, axis=-1, keepdims=True))
        grad_hnorm = jnp.dot(grad_logits, w_router.T, precision=lax.Precision.HIGHEST)
        grad_u = jnp.dot(place.astype(BF16), back_u, preferred_element_type=F32)
        grad_hid_b = (dy_wide + norm_pullback(grad_u + grad_hnorm)[0]).astype(BF16)
        grad_attn = jnp.einsum('td,hd->th', grad_hid_b, full_o, preferred_element_type=F32).astype(BF16)
        grad_q, grad_k, grad_v = attn_pullback(grad_attn.reshape(n_seq, SEQ_LEN, -1, HEAD_DIM))
        grad_xnorm = (jnp.einsum('th,dh->td', grad_q.reshape(toks, -1), full_q, preferred_element_type=F32)
                      + jnp.einsum('th,dh->td', grad_k.reshape(toks, -1), full_k, preferred_element_type=F32)
                      + jnp.einsum('th,dh->td', grad_v.reshape(toks, -1), full_v, preferred_element_type=F32))
        grad_x = (grad_hid_b.astype(F32) + x_pullback(grad_xnorm)[0]).astype(BF16)
        return y_tokens, grad_x, grad_gate, grad_up, grad_down

    return jax.shard_map(
        device_step, mesh=mesh,
        in_specs=(tok_spec, tok_spec, tok_spec, fsdp_spec, fsdp_spec, fsdp_spec, fsdp_spec,
                  P(None, None), expert_spec, expert_spec, expert_spec),
        out_specs=(tok_spec, tok_spec, grad_spec, grad_spec, grad_spec),
        check_vma=False)
```

```python
import functools
import math

import jax
import jax.numpy as jnp
from jax import lax
from jax.experimental import pallas as pl
from jax.experimental.pallas import tpu as pltpu
from jax.sharding import PartitionSpec as P

NORM_EPS = 1e-6
SEQ_LEN = 256
HEAD_DIM = 64
AXIS = 'ep'
F32 = jnp.float32
BF16 = jnp.bfloat16


class Place:
    def __init__(self, group):
        self.group = group
        self.side = math.isqrt(group // 2)
        self.me = lax.axis_index(AXIS)
        self.core = lax.rem(self.me, 2)
        self.x = lax.rem(self.me // 2, self.side)
        self.y = self.me // (2 * self.side)

    def wrap(self, v):
        return lax.rem(v + self.side, self.side)

    def at(self, dy, dx, dc=0):
        return (self.wrap(self.y + dy) * self.side + self.wrap(self.x + dx)) * 2 + lax.rem(self.core + dc, 2)


def remote(src, dst, k, target, ssem, rsem):
    return pltpu.make_async_remote_copy(src_ref=src, dst_ref=dst, send_sem=ssem.at[k], recv_sem=rsem.at[k],
                                        device_id={AXIS: target}, device_id_type=pl.DeviceIdType.MESH)


def near_peers(pl_):
    return [pl_.at(0, 1), pl_.at(0, -1), pl_.at(1, 0), pl_.at(-1, 0), pl_.at(0, 2), pl_.at(2, 0), pl_.at(0, 0, 1)]


class Sems:
    def __init__(self, ssem, rsem):
        self.ssem, self.rsem, self.used, self.sent = ssem, rsem, 0, []

    def send(self, src, dst, target):
        k = self.used
        self.used += 1
        copy = remote(src, dst, k, target, self.ssem, self.rsem)
        copy.start()
        self.sent.append(copy)
        return k

    def wait(self, k, dst, anyone):
        remote(dst, dst, k, anyone, self.ssem, self.rsem).wait_recv()


def gather_steps(place, sems, region, pieces, relay, halves):
    partner = place.at(0, 0, 1)

    def dev(h, a, b, dc=0):
        return place.at(b, a, dc) if h == 0 else place.at(a, b, dc)

    def send(h, a, b, lo, num, target):
        where = region(dev(h, a, b), lo, num)
        return sems.send(where, where, target)

    def wait(k, h, a, b, lo, num):
        sems.wait(k, region(dev(h, a, b), lo, num), partner)

    passed = []

    def pass_on(h, a, b, lo, num):
        passed.append((send(h, a, b, lo, num, partner), h, a, b, lo, num))

    first, second, rel1, rel2 = {}, {}, {}, {}
    shifts = (1, -1) if relay else (1, -1, 2)

    def go_second(h, a, lo, num):
        for s in shifts:
            second[h, a, s] = send(h, a, 0, lo, num, dev(h, 0, s))

    for h, lo, num in halves:
        for s in shifts:
            first[h, s] = send(h, 0, 0, lo, num, dev(h, s, 0))
    for h, lo, num in halves:
        go_second(h, 0, lo, num)
    for h, lo, num in halves:
        pass_on(h, 0, 0, lo, num)
    yield
    if not relay:
        for s in shifts:
            for h, lo, num in halves:
                wait(first[h, s], h, -s, 0, lo, num)
                go_second(h, -s, lo, num)
                pass_on(h, -s, 0, lo, num)
            yield
        for a in (0, -1, 1, -2):
            for s in shifts:
                for h, lo, num in halves:
                    wait(second[h, a, s], h, a, -s, lo, num)
                    pass_on(h, a, -s, lo, num)
            yield
    else:
        for s in shifts:
            for h, lo, num in halves:
                wait(first[h, s], h, -s, 0, lo, num)
                part = lo + (s == -1)
                rel1[h, s] = send(h, -s, 0, part, 1, dev(h, s, 0))
                go_second(h, -s, lo, num)
                pass_on(h, -s, 0, lo, num)
            yield

        def relay2(h, lo, num, a, s):
            wait(second[h, a, s], h, a, -s, lo, num)
            part = lo + (s == -1)
            rel2[h, a, s] = send(h, a, -s, part, 1, dev(h, 0, s))
            pass_on(h, a, -s, lo, num)

        for h, lo, num in halves:
            for s in shifts:
                relay2(h, lo, num, 0, s)
        yield
        for h, lo, num in halves:
            for s in shifts:
                wait(rel1[h, s], h, -2 * s, 0, lo + (s == -1), 1)
            go_second(h, 2, lo, num)
            pass_on(h, 2, 0, lo, num)
        yield
        for a in (-1, 1, 2):
            for s in shifts:
                for h, lo, num in halves:
                    relay2(h, lo, num, a, s)
            yield
        for a in (0, -1, 1, 2):
            for h, lo, num in halves:
                for s in shifts:
                    wait(rel2[h, a, s], h, a, -2 * s, lo + (s == -1), 1)
                pass_on(h, a, 2, lo, num)
            yield
    for k, h, a, b, lo, num in passed:
        sems.wait(k, region(dev(h, a, b, 1), lo, num), partner)
    yield


def finish(*gens):
    gens = list(gens)
    while gens:
        gens = [g for g in gens if next(g, gens) is not gens]


NN = (((1,), (0,)), ((), ()))
NT = (((1,), (1,)), ((), ()))
TN = (((0,), (0,)), ((), ()))
EXACT = lax.Precision.HIGHEST


def mm(a, b, dims=NN, precision=None):
    return lax.dot_general(a, b, dims, precision=precision, preferred_element_type=F32)


def three(v):
    a = v.astype(BF16)
    v = v - a.astype(F32)
    b = v.astype(BF16)
    return a, b, (v - b.astype(F32)).astype(BF16)


def iota(shape, dim):
    return lax.broadcasted_iota(jnp.int32, shape, dim)


def inv_rms(v):
    return lax.rsqrt(jnp.mean(v * v, axis=-1, keepdims=True) + NORM_EPS)


def rms_back(v, inv, g):
    return inv * g - v * (inv * inv * inv * jnp.mean(g * v, axis=-1, keepdims=True))


def block_offset(i, place):
    g, b = i // (2 * place.side), lax.rem(i, 2 * place.side)
    dx, dc = b // 2, lax.rem(b, 2)
    return lax.rem(g + dx, place.side), dx, dc


def layer_kernel(group, experts, cap, x_ref, idst_ref, dy_ref, wq_ref, wk_ref, wv_ref, wo_ref, wr_ref, wg_ref, wu_ref, wd_ref,
                 y_ref, gx_ref, gg_ref, gu_ref, gd_ref,
                 w_full, u_all, dy_all, ids_all, g_all, m_s, r_s, pick_s, ru_s, rdy_s, ag_s, au_s, mid_s, dag_s, dau_s,
                 zback, dback, prob_s, q_s, k_s, v_s, o_s, hid_s, place_s,
                 lsem, ssem, rsem):
    place = Place(group)
    me = place.me
    toks, d_model = x_ref.shape
    choices = idst_ref.shape[0]
    local, _, ff = wg_ref.shape
    depth = wq_ref.shape[0]
    per = 2 * place.side
    groups = group // per
    sems = Sems(ssem, rsem)

    def rows_of(d):
        return pl.ds(pl.multiple_of(d * depth, depth), depth)

    own_w = [pltpu.make_async_copy(w, w_full.at[i, rows_of(me)], lsem.at[i]) for i, w in enumerate((wq_ref, wk_ref, wv_ref, wo_ref))]
    for copy in own_w:
        copy.start()
    sem = pltpu.get_barrier_semaphore()
    peers = near_peers(place)
    for peer in peers:
        pl.semaphore_signal(sem, inc=1, device_id={AXIS: peer}, device_id_type=pl.DeviceIdType.MESH)

    dy_all[me] = dy_ref[...]
    idst = idst_ref[...].astype(F32)
    ids_all[me] = idst
    lane_e = iota((2 * experts, toks), 0).astype(F32)
    chosen_t = jnp.zeros((2 * experts, toks), F32)
    for j in range(choices):
        chosen_t += jnp.where(idst[j:j + 1, :] == lane_e, 1.0, 0.0)
    chosen = jnp.transpose(chosen_t)[:, :experts]
    before = (iota((toks, toks), 0) > iota((toks, toks), 1)).astype(F32).astype(BF16)
    rank = mm(before, chosen.astype(BF16))
    rank_b = jnp.where(chosen > 0.0, rank, -1.0).astype(BF16)
    x = x_ref[...].astype(F32)
    x_inv = inv_rms(x)
    a = (x * x_inv).astype(BF16)

    for copy in own_w:
        copy.wait()
    pl.semaphore_wait(sem, len(peers))
    quarter = toks // 4
    two = ((0, 0, 2), (1, 2, 2))
    w_steps = gather_steps(place, sems, lambda d, lo, num: w_full.at[pl.ds(lo, num), rows_of(d)], 4, False, two)
    ids_steps = gather_steps(place, sems, lambda d, lo, num: ids_all.at[d], 1, False, ((0, 0, 1),))
    dy_steps = gather_steps(place, sems, lambda d, lo, num: dy_all.at[d, pl.ds(lo * quarter, num * quarter)], 4, True, two)
    for _ in range(4):
        next(w_steps)
    next(ids_steps)
    next(dy_steps)
    for i in range(4):
        next(w_steps)
        next(ids_steps)
        next(dy_steps, None)
    finish(w_steps)

    q_s[...] = mm(a, w_full[0]).astype(BF16)
    k_s[...] = mm(a, w_full[1]).astype(BF16)
    v_s[...] = mm(a, w_full[2]).astype(BF16)
    next(dy_steps, None)
    causal = iota((toks, toks), 0) >= iota((toks, toks), 1)
    low = iota((toks, 2 * HEAD_DIM), 1) < HEAD_DIM
    zero_b = jnp.zeros((toks, 2 * HEAD_DIM), BF16)
    pairs = d_model // (2 * HEAD_DIM)
    scale = HEAD_DIM ** -0.5

    def half(v, side):
        return jnp.where(low, v, zero_b) if side == 0 else jnp.where(low, zero_b, v)

    for pair in range(pairs):
        lanes = pl.ds(pair * 2 * HEAD_DIM, 2 * HEAD_DIM)
        qp, kp, vp = q_s[:, lanes], k_s[:, lanes], v_s[:, lanes]
        outs = []
        for side in range(2):
            s = jnp.where(causal, mm(half(qp, side), kp, NT) * scale, -1e30)
            e = jnp.exp(s - jnp.max(s, axis=-1, keepdims=True))
            p = e / jnp.sum(e, axis=-1, keepdims=True)
            prob_s[2 * pair + side] = p
            outs.append(mm(p.astype(BF16), vp))
        o_s[:, lanes] = jnp.where(low, outs[0], outs[1]).astype(BF16)
        next(dy_steps, None)
        next(ids_steps, None)

    hid = (x + mm(o_s[...], w_full[3])).astype(BF16)
    hid_s[...] = hid
    h = hid.astype(F32)
    h_inv = inv_rms(h)
    n = h * h_inv
    u_all[me] = n.astype(BF16)
    logits = mm(n, wr_ref[...], precision=EXACT)
    top = jnp.max(jnp.where(chosen > 0.0, logits, -3e38), axis=-1, keepdims=True)
    expd = jnp.where(chosen > 0.0, jnp.exp(logits - top), 0.0)
    gates = expd / jnp.sum(expd, axis=-1, keepdims=True)
    gates_t = jnp.transpose(jnp.concatenate([gates, jnp.zeros_like(gates)], axis=-1))
    for j in range(choices):
        g_all[me, j:j + 1, :] = jnp.sum(jnp.where(idst[j:j + 1, :] == lane_e, gates_t, 0.0), axis=0, keepdims=True)

    u_steps = gather_steps(place, sems, lambda d, lo, num: u_all.at[d, pl.ds(lo * quarter, num * quarter)], 4, True, two)
    g_steps = gather_steps(place, sems, lambda d, lo, num: g_all.at[d], 1, False, ((0, 0, 1),))
    next(u_steps)
    next(g_steps)
    finish(ids_steps)

    first_e = (me * local).astype(F32)
    row8 = iota((8, toks), 0)

    def find(i, _):
        ids = ids_all[place.at(*block_offset(i, place))]
        m = jnp.zeros((8, toks), F32)
        for e in range(local):
            hit = jnp.sum(jnp.where(ids == first_e + e, 1.0, 0.0), axis=0, keepdims=True)
            m = jnp.where(row8 == e, hit, m)
        m_s[i] = m
        return 0

    lax.fori_loop(0, group, find, 0)
    next(u_steps)
    next(g_steps, None)
    m_flat = m_s[...].reshape(group * 8, toks)
    after = (iota((toks, toks), 0) < iota((toks, toks), 1)).astype(F32).astype(BF16)
    r_flat = jnp.where(m_flat > 0.0, mm(m_flat.astype(BF16), after), -1.0)
    r_s[...] = r_flat.reshape(group, 8, toks)
    next(u_steps)
    next(g_steps, None)
    slot = iota((cap, toks), 0).astype(F32)

    def build(i, _):
        r = r_s[i]
        for e in range(local):
            pick_s[i, pl.ds(e * cap, cap), :] = jnp.where(slot == r[e:e + 1, :], 1.0, 0.0).astype(BF16)
        return 0

    lax.fori_loop(0, group, build, 0)
    next(u_steps)
    next(g_steps, None)
    finish(dy_steps)

    def take_rows(i, source, dest):
        rows = mm(pick_s[i], source[place.at(*block_offset(i, place))]).astype(BF16)
        for e in range(local):
            dest[e, pl.ds(pl.multiple_of(i * cap, cap), cap), :] = rows[e * cap:(e + 1) * cap]

    def take_dy(i, _):
        take_rows(i, dy_all, rdy_s)
        return 0

    lax.fori_loop(0, group // 2, take_dy, 0)
    next(u_steps)
    next(g_steps, None)
    lax.fori_loop(group // 2, group, take_dy, 0)
    finish(u_steps, g_steps)
    for copy in sems.sent:
        copy.wait_send()
    sems.sent = []

    z_base = sems.used
    sems.used += 2 * group
    d_base = z_base + group
    span = per * cap

    def outgoing(part, i):
        return dy_all.at[i, pl.ds(part * local * cap, local * cap)]

    def ship(part, i, back, base):
        target = place.at(*block_offset(i, place))
        return remote(outgoing(part, i), back.at[me], base + i, target, ssem, rsem)

    def put(part, e, g, rows):
        for b in range(per):
            dy_all[g * per + b, pl.ds((part * local + e) * cap, cap), :] = rows[b * cap:(b + 1) * cap]

    def start_group(part, g, back, base):
        @pl.when(g > 0)
        def _():
            ship(part, g * per, back, base).start()

        @pl.when(g == 0)
        def _():
            back[me] = outgoing(part, 0)[...]
        for b in range(1, per):
            ship(part, g * per + b, back, base).start()

    def forward(g, _):
        for b in range(per):
            take_rows(g * per + b, u_all, ru_s)
        rows = pl.ds(pl.multiple_of(g * span, span), span)
        for e in range(local):
            ru = ru_s[e, rows, :]
            ag = mm(ru, wg_ref[e])
            au = mm(ru, wu_ref[e])
            mid = (ag * jax.nn.sigmoid(ag) * au).astype(BF16)
            ag_s[e, rows, :] = ag
            au_s[e, rows, :] = au
            mid_s[e, rows, :] = mid
            put(0, e, g, mm(mid, wd_ref[e]).astype(BF16))
        start_group(0, g, zback, z_base)
        return 0

    lax.fori_loop(0, groups, forward, 0)

    def backward(g, _):
        for b in range(per):
            i = g * per + b
            d = place.at(*block_offset(i, place))
            ids, gts = ids_all[d], g_all[d]
            for e in range(local):
                gate = jnp.sum(jnp.where(ids == first_e + e, gts, 0.0), axis=0, keepdims=True)
                col = jnp.sum(pick_s[i, pl.ds(e * cap, cap), :].astype(F32) * gate, axis=-1, keepdims=True)
                at = pl.ds(pl.multiple_of(i * cap, cap), cap)
                rdy_s[e, at, :] = (col * rdy_s[e, at, :].astype(F32)).astype(BF16)
        rows = pl.ds(pl.multiple_of(g * span, span), span)
        for e in range(local):
            gm = mm(rdy_s[e, rows, :], wd_ref[e], NT)
            ag, au = ag_s[e, rows, :], au_s[e, rows, :]
            sg = jax.nn.sigmoid(ag)
            dag = (gm * au * sg * (1.0 + ag * (1.0 - sg))).astype(BF16)
            dau = (gm * ag * sg).astype(BF16)
            dag_s[e, rows, :] = dag
            dau_s[e, rows, :] = dau
            put(1, e, g, (mm(dag, wg_ref[e], NT) + mm(dau, wu_ref[e], NT)).astype(BF16))
        start_group(1, g, dback, d_base)
        return 0

    lax.fori_loop(0, groups, backward, 0)

    def weights(e, _):
        gd_ref[e] = mm(mid_s[e], rdy_s[e], TN).astype(BF16)
        gg_ref[e] = mm(ru_s[e], dag_s[e], TN).astype(BF16)
        gu_ref[e] = mm(ru_s[e], dau_s[e], TN).astype(BF16)
        return 0

    lax.fori_loop(0, local, weights, 0)

    def arrived(part, back, base):
        def one(i, _):
            dy_, dx_, dc_ = block_offset(i, place)
            origin = place.at(-dy_, -dx_, dc_)
            remote(back.at[origin], back.at[origin], base + i, origin, ssem, rsem).wait_recv()
            return 0
        lax.fori_loop(1, group, one, 0)

    wide = per * local * cap
    col = iota((1, wide), 1)
    colmod = col
    for _ in range(1, per * local):
        colmod = jnp.where(colmod >= cap, colmod - cap, colmod)
    colmod = colmod.astype(F32)
    g3 = three(gates)
    dyv = dy_ref[...]
    e_row, e_col = iota((experts, wide), 0), iota((experts, wide), 1)

    def combine(c, carry):
        y_sum, gg_sum = carry
        base = (e_row - c * per * local) * cap
        spread = jnp.where((e_col >= base) & (e_col < base + cap), 1.0, 0.0).astype(BF16)
        z = zback[pl.ds(c * per, per)].reshape(wide, d_model)
        here = mm(rank_b, spread) == colmod
        place_s[c] = jnp.where(here, 1.0, 0.0).astype(BF16)
        for piece in g3:
            y_sum += mm(jnp.where(here, mm(piece, spread), 0.0).astype(BF16), z)
        for piece in three(jnp.where(here, mm(dyv, z, NT), 0.0)):
            gg_sum += mm(piece, spread, NT)
        return y_sum, gg_sum

    arrived(0, zback, z_base)
    y_sum, g_gates = lax.fori_loop(0, groups, combine, (jnp.zeros((toks, d_model), F32), jnp.zeros((toks, experts), F32)))
    y_ref[...] = (hid_s[...].astype(F32) + y_sum).astype(BF16)
    g_logits = gates * (g_gates - jnp.sum(gates * g_gates, axis=-1, keepdims=True))
    g_hnorm = mm(g_logits, wr_ref[...], NT, EXACT)

    arrived(1, dback, d_base)
    gn = g_hnorm
    for c in range(groups):
        gn += mm(place_s[c], dback[c * per:(c + 1) * per].reshape(wide, d_model))
    h = hid_s[...].astype(F32)
    h_inv = inv_rms(h)
    g_hid = (dyv.astype(F32) + rms_back(h, h_inv, gn)).astype(BF16)
    o_s[...] = mm(g_hid, w_full[3], NT).astype(BF16)
    g_xn = jnp.zeros((toks, d_model), F32)
    for pair in range(pairs):
        lanes = pl.ds(pair * 2 * HEAD_DIM, 2 * HEAD_DIM)
        qp, kp, vp, dop = q_s[:, lanes], k_s[:, lanes], v_s[:, lanes], o_s[:, lanes]
        dq, dk, dv = [], [], []
        for side in range(2):
            p = prob_s[2 * pair + side]
            dp = mm(half(dop, side), vp, NT)
            ds = (p * (dp - jnp.sum(dp * p, axis=-1, keepdims=True)) * scale).astype(BF16)
            dq.append(mm(ds, kp))
            dk.append(mm(ds, qp, TN))
            dv.append(mm(p.astype(BF16), dop, TN))
        for i, parts in enumerate((dq, dk, dv)):
            grad = jnp.where(low, parts[0], parts[1]).astype(BF16)
            g_xn += mm(grad, w_full[i, :, lanes], NT)
    x = x_ref[...].astype(F32)
    gx_ref[...] = (g_hid.astype(F32) + rms_back(x, inv_rms(x), g_xn)).astype(BF16)

    def sent(i, _):
        ship(0, i, zback, z_base).wait_send()
        ship(1, i, dback, d_base).wait_send()
        return 0

    lax.fori_loop(1, group, sent, 0)


def solution(mesh):
    group = mesh.shape[AXIS]
    tok_spec = P(('dp', 'ep'), None)
    fsdp_spec = P('ep', None)
    expert_spec = P('ep', None, None)
    grad_spec = P(('dp', 'ep'), None, None)

    def device_step(x_tokens, expert_ids, grad_y, w_q, w_k, w_v, w_o, w_router, w_gate, w_up, w_down):
        toks, d_model = x_tokens.shape
        choices = expert_ids.shape[1]
        experts = w_router.shape[1]
        local, _, ff = w_gate.shape
        avg_load = toks * choices // experts
        cap = avg_load + avg_load // 2
        assert toks == SEQ_LEN
        heads = w_q.shape[1] // HEAD_DIM
        shape, vm = jax.ShapeDtypeStruct, pltpu.VMEM
        rows = group * cap
        per = 2 * math.isqrt(group // 2)
        in_vmem = pl.BlockSpec(memory_space=pltpu.VMEM)
        in_hbm = pl.BlockSpec(memory_space=pl.ANY)
        n_sem = 62 + 31 + 84 + 84 + 31 + 2 * group
        square = vm((toks, d_model), BF16)
        return pl.pallas_call(
            functools.partial(layer_kernel, group, experts, cap),
            out_shape=[shape(x_tokens.shape, BF16), shape(x_tokens.shape, BF16), shape(w_gate.shape, BF16),
                       shape(w_up.shape, BF16), shape(w_down.shape, BF16)],
            in_specs=[in_vmem] * 3 + [in_hbm] * 4 + [in_vmem] * 4,
            out_specs=[in_vmem] * 5,
            scratch_shapes=[
                vm((4, group * w_q.shape[0], d_model), BF16), vm((group, toks, d_model), BF16), vm((group, toks, d_model), BF16),
                vm((group, choices, toks), F32), vm((group, choices, toks), F32), vm((group, 8, toks), F32), vm((group, 8, toks), F32),
                vm((group, local * cap, toks), BF16), vm((local, rows, d_model), BF16), vm((local, rows, d_model), BF16),
                vm((local, rows, ff), F32), vm((local, rows, ff), F32),
                vm((local, rows, ff), BF16), vm((local, rows, ff), BF16), vm((local, rows, ff), BF16),
                vm((group, local * cap, d_model), BF16), vm((group, local * cap, d_model), BF16),
                vm((heads, toks, toks), F32), square, square, square, square, square,
                vm((group // per, toks, per * local * cap), BF16),
                pltpu.SemaphoreType.DMA((4,)), pltpu.SemaphoreType.DMA((n_sem,)), pltpu.SemaphoreType.DMA((n_sem,))],
            compiler_params=pltpu.CompilerParams(collective_id=1, has_side_effects=True, vmem_limit_bytes=67043328),
            name='layer')(x_tokens, expert_ids.T, grad_y, w_q, w_k, w_v, w_o, w_router, w_gate, w_up, w_down)

    return jax.shard_map(
        device_step, mesh=mesh,
        in_specs=(tok_spec, tok_spec, tok_spec, fsdp_spec, fsdp_spec, fsdp_spec, fsdp_spec,
                  P(None, None), expert_spec, expert_spec, expert_spec),
        out_specs=(tok_spec, tok_spec, grad_spec, grad_spec, grad_spec),
        check_vma=False)
```

```python
import functools
import math

import jax
import jax.numpy as jnp
from jax import lax
from jax.experimental import pallas as pl
from jax.experimental.pallas import tpu as pltpu
from jax.sharding import PartitionSpec as P

NORM_EPS = 1e-6
SEQ_LEN = 256
HEAD_DIM = 64
AXIS = 'ep'
N_SEND = 9
N_RECV = 109
F32 = jnp.float32
BF16 = jnp.bfloat16


class Place:
    def __init__(self, group):
        self.group = group
        self.side = math.isqrt(group // 2)
        self.me = lax.axis_index(AXIS)
        self.core = lax.rem(self.me, 2)
        self.x = lax.rem(self.me // 2, self.side)
        self.y = self.me // (2 * self.side)

    def wrap(self, v):
        return lax.rem(v + self.side, self.side)

    def at(self, dy, dx, dc=0):
        return (self.wrap(self.y + dy) * self.side + self.wrap(self.x + dx)) * 2 + lax.rem(self.core + dc, 2)


def near_peers(pl_):
    return [pl_.at(0, 1), pl_.at(0, -1), pl_.at(1, 0), pl_.at(-1, 0), pl_.at(0, 2), pl_.at(2, 0), pl_.at(0, 0, 1)]


class Sems:
    def __init__(self, ssem, rsem):
        self.ssem, self.rsem, self.n_send, self.n_recv = ssem, rsem, 0, 0

    def new_send(self):
        self.n_send += 1
        return self.n_send - 1

    def new_recv(self, count=1):
        self.n_recv += count
        return self.n_recv - count

    def copy(self, src, dst, ks, kr, target):
        return pltpu.make_async_remote_copy(
            src_ref=src, dst_ref=dst, send_sem=self.ssem.at[ks], recv_sem=self.rsem.at[kr],
            device_id={AXIS: target}, device_id_type=pl.DeviceIdType.MESH)


def gather_steps(place, sems, region, most, relay, halves, merge=False):
    partner = place.at(0, 0, 1)
    chips = place.side * place.side
    ks, k_pass = sems.new_send(), sems.new_recv()
    k_second = sems.new_recv() if merge else None

    def dev(h, a, b, dc=0):
        return place.at(b, a, dc) if h == 0 else place.at(a, b, dc)

    def send(h, a, b, lo, num, target, kr=None):
        where = region(dev(h, a, b), lo, num)
        kr = sems.new_recv() if kr is None else kr
        sems.copy(where, where, ks, kr, target).start()
        return kr

    def wait(kr, h, a, b, lo, num):
        where = region(dev(h, a, b), lo, num)
        sems.copy(where, where, ks, kr, partner).wait_recv()

    def wait_most(kr, n):
        sems.copy(most(n), most(n), ks, kr, partner).wait_recv()

    def pass_on(h, a, b, lo, num):
        send(h, a, b, lo, num, partner, k_pass)

    first, second, rel1, rel2 = {}, {}, {}, {}
    shifts = (1, -1) if relay else (1, -1, 2)

    def go_second(h, a, lo, num):
        for s in shifts:
            second[h, a, s] = send(h, a, 0, lo, num, dev(h, 0, s), k_second)

    for h, lo, num in halves:
        for s in shifts:
            first[h, s] = send(h, 0, 0, lo, num, dev(h, s, 0))
    for h, lo, num in halves:
        go_second(h, 0, lo, num)
    for h, lo, num in halves:
        pass_on(h, 0, 0, lo, num)
    yield
    if not relay:
        for s in shifts:
            for h, lo, num in halves:
                wait(first[h, s], h, -s, 0, lo, num)
                go_second(h, -s, lo, num)
                pass_on(h, -s, 0, lo, num)
            yield
        if merge:
            wait_most(k_second, chips - place.side)
        for a in (0, -1, 1, -2):
            for s in shifts:
                for h, lo, num in halves:
                    if not merge:
                        wait(second[h, a, s], h, a, -s, lo, num)
                    pass_on(h, a, -s, lo, num)
            yield
    else:
        def relay_on(kr, h, a, b, lo, s, ta, tb):
            part = lo + (s == -1)
            return send(h, a, b, part, 1, dev(h, ta, tb), kr)

        for s in shifts:
            for h, lo, num in halves:
                wait(first[h, s], h, -s, 0, lo, num)
                rel1[h] = relay_on(rel1.get(h), h, -s, 0, lo, s, s, 0)
                go_second(h, -s, lo, num)
                pass_on(h, -s, 0, lo, num)
            yield

        def relay2(h, lo, num, a, s):
            wait(second[h, a, s], h, a, -s, lo, num)
            rel2[h, a] = relay_on(rel2.get((h, a)), h, a, -s, lo, s, 0, s)
            pass_on(h, a, -s, lo, num)

        for h, lo, num in halves:
            for s in shifts:
                relay2(h, lo, num, 0, s)
        yield
        for h, lo, num in halves:
            wait(rel1[h], h, 2, 0, lo, num)
            go_second(h, 2, lo, num)
            pass_on(h, 2, 0, lo, num)
        yield
        for a in (-1, 1, 2):
            for s in shifts:
                for h, lo, num in halves:
                    relay2(h, lo, num, a, s)
            yield
        for a in (0, -1, 1, 2):
            for h, lo, num in halves:
                wait(rel2[h, a], h, a, 2, lo, num)
                pass_on(h, a, 2, lo, num)
            yield
    wait_most(k_pass, chips)
    yield
    sems.copy(most(2 * chips - 1), most(2 * chips - 1), ks, k_pass, partner).wait_send()
    yield


def finish(*gens):
    gens = list(gens)
    while gens:
        gens = [g for g in gens if next(g, gens) is not gens]


NN = (((1,), (0,)), ((), ()))
NT = (((1,), (1,)), ((), ()))
TN = (((0,), (0,)), ((), ()))
EXACT = lax.Precision.HIGHEST


def mm(a, b, dims=NN, precision=None):
    return lax.dot_general(a, b, dims, precision=precision, preferred_element_type=F32)


def three(v):
    a = v.astype(BF16)
    v = v - a.astype(F32)
    b = v.astype(BF16)
    return a, b, (v - b.astype(F32)).astype(BF16)


def iota(shape, dim):
    return lax.broadcasted_iota(jnp.int32, shape, dim)


def inv_rms(v):
    return lax.rsqrt(jnp.mean(v * v, axis=-1, keepdims=True) + NORM_EPS)


def rms_back(v, inv, g):
    return inv * g - v * (inv * inv * inv * jnp.mean(g * v, axis=-1, keepdims=True))


def block_offset(i, side):
    return lax.rem(i // 2, side), i // (2 * side), lax.rem(i, 2)


def block_place(i, e, side):
    dy, dx, dc = block_offset(i, side)
    return i if e == 0 else (dy * side + dx) * 2 + dc


def layer_kernel(group, experts, cap, x_ref, idst_ref, dy_ref, wq_ref, wk_ref, wv_ref, wo_ref, wr_ref, wg_in, wu_in, wd_in,
                 y_ref, gx_ref, gg_ref, gu_ref, gd_ref,
                 w_full, u_all, dy_all, ids_all, g_all, m_s, r_s, pick_s, ru_s, rdy_s, ag_s, au_s, mid_s, dag_s, dau_s,
                 wg_ref, wu_ref, wd_ref, relay, zback, dback, prob_s, q_s, k_s, v_s, o_s, hid_s, place_s, gg_s, gu_s, gd_s, y_s,
                 lsem, ssem, rsem):
    place = Place(group)
    me = place.me
    toks, d_model = x_ref.shape
    choices = idst_ref.shape[0]
    local, _, ff = wg_in.shape
    depth = wq_ref.shape[0]
    per = 2 * place.side
    groups = group // per
    sems = Sems(ssem, rsem)

    def rows_of(d):
        return pl.ds(pl.multiple_of(d * depth, depth), depth)

    own_w = [pltpu.make_async_copy(w, w_full.at[i, rows_of(me)], lsem.at[i]) for i, w in enumerate((wq_ref, wk_ref, wv_ref, wo_ref))]
    experts_in = [pltpu.make_async_copy(src, dst, lsem.at[4 + i])
                  for i, (src, dst) in enumerate(((wg_in, wg_ref), (wu_in, wu_ref), (wd_in, wd_ref)))]
    for copy in own_w + experts_in:
        copy.start()
    sem = pltpu.get_barrier_semaphore()
    peers = near_peers(place)
    for peer in peers:
        pl.semaphore_signal(sem, inc=1, device_id={AXIS: peer}, device_id_type=pl.DeviceIdType.MESH)

    dy_all[me] = dy_ref[...]
    idst = idst_ref[...].astype(F32)
    ids_all[me] = idst
    lane_e = iota((2 * experts, toks), 0).astype(F32)
    chosen_t = jnp.zeros((2 * experts, toks), F32)
    for j in range(choices):
        chosen_t += jnp.where(idst[j:j + 1, :] == lane_e, 1.0, 0.0)
    chosen = jnp.transpose(chosen_t)[:, :experts]
    before = (iota((toks, toks), 0) > iota((toks, toks), 1)).astype(F32).astype(BF16)
    rank = mm(before, chosen.astype(BF16))
    rank_b = jnp.where(chosen > 0.0, rank, -1.0).astype(BF16)
    x = x_ref[...].astype(F32)
    x_inv = inv_rms(x)
    a = (x * x_inv).astype(BF16)

    for copy in own_w:
        copy.wait()
    pl.semaphore_wait(sem, len(peers))
    quarter = toks // 4
    two = ((0, 0, 2), (1, 2, 2))
    w_steps = gather_steps(place, sems, lambda d, lo, num: w_full.at[pl.ds(lo, num), rows_of(d)],
                           lambda n: w_full.at[:, pl.ds(0, n * depth)], False, two)
    ids_steps = gather_steps(place, sems, lambda d, lo, num: ids_all.at[d], lambda n: ids_all.at[pl.ds(0, n)], False, ((0, 0, 1),), True)
    dy_steps = gather_steps(place, sems, lambda d, lo, num: dy_all.at[d, pl.ds(lo * quarter, num * quarter)],
                            lambda n: dy_all.at[pl.ds(0, n)], True, two)
    for _ in range(4):
        next(w_steps)
    next(dy_steps)
    finish(w_steps)
    next(ids_steps)

    q_s[...] = mm(a, w_full[0]).astype(BF16)
    k_s[...] = mm(a, w_full[1]).astype(BF16)
    v_s[...] = mm(a, w_full[2]).astype(BF16)
    next(dy_steps, None)
    causal = iota((toks, toks), 0) >= iota((toks, toks), 1)
    low = iota((toks, 2 * HEAD_DIM), 1) < HEAD_DIM
    zero_b = jnp.zeros((toks, 2 * HEAD_DIM), BF16)
    pairs = d_model // (2 * HEAD_DIM)
    scale = HEAD_DIM ** -0.5

    def half(v, side):
        return jnp.where(low, v, zero_b) if side == 0 else jnp.where(low, zero_b, v)

    for pair in range(pairs):
        lanes = pl.ds(pair * 2 * HEAD_DIM, 2 * HEAD_DIM)
        qp, kp, vp = q_s[:, lanes], k_s[:, lanes], v_s[:, lanes]
        outs = []
        for hf in range(2):
            s = jnp.where(causal, mm(half(qp, hf), kp, NT) * scale, -1e30)
            e = jnp.exp(s - jnp.max(s, axis=-1, keepdims=True))
            p = e / jnp.sum(e, axis=-1, keepdims=True)
            prob_s[2 * pair + hf] = p
            outs.append(mm(p.astype(BF16), vp))
        o_s[:, lanes] = jnp.where(low, outs[0], outs[1]).astype(BF16)
        next(dy_steps, None)
        next(ids_steps, None)

    hid = (x + mm(o_s[...], w_full[3])).astype(BF16)
    hid_s[...] = hid
    h = hid.astype(F32)
    h_inv = inv_rms(h)
    n = h * h_inv
    u_all[me] = n.astype(BF16)
    logits = mm(n, wr_ref[...], NT, EXACT)
    top = jnp.max(jnp.where(chosen > 0.0, logits, -3e38), axis=-1, keepdims=True)
    expd = jnp.where(chosen > 0.0, jnp.exp(logits - top), 0.0)
    gates = expd / jnp.sum(expd, axis=-1, keepdims=True)
    gates_t = jnp.transpose(jnp.concatenate([gates, jnp.zeros_like(gates)], axis=-1))
    for j in range(choices):
        g_all[me, j:j + 1, :] = jnp.sum(jnp.where(idst[j:j + 1, :] == lane_e, gates_t, 0.0), axis=0, keepdims=True)

    u_steps = gather_steps(place, sems, lambda d, lo, num: u_all.at[d, pl.ds(lo * quarter, num * quarter)],
                           lambda n: u_all.at[pl.ds(0, n)], True, two)
    g_steps = gather_steps(place, sems, lambda d, lo, num: g_all.at[d], lambda n: g_all.at[pl.ds(0, n)], False, ((0, 0, 1),), True)
    next(u_steps)
    next(g_steps)
    finish(ids_steps)

    first_e = (me * local).astype(F32)
    row8 = iota((8, toks), 0)

    def find(i, _):
        ids = ids_all[place.at(*block_offset(i, place.side))]
        m = jnp.zeros((8, toks), F32)
        for e in range(local):
            hit = jnp.sum(jnp.where(ids == first_e + e, 1.0, 0.0), axis=0, keepdims=True)
            m = jnp.where(row8 == e, hit, m)
        m_s[i] = m
        return 0

    lax.fori_loop(0, group, find, 0)
    next(u_steps)
    next(dy_steps, None)
    m_flat = m_s[...].reshape(group * 8, toks)
    after = (iota((toks, toks), 0) < iota((toks, toks), 1)).astype(F32).astype(BF16)
    r_flat = jnp.where(m_flat > 0.0, mm(m_flat.astype(BF16), after), -1.0)
    r_s[...] = r_flat.reshape(group, 8, toks)
    next(u_steps)
    next(dy_steps, None)
    next(g_steps, None)
    slot = iota((cap, toks), 0).astype(F32)

    def build(i, _):
        r = r_s[i]
        for e in range(local):
            pick_s[i, pl.ds(e * cap, cap), :] = jnp.where(slot == r[e:e + 1, :], 1.0, 0.0).astype(BF16)
        return 0

    lax.fori_loop(0, group, build, 0)

    def take_rows(i, source, dest):
        rows = mm(pick_s[i], source[place.at(*block_offset(i, place.side))]).astype(BF16)
        for e in range(local):
            at = block_place(i, e, place.side) * cap
            dest[e, pl.ds(pl.multiple_of(at, cap), cap), :] = rows[e * cap:(e + 1) * cap]

    def take_dy(g, _):
        for b in range(per):
            take_rows(g * per + b, dy_all, rdy_s)
        return 0

    while next(u_steps, place) is None:
        next(dy_steps, None)
        next(g_steps, None)
    for copy in experts_in:
        copy.wait()

    span = per * cap
    side = place.side

    def axis(e, d1, d2, dc):
        return place.at(d2, d1, dc) if e == 0 else place.at(d1, d2, dc)

    k_first = sems.new_recv(2 * local)
    k_second = sems.new_recv(2)
    k_sent = [(sems.new_send(), sems.new_send()) for _ in range(2)]

    def first_hop(part, e, d1):
        src = u_all.at[pl.ds(d1 * per, per), pl.ds((part * local + e) * cap, cap)]
        return sems.copy(src, relay.at[part, e, d1], k_sent[part][0], k_first + part * local + e, axis(e, d1, 0, 0))

    def first_done(part, e):
        at = relay.at[part, e, pl.ds(1, side - 1)]
        return sems.copy(at, at, k_sent[part][0], k_first + part * local + e, me)

    def second_hop(part, e, d2, dc):
        back = (zback, dback)[part]
        return sems.copy(relay.at[part, e, :, 2 * d2 + dc], back.at[e, d2, dc], k_sent[part][1], k_second + part,
                         axis(e, 0, d2, dc))

    def all_first(part):
        at = relay.at[part, :, pl.ds(1, side - 1)]
        return sems.copy(at, at, k_sent[part][0], k_second, me)

    def all_second(part):
        at = relay.at[part, :, :, pl.ds(0, per - 1)]
        return sems.copy(at, at, k_sent[part][1], k_second + part, me)

    ahead = [(d2, dc) for d2 in range(side) for dc in range(2)][1:]
    ahead.sort(key=lambda t: -min(t[0], side - t[0]))

    def pass_rows(part):
        for e in range(local):
            first_done(part, e).wait_recv()
            for d2, dc in ahead:
                second_hop(part, e, d2, dc).start()
        for e in range(local):
            (zback, dback)[part][e, 0, 0] = relay[part, e, :, 0]

    def put(part, e, g, rows):
        @pl.when(g > 0)
        def _():
            for b in range(per):
                u_all[g * per + b, pl.ds((part * local + e) * cap, cap), :] = rows[b * cap:(b + 1) * cap]
            first_hop(part, e, g).start()

        @pl.when(g == 0)
        def _():
            for b in range(per):
                relay[part, e, 0, b] = rows[b * cap:(b + 1) * cap]

    def take_u(g, _):
        for b in range(per):
            take_rows(g * per + b, u_all, ru_s)
        return 0

    lax.fori_loop(0, groups, take_u, 0)

    def forward(step, _):
        g = lax.rem(step + side // 2, side)
        rows = pl.ds(pl.multiple_of(g * span, span), span)
        for e in range(local):
            ru = ru_s[e, rows, :]
            ag = mm(ru, wg_ref[e])
            au = mm(ru, wu_ref[e])
            mid = (ag * jax.nn.sigmoid(ag) * au).astype(BF16)
            ag_s[e, rows, :] = ag
            au_s[e, rows, :] = au
            mid_s[e, rows, :] = mid
            put(0, e, g, mm(mid, wd_ref[e]).astype(BF16))
        return 0

    lax.fori_loop(0, groups, forward, 0)

    def weigh(q, _):
        for i in [q * side + b for b in range(side)]:
            d = place.at(*block_offset(i, side))
            ids, gts = ids_all[d], g_all[d]
            for e in range(local):
                gate = jnp.sum(jnp.where(ids == first_e + e, gts, 0.0), axis=0, keepdims=True)
                col = jnp.sum(pick_s[i, pl.ds(e * cap, cap), :].astype(F32) * gate, axis=-1, keepdims=True)
                at = pl.ds(pl.multiple_of(block_place(i, e, side) * cap, cap), cap)
                rdy_s[e, at, :] = (col * rdy_s[e, at, :].astype(F32)).astype(BF16)
        return 0

    finish(g_steps, dy_steps)
    lax.fori_loop(0, groups, take_dy, 0)
    lax.fori_loop(0, group // side, weigh, 0)

    def backward(step, _):
        g = lax.rem(step + side // 2, side)
        rows = pl.ds(pl.multiple_of(g * span, span), span)
        for e in range(local):
            gm = mm(rdy_s[e, rows, :], wd_ref[e], NT)
            ag, au = ag_s[e, rows, :], au_s[e, rows, :]
            sg = jax.nn.sigmoid(ag)
            dag = (gm * au * sg * (1.0 + ag * (1.0 - sg))).astype(BF16)
            dau = (gm * ag * sg).astype(BF16)
            dag_s[e, rows, :] = dag
            dau_s[e, rows, :] = dau
            put(1, e, g, (mm(dag, wg_ref[e], NT) + mm(dau, wu_ref[e], NT)).astype(BF16))
        return 0

    lax.fori_loop(0, groups, backward, 0)

    def weights(e, _):
        gd_s[e] = mm(mid_s[e], rdy_s[e], TN).astype(BF16)
        gg_s[e] = mm(ru_s[e], dag_s[e], TN).astype(BF16)
        gu_s[e] = mm(ru_s[e], dau_s[e], TN).astype(BF16)
        return 0

    lax.fori_loop(0, local, weights, 0)
    grads_out = [pltpu.make_async_copy(src, dst, lsem.at[i])
                 for i, (src, dst) in enumerate(((gg_s, gg_ref), (gu_s, gu_ref), (gd_s, gd_ref), (y_s, y_ref)))]
    for copy in grads_out[:3]:
        copy.start()

    wide = per * local * cap
    col = iota((1, wide), 1)
    colmod = col
    for _ in range(1, per * local):
        colmod = jnp.where(colmod >= cap, colmod - cap, colmod)
    colmod = colmod.astype(F32)
    g3 = three(gates)
    dyv = dy_ref[...]
    e_row = iota((experts, wide), 0).astype(F32)
    halves = group // per // local

    def combine(c, carry):
        y_sum, gg_sum = carry
        e, top = c // halves, lax.rem(c, halves) * (side // halves)
        owner = jnp.zeros((1, wide), F32)
        for k in range(wide // cap):
            d2, dc, d1 = top + k // per, (k // side) % 2, k % side
            dx, dy = jnp.where(e == 0, d1, d2), jnp.where(e == 0, d2, d1)
            of_block = (place.at(-dy, -dx, dc) * local + e).astype(F32)
            owner = jnp.where((col >= k * cap) & (col < (k + 1) * cap), of_block, owner)
        spread = jnp.where(e_row == owner, 1.0, 0.0).astype(BF16)
        z = zback[e, pl.ds(top, side // halves)].reshape(wide, d_model)
        here = mm(rank_b, spread) == colmod
        place_s[c] = jnp.where(here, 1.0, 0.0).astype(BF16)
        for piece in g3:
            y_sum += mm(jnp.where(here, mm(piece, spread), 0.0).astype(BF16), z)
        for piece in three(jnp.where(here, mm(dyv, z, NT), 0.0)):
            gg_sum += mm(piece, spread, NT)
        return y_sum, gg_sum

    pass_rows(0)
    pass_rows(1)
    all_second(0).wait_recv()
    y_sum, g_gates = lax.fori_loop(0, groups, combine, (jnp.zeros((toks, d_model), F32), jnp.zeros((toks, experts), F32)))
    y_s[...] = (hid_s[...].astype(F32) + y_sum).astype(BF16)
    g_logits = gates * (g_gates - jnp.sum(gates * g_gates, axis=-1, keepdims=True))
    g_hnorm = mm(g_logits, wr_ref[...], NN, EXACT)

    grads_out[3].start()
    all_second(1).wait_recv()
    gn = g_hnorm
    for c in range(groups):
        top = c % halves * (side // halves)
        gn += mm(place_s[c], dback[c // halves, top:top + side // halves].reshape(wide, d_model))
    h = hid_s[...].astype(F32)
    h_inv = inv_rms(h)
    g_hid = (dyv.astype(F32) + rms_back(h, h_inv, gn)).astype(BF16)
    o_s[...] = mm(g_hid, w_full[3], NT).astype(BF16)
    g_xn = jnp.zeros((toks, d_model), F32)
    for pair in range(pairs):
        lanes = pl.ds(pair * 2 * HEAD_DIM, 2 * HEAD_DIM)
        qp, kp, vp, dop = q_s[:, lanes], k_s[:, lanes], v_s[:, lanes], o_s[:, lanes]
        dq, dk, dv = [], [], []
        for hf in range(2):
            p = prob_s[2 * pair + hf]
            dp = mm(half(dop, hf), vp, NT)
            ds = (p * (dp - jnp.sum(dp * p, axis=-1, keepdims=True)) * scale).astype(BF16)
            dq.append(mm(ds, kp))
            dk.append(mm(ds, qp, TN))
            dv.append(mm(p.astype(BF16), dop, TN))
        for i, parts in enumerate((dq, dk, dv)):
            grad = jnp.where(low, parts[0], parts[1]).astype(BF16)
            g_xn += mm(grad, w_full[i, :, lanes], NT)
    x = x_ref[...].astype(F32)
    gx_ref[...] = (g_hid.astype(F32) + rms_back(x, inv_rms(x), g_xn)).astype(BF16)

    for copy in grads_out:
        copy.wait()
    for part in range(2):
        all_first(part).wait_send()
        all_second(part).wait_send()
    assert (sems.n_send, sems.n_recv) == (N_SEND, N_RECV), (sems.n_send, sems.n_recv)


def settle_kernel(*refs):
    n = (len(refs) - 2) // 3
    ins, outs, held, lsem, ssem = refs[:n], refs[n:2 * n], refs[2 * n:3 * n], refs[-2], refs[-1]
    loads = [pltpu.make_async_copy(a, h, lsem.at[i]) for i, (a, h) in enumerate(zip(ins, held))]
    stores = [pltpu.make_async_copy(h, o, ssem.at[i]) for i, (h, o) in enumerate(zip(held, outs))]
    for copy in loads:
        copy.start()
    for load, store in zip(loads, stores):
        load.wait()
        store.start()
    for copy in stores:
        copy.wait()


def settle(*arrays):
    n = len(arrays)
    hbm = pl.BlockSpec(memory_space=pl.ANY)
    return pl.pallas_call(
        settle_kernel, out_shape=[jax.ShapeDtypeStruct(a.shape, a.dtype) for a in arrays],
        in_specs=[hbm] * n, out_specs=[hbm] * n,
        scratch_shapes=[pltpu.VMEM(a.shape, a.dtype) for a in arrays] + [pltpu.SemaphoreType.DMA((n,))] * 2,
        name='settle')(*arrays)


def solution(mesh):
    group = mesh.shape[AXIS]
    tok_spec = P(('dp', 'ep'), None)
    fsdp_spec = P('ep', None)
    expert_spec = P('ep', None, None)
    grad_spec = P(('dp', 'ep'), None, None)

    def device_step(x_tokens, expert_ids, grad_y, w_q, w_k, w_v, w_o, w_router, w_gate, w_up, w_down):
        toks, d_model = x_tokens.shape
        choices = expert_ids.shape[1]
        experts = w_router.shape[1]
        local, _, ff = w_gate.shape
        avg_load = toks * choices // experts
        cap = avg_load + avg_load // 2
        assert toks == SEQ_LEN
        heads = w_q.shape[1] // HEAD_DIM
        shape, vm = jax.ShapeDtypeStruct, pltpu.VMEM
        rows = group * cap
        side = math.isqrt(group // 2)
        per = 2 * side
        hop = (side, per, cap, d_model)
        assert local == 2
        in_vmem = pl.BlockSpec(memory_space=pltpu.VMEM)
        in_hbm = pl.BlockSpec(memory_space=pl.ANY)
        square = vm((toks, d_model), BF16)
        outs = pl.pallas_call(
            functools.partial(layer_kernel, group, experts, cap),
            out_shape=[shape(x_tokens.shape, BF16), shape(x_tokens.shape, BF16), shape(w_gate.shape, BF16),
                       shape(w_up.shape, BF16), shape(w_down.shape, BF16)],
            in_specs=[in_vmem] * 3 + [in_hbm] * 4 + [in_vmem] + [in_hbm] * 3,
            out_specs=[in_hbm, in_vmem] + [in_hbm] * 3,
            scratch_shapes=[
                vm((4, group * w_q.shape[0], d_model), BF16), vm((group, toks, d_model), BF16), vm((group, toks, d_model), BF16),
                vm((group, choices, toks), F32), vm((group, choices, toks), F32), vm((group, 8, toks), F32), vm((group, 8, toks), F32),
                vm((group, local * cap, toks), BF16), vm((local, rows, d_model), BF16), vm((local, rows, d_model), BF16),
                vm((local, rows, ff), F32), vm((local, rows, ff), F32),
                vm((local, rows, ff), BF16), vm((local, rows, ff), BF16), vm((local, rows, ff), BF16),
                vm(w_gate.shape, BF16), vm(w_up.shape, BF16), vm(w_down.shape, BF16), vm((2, local) + hop, BF16),
                vm((local, side, 2, side, cap, d_model), BF16), vm((local, side, 2, side, cap, d_model), BF16),
                vm((heads, toks, toks), F32), square, square, square, square, square,
                vm((group // per, toks, per * local * cap), BF16),
                vm(w_gate.shape, BF16), vm(w_up.shape, BF16), vm(w_down.shape, BF16), square,
                pltpu.SemaphoreType.DMA((7,)), pltpu.SemaphoreType.DMA((N_SEND,)), pltpu.SemaphoreType.DMA((N_RECV,))],
            compiler_params=pltpu.CompilerParams(collective_id=1, has_side_effects=True, vmem_limit_bytes=67043328),
            name='layer')(x_tokens, expert_ids.T, grad_y, w_q, w_k, w_v, w_o, w_router.T, w_gate, w_up, w_down)
        return settle(*outs)

    return jax.shard_map(
        device_step, mesh=mesh,
        in_specs=(tok_spec, tok_spec, tok_spec, fsdp_spec, fsdp_spec, fsdp_spec, fsdp_spec,
                  P(None, None), expert_spec, expert_spec, expert_spec),
        out_specs=(tok_spec, tok_spec, grad_spec, grad_spec, grad_spec),
        check_vma=False)
```

```python
import functools
import math

import jax
import jax.numpy as jnp
from jax import lax
from jax.experimental import pallas as pl
from jax.experimental.pallas import tpu as pltpu
from jax.sharding import PartitionSpec as P

NORM_EPS = 1e-6
SEQ_LEN = 256
HEAD_DIM = 64
AXIS = 'ep'
N_SEND = 10
N_RECV = 110
F32 = jnp.float32
BF16 = jnp.bfloat16


class Place:
    def __init__(self, group):
        self.group = group
        self.side = math.isqrt(group // 2)
        self.me = lax.axis_index(AXIS)
        self.core = lax.rem(self.me, 2)
        self.x = lax.rem(self.me // 2, self.side)
        self.y = self.me // (2 * self.side)

    def wrap(self, v):
        return lax.rem(v + self.side, self.side)

    def at(self, dy, dx, dc=0):
        return (self.wrap(self.y + dy) * self.side + self.wrap(self.x + dx)) * 2 + lax.rem(self.core + dc, 2)


def near_peers(pl_):
    return [pl_.at(0, 1), pl_.at(0, -1), pl_.at(1, 0), pl_.at(-1, 0), pl_.at(0, 2), pl_.at(2, 0), pl_.at(0, 0, 1)]


class Sems:
    def __init__(self, ssem, rsem):
        self.ssem, self.rsem, self.n_send, self.n_recv = ssem, rsem, 0, 0

    def new_send(self):
        self.n_send += 1
        return self.n_send - 1

    def new_recv(self, count=1):
        self.n_recv += count
        return self.n_recv - count

    def copy(self, src, dst, ks, kr, target):
        return pltpu.make_async_remote_copy(
            src_ref=src, dst_ref=dst, send_sem=self.ssem.at[ks], recv_sem=self.rsem.at[kr],
            device_id={AXIS: target}, device_id_type=pl.DeviceIdType.MESH)


def gather_steps(place, sems, region, most, relay, halves, merge=False):
    partner = place.at(0, 0, 1)
    chips = place.side * place.side
    ks, k_pass = sems.new_send(), sems.new_recv()
    k_second = sems.new_recv() if merge else None

    def dev(h, a, b, dc=0):
        return place.at(b, a, dc) if h == 0 else place.at(a, b, dc)

    def send(h, a, b, lo, num, target, kr=None):
        where = region(dev(h, a, b), lo, num)
        kr = sems.new_recv() if kr is None else kr
        sems.copy(where, where, ks, kr, target).start()
        return kr

    def wait(kr, h, a, b, lo, num):
        where = region(dev(h, a, b), lo, num)
        sems.copy(where, where, ks, kr, partner).wait_recv()

    def wait_most(kr, n):
        sems.copy(most(n), most(n), ks, kr, partner).wait_recv()

    def pass_on(h, a, b, lo, num):
        send(h, a, b, lo, num, partner, k_pass)

    first, second, rel1, rel2 = {}, {}, {}, {}
    shifts = (1, -1) if relay else (1, -1, 2)

    def go_second(h, a, lo, num):
        for s in shifts:
            second[h, a, s] = send(h, a, 0, lo, num, dev(h, 0, s), k_second)

    for h, lo, num in halves:
        for s in shifts:
            first[h, s] = send(h, 0, 0, lo, num, dev(h, s, 0))
    for h, lo, num in halves:
        go_second(h, 0, lo, num)
    for h, lo, num in halves:
        pass_on(h, 0, 0, lo, num)
    yield
    if not relay:
        for s in shifts:
            for h, lo, num in halves:
                wait(first[h, s], h, -s, 0, lo, num)
                go_second(h, -s, lo, num)
                pass_on(h, -s, 0, lo, num)
            yield
        if merge:
            wait_most(k_second, chips - place.side)
        for a in (0, -1, 1, -2):
            for s in shifts:
                for h, lo, num in halves:
                    if not merge:
                        wait(second[h, a, s], h, a, -s, lo, num)
                    pass_on(h, a, -s, lo, num)
            yield
    else:
        def relay_on(kr, h, a, b, lo, s, ta, tb):
            part = lo + (s == -1)
            return send(h, a, b, part, 1, dev(h, ta, tb), kr)

        for s in shifts:
            for h, lo, num in halves:
                wait(first[h, s], h, -s, 0, lo, num)
                rel1[h] = relay_on(rel1.get(h), h, -s, 0, lo, s, s, 0)
                go_second(h, -s, lo, num)
                pass_on(h, -s, 0, lo, num)
            yield

        def relay2(h, lo, num, a, s):
            wait(second[h, a, s], h, a, -s, lo, num)
            rel2[h, a] = relay_on(rel2.get((h, a)), h, a, -s, lo, s, 0, s)
            pass_on(h, a, -s, lo, num)

        for h, lo, num in halves:
            for s in shifts:
                relay2(h, lo, num, 0, s)
        yield
        for h, lo, num in halves:
            wait(rel1[h], h, 2, 0, lo, num)
            go_second(h, 2, lo, num)
            pass_on(h, 2, 0, lo, num)
        yield
        for a in (-1, 1, 2):
            for s in shifts:
                for h, lo, num in halves:
                    relay2(h, lo, num, a, s)
            yield
        for a in (0, -1, 1, 2):
            for h, lo, num in halves:
                wait(rel2[h, a], h, a, 2, lo, num)
                pass_on(h, a, 2, lo, num)
            yield
    wait_most(k_pass, chips)
    yield
    sems.copy(most(2 * chips - 1), most(2 * chips - 1), ks, k_pass, partner).wait_send()
    yield


def finish(*gens):
    gens = list(gens)
    while gens:
        gens = [g for g in gens if next(g, gens) is not gens]


NN = (((1,), (0,)), ((), ()))
NT = (((1,), (1,)), ((), ()))
TN = (((0,), (0,)), ((), ()))
EXACT = lax.Precision.HIGHEST


def mm(a, b, dims=NN, precision=None):
    return lax.dot_general(a, b, dims, precision=precision, preferred_element_type=F32)


def three(v):
    a = v.astype(BF16)
    v = v - a.astype(F32)
    b = v.astype(BF16)
    return a, b, (v - b.astype(F32)).astype(BF16)


def iota(shape, dim):
    return lax.broadcasted_iota(jnp.int32, shape, dim)


def inv_rms(v):
    return lax.rsqrt(jnp.mean(v * v, axis=-1, keepdims=True) + NORM_EPS)


def rms_back(v, inv, g):
    return inv * g - v * (inv * inv * inv * jnp.mean(g * v, axis=-1, keepdims=True))


def turn(place, dest_core, d1, d2):
    along_x = dest_core == 0
    return jnp.where(along_x, d2, d1), jnp.where(along_x, d1, d2)


def block_offset(i, place):
    side = place.side
    d1, dc = i // (2 * side), lax.rem(i // side, 2)
    d2 = lax.rem(i // 2, 2) + 2 * lax.rem(i, 2)
    dy, dx = turn(place, lax.rem(place.core + dc, 2), d1, d2)
    return dy, dx, dc


def layer_kernel(group, experts, cap, x_ref, idst_ref, dy_ref, wq_ref, wk_ref, wv_ref, wo_ref, wr_ref, wg_in, wu_in, wd_in,
                 y_ref, gx_ref, gg_ref, gu_ref, gd_ref,
                 w_full, u_all, dy_all, ids_all, g_all, m_s, r_s, pick_s, ru_s, rdy_s, ag_s, au_s, mid_s, dag_s, dau_s,
                 wg_ref, wu_ref, wd_ref, relay, sums, total, small, smalls, prob_s, q_s, k_s, v_s, o_s, hid_s, place_s, gg_s, gu_s, gd_s, y_s,
                 lsem, ssem, rsem):
    place = Place(group)
    me = place.me
    toks, d_model = x_ref.shape
    choices = idst_ref.shape[0]
    local, _, ff = wg_in.shape
    depth = wq_ref.shape[0]
    per = 2 * place.side
    groups = group // per
    sems = Sems(ssem, rsem)

    def rows_of(d):
        return pl.ds(pl.multiple_of(d * depth, depth), depth)

    own_w = [pltpu.make_async_copy(w, w_full.at[i, rows_of(me)], lsem.at[i]) for i, w in enumerate((wq_ref, wk_ref, wv_ref, wo_ref))]
    experts_in = [pltpu.make_async_copy(src, dst, lsem.at[4 + i])
                  for i, (src, dst) in enumerate(((wg_in, wg_ref), (wu_in, wu_ref), (wd_in, wd_ref)))]
    for copy in own_w + experts_in:
        copy.start()
    sem = pltpu.get_barrier_semaphore()
    peers = near_peers(place)
    for peer in peers:
        pl.semaphore_signal(sem, inc=1, device_id={AXIS: peer}, device_id_type=pl.DeviceIdType.MESH)

    dy_all[me] = dy_ref[...]
    idst = idst_ref[...].astype(F32)
    ids_all[me] = idst
    lane_e = iota((2 * experts, toks), 0).astype(F32)
    chosen_t = jnp.zeros((2 * experts, toks), F32)
    for j in range(choices):
        chosen_t += jnp.where(idst[j:j + 1, :] == lane_e, 1.0, 0.0)
    chosen = jnp.transpose(chosen_t)[:, :experts]
    before = (iota((toks, toks), 0) > iota((toks, toks), 1)).astype(F32).astype(BF16)
    x = x_ref[...].astype(F32)
    x_inv = inv_rms(x)
    a = (x * x_inv).astype(BF16)

    for copy in own_w:
        copy.wait()
    pl.semaphore_wait(sem, len(peers))
    quarter = toks // 4
    two = ((0, 0, 2), (1, 2, 2))
    w_steps = gather_steps(place, sems, lambda d, lo, num: w_full.at[pl.ds(lo, num), rows_of(d)],
                           lambda n: w_full.at[:, pl.ds(0, n * depth)], False, two)
    ids_steps = gather_steps(place, sems, lambda d, lo, num: ids_all.at[d], lambda n: ids_all.at[pl.ds(0, n)], False, ((0, 0, 1),), True)
    dy_steps = gather_steps(place, sems, lambda d, lo, num: dy_all.at[d, pl.ds(lo * quarter, num * quarter)],
                            lambda n: dy_all.at[pl.ds(0, n)], True, two)
    for _ in range(4):
        next(w_steps)
    next(dy_steps)
    finish(w_steps)
    next(ids_steps)

    q_s[...] = mm(a, w_full[0]).astype(BF16)
    k_s[...] = mm(a, w_full[1]).astype(BF16)
    v_s[...] = mm(a, w_full[2]).astype(BF16)
    next(dy_steps, None)
    causal = iota((toks, toks), 0) >= iota((toks, toks), 1)
    low = iota((toks, 2 * HEAD_DIM), 1) < HEAD_DIM
    zero_b = jnp.zeros((toks, 2 * HEAD_DIM), BF16)
    pairs = d_model // (2 * HEAD_DIM)
    scale = HEAD_DIM ** -0.5

    def half(v, side):
        return jnp.where(low, v, zero_b) if side == 0 else jnp.where(low, zero_b, v)

    for pair in range(pairs):
        lanes = pl.ds(pair * 2 * HEAD_DIM, 2 * HEAD_DIM)
        qp, kp, vp = q_s[:, lanes], k_s[:, lanes], v_s[:, lanes]
        outs = []
        for hf in range(2):
            s = jnp.where(causal, mm(half(qp, hf), kp, NT) * scale, -1e30)
            e = jnp.exp(s - jnp.max(s, axis=-1, keepdims=True))
            p = e / jnp.sum(e, axis=-1, keepdims=True)
            prob_s[2 * pair + hf] = p
            outs.append(mm(p.astype(BF16), vp))
        o_s[:, lanes] = jnp.where(low, outs[0], outs[1]).astype(BF16)
        if pair >= 2:
            next(dy_steps, None)
        next(ids_steps, None)

    hid = (x + mm(o_s[...], w_full[3])).astype(BF16)
    hid_s[...] = hid
    h = hid.astype(F32)
    h_inv = inv_rms(h)
    n = h * h_inv
    u_all[me] = n.astype(BF16)
    logits = mm(n, wr_ref[...], NT, EXACT)
    top = jnp.max(jnp.where(chosen > 0.0, logits, -3e38), axis=-1, keepdims=True)
    expd = jnp.where(chosen > 0.0, jnp.exp(logits - top), 0.0)
    gates = expd / jnp.sum(expd, axis=-1, keepdims=True)
    gates_t = jnp.transpose(jnp.concatenate([gates, jnp.zeros_like(gates)], axis=-1))
    for j in range(choices):
        g_all[me, j:j + 1, :] = jnp.sum(jnp.where(idst[j:j + 1, :] == lane_e, gates_t, 0.0), axis=0, keepdims=True)

    u_steps = gather_steps(place, sems, lambda d, lo, num: u_all.at[d, pl.ds(lo * quarter, num * quarter)],
                           lambda n: u_all.at[pl.ds(0, n)], True, two)
    g_steps = gather_steps(place, sems, lambda d, lo, num: g_all.at[d], lambda n: g_all.at[pl.ds(0, n)], False, ((0, 0, 1),), True)
    next(u_steps)
    next(g_steps)
    finish(ids_steps)

    first_e = (me * local).astype(F32)
    row8 = iota((8, toks), 0)

    def find(i, _):
        ids = ids_all[place.at(*block_offset(i, place))]
        m = jnp.zeros((8, toks), F32)
        for e in range(local):
            hit = jnp.sum(jnp.where(ids == first_e + e, 1.0, 0.0), axis=0, keepdims=True)
            m = jnp.where(row8 == e, hit, m)
        m_s[i] = m
        return 0

    lax.fori_loop(0, group, find, 0)
    next(u_steps)
    next(dy_steps, None)
    m_flat = m_s[...].reshape(group * 8, toks)
    after = (iota((toks, toks), 0) < iota((toks, toks), 1)).astype(F32).astype(BF16)
    r_flat = jnp.where(m_flat > 0.0, mm(m_flat.astype(BF16), after), -1.0)
    r_s[...] = r_flat.reshape(group, 8, toks)
    next(u_steps)
    next(dy_steps, None)
    next(g_steps, None)
    slot = iota((cap, toks), 0).astype(F32)

    def build(i, _):
        r = r_s[i]
        for e in range(local):
            pick_s[i, pl.ds(e * cap, cap), :] = jnp.where(slot == r[e:e + 1, :], 1.0, 0.0).astype(BF16)
        return 0

    lax.fori_loop(0, group, build, 0)

    def take_rows(i, source, dest):
        rows = mm(pick_s[i], source[place.at(*block_offset(i, place))]).astype(BF16)
        for e in range(local):
            at = i * cap
            dest[e, pl.ds(pl.multiple_of(at, cap), cap), :] = rows[e * cap:(e + 1) * cap]

    def take_dy(g, _):
        for b in range(per):
            take_rows(g * per + b, dy_all, rdy_s)
        return 0

    while next(u_steps, place) is None:
        next(dy_steps, None)
        next(g_steps, None)
    for copy in experts_in:
        copy.wait()

    span = per * cap
    side = place.side
    both = local * cap
    k_first, k_second, k_small = sems.new_recv(4), sems.new_recv(2), sems.new_recv()
    k_rows, k_sums, k_smalls = [sems.new_send() for _ in range(2)], [sems.new_send() for _ in range(2)], sems.new_send()

    def first_hop(part, d1, dc, p):
        core = lax.rem(place.core + dc, 2)
        relay_dc = (dc + p) % 2
        src = u_all.at[pl.ds(d1 * per + dc * side + 2 * p, 2), pl.ds(part * both, both)]
        return sems.copy(src, relay.at[part, p, :, 2 * d1 + relay_dc], k_rows[part], k_first + 2 * part + p,
                         place.at(*turn(place, core, d1, 0), relay_dc))

    def first_done(part, p):
        at = relay.at[part, p, :, pl.ds(1, per - 1)]
        return sems.copy(at, at, k_rows[part], k_first + 2 * part + p, me)

    def dest_of(p, j):
        core = lax.rem(place.core + p, 2)
        return place.at(*turn(place, core, 0, p + 2 * j), p)

    def second_hop(part, p, j):
        return sems.copy(sums.at[part, 2 * j + p - 1], total.at[part, 2 * j + p], k_sums[part], k_second + part, dest_of(p, j))

    def small_hop(p, j):
        return sems.copy(small.at[2 * j + p - 1], smalls.at[2 * j + p], k_smalls, k_small, dest_of(p, j))

    def put(part, e, g, rows):
        for b in range(per):
            u_all[g * per + b, pl.ds(part * both + e * cap, cap), :] = rows[b * cap:(b + 1) * cap]

    def start_group(part, g):
        @pl.when(g > 0)
        def _():
            for dc in range(2):
                for p in range(2):
                    first_hop(part, g, dc, p).start()

        @pl.when(g == 0)
        def _():
            for p in range(2):
                first_hop(part, 0, 1 - p, p).start()
                for j in range(2):
                    relay[part, p, j, 0] = u_all[p * side + 2 * p + j, pl.ds(part * both, both), :]

    def take_u(g, _):
        for b in range(per):
            take_rows(g * per + b, u_all, ru_s)
        return 0

    lax.fori_loop(0, groups, take_u, 0)

    def forward(step, _):
        g = lax.rem(step + side // 2, side)
        rows = pl.ds(pl.multiple_of(g * span, span), span)
        for e in range(local):
            ru = ru_s[e, rows, :]
            ag = mm(ru, wg_ref[e])
            au = mm(ru, wu_ref[e])
            mid = (ag * jax.nn.sigmoid(ag) * au).astype(BF16)
            ag_s[e, rows, :] = ag
            au_s[e, rows, :] = au
            mid_s[e, rows, :] = mid
            put(0, e, g, mm(mid, wd_ref[e]).astype(BF16))
        start_group(0, g)
        return 0

    lax.fori_loop(0, groups, forward, 0)

    def weigh(q, _):
        for i in [q * side + b for b in range(side)]:
            d = place.at(*block_offset(i, place))
            ids, gts = ids_all[d], g_all[d]
            for e in range(local):
                gate = jnp.sum(jnp.where(ids == first_e + e, gts, 0.0), axis=0, keepdims=True)
                col = jnp.sum(pick_s[i, pl.ds(e * cap, cap), :].astype(F32) * gate, axis=-1, keepdims=True)
                at = pl.ds(pl.multiple_of(i * cap, cap), cap)
                rdy_s[e, at, :] = (col * rdy_s[e, at, :].astype(F32)).astype(BF16)
        return 0

    finish(g_steps, dy_steps)
    lax.fori_loop(0, groups, take_dy, 0)
    lax.fori_loop(0, group // side, weigh, 0)

    def backward(step, _):
        g = lax.rem(step + side // 2, side)
        rows = pl.ds(pl.multiple_of(g * span, span), span)
        for e in range(local):
            gm = mm(rdy_s[e, rows, :], wd_ref[e], NT)
            ag, au = ag_s[e, rows, :], au_s[e, rows, :]
            sg = jax.nn.sigmoid(ag)
            dag = (gm * au * sg * (1.0 + ag * (1.0 - sg))).astype(BF16)
            dau = (gm * ag * sg).astype(BF16)
            dag_s[e, rows, :] = dag
            dau_s[e, rows, :] = dau
            put(1, e, g, (mm(dag, wg_ref[e], NT) + mm(dau, wu_ref[e], NT)).astype(BF16))
        start_group(1, g)
        return 0

    lax.fori_loop(0, groups, backward, 0)

    def weights(e, _):
        gd_s[e] = mm(mid_s[e], rdy_s[e], TN).astype(BF16)
        gg_s[e] = mm(ru_s[e], dag_s[e], TN).astype(BF16)
        gu_s[e] = mm(ru_s[e], dau_s[e], TN).astype(BF16)
        return 0

    lax.fori_loop(0, local, weights, 0)
    grads_out = [pltpu.make_async_copy(src, dst, lsem.at[i])
                 for i, (src, dst) in enumerate(((gg_s, gg_ref), (gu_s, gu_ref), (gd_s, gd_ref), (y_s, y_ref)))]
    for copy in grads_out[:3]:
        copy.start()

    wide = per * both
    blocks = wide // cap
    col = iota((1, wide), 1)
    colmod = col
    for _ in range(1, blocks):
        colmod = jnp.where(colmod >= cap, colmod - cap, colmod)
    colmod = colmod.astype(F32)
    e_row = iota((experts, wide), 0).astype(F32)
    blk = iota((blocks, wide), 0) * cap
    blk_col = iota((blocks, wide), 1)
    block_of = jnp.where((blk_col >= blk) & (blk_col < blk + cap), 1.0, 0.0).astype(BF16)

    def owner_at(core, p, d1, dc, d2, e):
        dy, dx = turn(place, core, -d1, -d2)
        return (place.at(dy, dx, p + dc) * local + e).astype(F32)

    def relay_z(q, _):
        p, j = q % 2, q // 2
        core = lax.rem(place.core + p, 2)
        dest = dest_of(p, j)
        owner = jnp.zeros((1, wide), F32)
        for b in range(blocks):
            s, e = b // local, b % local
            owner = jnp.where((col >= b * cap) & (col < (b + 1) * cap), owner_at(core, 0, s // 2, s % 2, 0, e), owner)
        spread = jnp.where(e_row == owner, 1.0, 0.0).astype(BF16)
        ids, gts = ids_all[dest], g_all[dest]
        e_in = iota((2 * experts, toks), 0)
        e_id = jnp.where(e_in >= experts, e_in - experts, e_in).astype(F32)
        both_t = jnp.zeros((2 * experts, toks), F32)
        for c in range(choices):
            both_t += jnp.where(ids[c:c + 1, :] == e_id, jnp.where(e_in >= experts, gts[c:c + 1, :], 1.0), 0.0)
        both_v = jnp.transpose(both_t)
        chose, weight = both_v[:, :experts], both_v[:, experts:]
        ranks = jnp.where(chose > 0.0, mm(before, chose.astype(BF16)), -1.0).astype(BF16)
        z = relay[0, p, j].reshape(wide, d_model)
        here = mm(ranks, spread) == colmod
        place_s[q] = jnp.where(here, 1.0, 0.0).astype(BF16)
        y_sum = jnp.zeros((toks, d_model), F32)
        for piece in three(weight):
            y_sum += mm(jnp.where(here, mm(piece, spread), 0.0).astype(BF16), z)
        gg_sum = jnp.zeros((blocks, toks), F32)
        for piece in three(jnp.where(here, mm(dy_all[dest], z, NT), 0.0)):
            gg_sum += mm(block_of, piece, NT)

        @pl.when(q == 0)
        def _():
            total[0, 0] = y_sum
            smalls[0] = gg_sum

        @pl.when(q > 0)
        def _():
            sums[0, q - 1] = y_sum
            small[q - 1] = gg_sum
            second_hop(0, p, j).start()
            small_hop(p, j).start()
        return 0

    for p in range(2):
        first_done(0, p).wait_recv()
    lax.fori_loop(0, side, lambda t, _: relay_z(lax.rem(t + 2, side), 0), 0)
    for p in range(2):
        first_done(1, p).wait_recv()

    def relay_d(q, _):
        p, j = q % 2, q // 2
        sums_d = mm(place_s[q], relay[1, p, j].reshape(wide, d_model))

        @pl.when(q == 0)
        def _():
            total[1, 0] = sums_d

        @pl.when(q > 0)
        def _():
            sums[1, q - 1] = sums_d
            second_hop(1, p, j).start()
        return 0

    lax.fori_loop(0, side, lambda t, _: relay_d(lax.rem(t + 2, side), 0), 0)

    rest = pl.ds(1, side - 1)
    sems.copy(total.at[0, rest], total.at[0, rest], k_sums[0], k_second, me).wait_recv()
    sems.copy(smalls.at[rest], smalls.at[rest], k_smalls, k_small, me).wait_recv()
    dyv = dy_ref[...]
    y_s[...] = (hid_s[...].astype(F32) + ((total[0, 0] + total[0, 1]) + (total[0, 2] + total[0, 3]))).astype(BF16)
    grads_out[3].start()
    m_col = iota((experts, 1), 0)
    owner = jnp.zeros((experts, 1), F32)
    for m in range(experts):
        d2, s, e = m // blocks, (m % blocks) // local, m % local
        owner = jnp.where(m_col == m, owner_at(place.core, d2 % 2, s // 2, s % 2, d2, e), owner)
    perm = jnp.where(owner == iota((experts, experts), 1).astype(F32), 1.0, 0.0).astype(BF16)
    g_gates = jnp.zeros((toks, experts), F32)
    for piece in three(smalls[...].reshape(experts, toks)):
        g_gates += mm(piece, perm, TN)
    g_logits = gates * (g_gates - jnp.sum(gates * g_gates, axis=-1, keepdims=True))
    g_hnorm = mm(g_logits, wr_ref[...], NN, EXACT)
    sems.copy(total.at[1, rest], total.at[1, rest], k_sums[1], k_second + 1, me).wait_recv()
    gn = g_hnorm + ((total[1, 0] + total[1, 1]) + (total[1, 2] + total[1, 3]))
    h = hid_s[...].astype(F32)
    h_inv = inv_rms(h)
    g_hid = (dyv.astype(F32) + rms_back(h, h_inv, gn)).astype(BF16)
    o_s[...] = mm(g_hid, w_full[3], NT).astype(BF16)
    g_xn = jnp.zeros((toks, d_model), F32)
    for pair in range(pairs):
        lanes = pl.ds(pair * 2 * HEAD_DIM, 2 * HEAD_DIM)
        qp, kp, vp, dop = q_s[:, lanes], k_s[:, lanes], v_s[:, lanes], o_s[:, lanes]
        dq, dk, dv = [], [], []
        for hf in range(2):
            p = prob_s[2 * pair + hf]
            dp = mm(half(dop, hf), vp, NT)
            ds = (p * (dp - jnp.sum(dp * p, axis=-1, keepdims=True)) * scale).astype(BF16)
            dq.append(mm(ds, kp))
            dk.append(mm(ds, qp, TN))
            dv.append(mm(p.astype(BF16), dop, TN))
        for i, parts in enumerate((dq, dk, dv)):
            grad = jnp.where(low, parts[0], parts[1]).astype(BF16)
            g_xn += mm(grad, w_full[i, :, lanes], NT)
    x = x_ref[...].astype(F32)
    gx_ref[...] = (g_hid.astype(F32) + rms_back(x, inv_rms(x), g_xn)).astype(BF16)

    for copy in grads_out:
        copy.wait()
    for part in range(2):
        at = relay.at[part, :, :, pl.ds(1, per - 1)]
        sems.copy(at, at, k_rows[part], k_first, me).wait_send()
        sems.copy(sums.at[part], sums.at[part], k_sums[part], k_second, me).wait_send()
    sems.copy(small, small, k_smalls, k_small, me).wait_send()
    assert (sems.n_send, sems.n_recv) == (N_SEND, N_RECV), (sems.n_send, sems.n_recv)


def settle_kernel(*refs):
    n = (len(refs) - 2) // 3
    ins, outs, held, lsem, ssem = refs[:n], refs[n:2 * n], refs[2 * n:3 * n], refs[-2], refs[-1]
    loads = [pltpu.make_async_copy(a, h, lsem.at[i]) for i, (a, h) in enumerate(zip(ins, held))]
    stores = [pltpu.make_async_copy(h, o, ssem.at[i]) for i, (h, o) in enumerate(zip(held, outs))]
    for copy in loads:
        copy.start()
    for load, store in zip(loads, stores):
        load.wait()
        store.start()
    for copy in stores:
        copy.wait()


def settle(*arrays):
    n = len(arrays)
    hbm = pl.BlockSpec(memory_space=pl.ANY)
    return pl.pallas_call(
        settle_kernel, out_shape=[jax.ShapeDtypeStruct(a.shape, a.dtype) for a in arrays],
        in_specs=[hbm] * n, out_specs=[hbm] * n,
        scratch_shapes=[pltpu.VMEM(a.shape, a.dtype) for a in arrays] + [pltpu.SemaphoreType.DMA((n,))] * 2,
        name='settle')(*arrays)


def solution(mesh):
    group = mesh.shape[AXIS]
    tok_spec = P(('dp', 'ep'), None)
    fsdp_spec = P('ep', None)
    expert_spec = P('ep', None, None)
    grad_spec = P(('dp', 'ep'), None, None)

    def device_step(x_tokens, expert_ids, grad_y, w_q, w_k, w_v, w_o, w_router, w_gate, w_up, w_down):
        toks, d_model = x_tokens.shape
        choices = expert_ids.shape[1]
        experts = w_router.shape[1]
        local, _, ff = w_gate.shape
        avg_load = toks * choices // experts
        cap = avg_load + avg_load // 2
        assert toks == SEQ_LEN
        heads = w_q.shape[1] // HEAD_DIM
        shape, vm = jax.ShapeDtypeStruct, pltpu.VMEM
        rows = group * cap
        side = math.isqrt(group // 2)
        per = 2 * side
        assert local == 2
        in_vmem = pl.BlockSpec(memory_space=pltpu.VMEM)
        in_hbm = pl.BlockSpec(memory_space=pl.ANY)
        square = vm((toks, d_model), BF16)
        outs = pl.pallas_call(
            functools.partial(layer_kernel, group, experts, cap),
            out_shape=[shape(x_tokens.shape, BF16), shape(x_tokens.shape, BF16), shape(w_gate.shape, BF16),
                       shape(w_up.shape, BF16), shape(w_down.shape, BF16)],
            in_specs=[in_vmem] * 3 + [in_hbm] * 4 + [in_vmem] + [in_hbm] * 3,
            out_specs=[in_hbm, in_vmem] + [in_hbm] * 3,
            scratch_shapes=[
                vm((4, group * w_q.shape[0], d_model), BF16), vm((group, toks, d_model), BF16), vm((group, toks, d_model), BF16),
                vm((group, choices, toks), F32), vm((group, choices, toks), F32), vm((group, 8, toks), F32), vm((group, 8, toks), F32),
                vm((group, local * cap, toks), BF16), vm((local, rows, d_model), BF16), vm((local, rows, d_model), BF16),
                vm((local, rows, ff), F32), vm((local, rows, ff), F32),
                vm((local, rows, ff), BF16), vm((local, rows, ff), BF16), vm((local, rows, ff), BF16),
                vm(w_gate.shape, BF16), vm(w_up.shape, BF16), vm(w_down.shape, BF16), vm((2, 2, 2, per, local * cap, d_model), BF16),
                vm((2, side - 1, toks, d_model), F32), vm((2, side, toks, d_model), F32),
                vm((side - 1, experts // side, toks), F32), vm((side, experts // side, toks), F32),
                vm((heads, toks, toks), F32), square, square, square, square, square,
                vm((group // per, toks, per * local * cap), BF16),
                vm(w_gate.shape, BF16), vm(w_up.shape, BF16), vm(w_down.shape, BF16), square,
                pltpu.SemaphoreType.DMA((7,)), pltpu.SemaphoreType.DMA((N_SEND,)), pltpu.SemaphoreType.DMA((N_RECV,))],
            compiler_params=pltpu.CompilerParams(collective_id=1, has_side_effects=True, vmem_limit_bytes=67043328),
            name='layer')(x_tokens, expert_ids.T, grad_y, w_q, w_k, w_v, w_o, w_router.T, w_gate, w_up, w_down)
        return settle(*outs)

    return jax.shard_map(
        device_step, mesh=mesh,
        in_specs=(tok_spec, tok_spec, tok_spec, fsdp_spec, fsdp_spec, fsdp_spec, fsdp_spec,
                  P(None, None), expert_spec, expert_spec, expert_spec),
        out_specs=(tok_spec, tok_spec, grad_spec, grad_spec, grad_spec),
        check_vma=False)
```

```python
import functools
import math

import jax
import jax.numpy as jnp
from jax import lax
from jax.experimental import pallas as pl
from jax.experimental.pallas import tpu as pltpu
from jax.sharding import PartitionSpec as P

NORM_EPS = 1e-6
SEQ_LEN = 256
HEAD_DIM = 64
AXIS = 'ep'
N_SEND = 10
N_RECV = 110
F32 = jnp.float32
BF16 = jnp.bfloat16


class Place:
    def __init__(self, group):
        self.group = group
        self.side = math.isqrt(group // 2)
        self.me = lax.axis_index(AXIS)
        self.core = lax.rem(self.me, 2)
        self.x = lax.rem(self.me // 2, self.side)
        self.y = self.me // (2 * self.side)

    def wrap(self, v):
        return lax.rem(v + self.side, self.side)

    def at(self, dy, dx, dc=0):
        return (self.wrap(self.y + dy) * self.side + self.wrap(self.x + dx)) * 2 + lax.rem(self.core + dc, 2)


def near_peers(pl_):
    return [pl_.at(0, 1), pl_.at(0, -1), pl_.at(1, 0), pl_.at(-1, 0), pl_.at(0, 2), pl_.at(2, 0), pl_.at(0, 0, 1)]


class Sems:
    def __init__(self, ssem, rsem):
        self.ssem, self.rsem, self.n_send, self.n_recv = ssem, rsem, 0, 0

    def new_send(self):
        self.n_send += 1
        return self.n_send - 1

    def new_recv(self, count=1):
        self.n_recv += count
        return self.n_recv - count

    def copy(self, src, dst, ks, kr, target):
        return pltpu.make_async_remote_copy(
            src_ref=src, dst_ref=dst, send_sem=self.ssem.at[ks], recv_sem=self.rsem.at[kr],
            device_id={AXIS: target}, device_id_type=pl.DeviceIdType.MESH)


def gather_steps(place, sems, region, most, relay, halves, merge=False):
    partner = place.at(0, 0, 1)
    chips = place.side * place.side
    ks, k_pass = sems.new_send(), sems.new_recv()
    k_second = sems.new_recv() if merge else None

    def dev(h, a, b, dc=0):
        return place.at(b, a, dc) if h == 0 else place.at(a, b, dc)

    def send(h, a, b, lo, num, target, kr=None):
        where = region(dev(h, a, b), lo, num)
        kr = sems.new_recv() if kr is None else kr
        sems.copy(where, where, ks, kr, target).start()
        return kr

    def wait(kr, h, a, b, lo, num):
        where = region(dev(h, a, b), lo, num)
        sems.copy(where, where, ks, kr, partner).wait_recv()

    def wait_most(kr, n):
        sems.copy(most(n), most(n), ks, kr, partner).wait_recv()

    def pass_on(h, a, b, lo, num):
        send(h, a, b, lo, num, partner, k_pass)

    first, second, rel1, rel2 = {}, {}, {}, {}
    shifts = (1, -1) if relay else (1, -1, 2)

    def go_second(h, a, lo, num):
        for s in shifts:
            second[h, a, s] = send(h, a, 0, lo, num, dev(h, 0, s), k_second)

    for h, lo, num in halves:
        for s in shifts:
            first[h, s] = send(h, 0, 0, lo, num, dev(h, s, 0))
    for h, lo, num in halves:
        go_second(h, 0, lo, num)
    for h, lo, num in halves:
        pass_on(h, 0, 0, lo, num)
    yield
    if not relay:
        for s in shifts:
            for h, lo, num in halves:
                wait(first[h, s], h, -s, 0, lo, num)
                go_second(h, -s, lo, num)
                pass_on(h, -s, 0, lo, num)
            yield
        if merge:
            wait_most(k_second, chips - place.side)
        for a in (0, -1, 1, -2):
            for s in shifts:
                for h, lo, num in halves:
                    if not merge:
                        wait(second[h, a, s], h, a, -s, lo, num)
                    pass_on(h, a, -s, lo, num)
            yield
    else:
        def relay_on(kr, h, a, b, lo, s, ta, tb):
            part = lo + (s == -1)
            return send(h, a, b, part, 1, dev(h, ta, tb), kr)

        for s in shifts:
            for h, lo, num in halves:
                wait(first[h, s], h, -s, 0, lo, num)
                rel1[h] = relay_on(rel1.get(h), h, -s, 0, lo, s, s, 0)
                go_second(h, -s, lo, num)
                pass_on(h, -s, 0, lo, num)
            yield

        def relay2(h, lo, num, a, s):
            wait(second[h, a, s], h, a, -s, lo, num)
            rel2[h, a] = relay_on(rel2.get((h, a)), h, a, -s, lo, s, 0, s)
            pass_on(h, a, -s, lo, num)

        for h, lo, num in halves:
            for s in shifts:
                relay2(h, lo, num, 0, s)
        yield
        for h, lo, num in halves:
            wait(rel1[h], h, 2, 0, lo, num)
            go_second(h, 2, lo, num)
            pass_on(h, 2, 0, lo, num)
        yield
        for a in (-1, 1, 2):
            for s in shifts:
                for h, lo, num in halves:
                    relay2(h, lo, num, a, s)
            yield
        for a in (0, -1, 1, 2):
            for h, lo, num in halves:
                wait(rel2[h, a], h, a, 2, lo, num)
                pass_on(h, a, 2, lo, num)
            yield
    wait_most(k_pass, chips)
    yield
    sems.copy(most(2 * chips - 1), most(2 * chips - 1), ks, k_pass, partner).wait_send()
    yield


def finish(*gens):
    gens = list(gens)
    while gens:
        gens = [g for g in gens if next(g, gens) is not gens]


NN = (((1,), (0,)), ((), ()))
NT = (((1,), (1,)), ((), ()))
TN = (((0,), (0,)), ((), ()))
EXACT = lax.Precision.HIGHEST


def mm(a, b, dims=NN, precision=None):
    return lax.dot_general(a, b, dims, precision=precision, preferred_element_type=F32)


def three(v):
    a = v.astype(BF16)
    v = v - a.astype(F32)
    b = v.astype(BF16)
    return a, b, (v - b.astype(F32)).astype(BF16)


def iota(shape, dim):
    return lax.broadcasted_iota(jnp.int32, shape, dim)


def inv_rms(v):
    return lax.rsqrt(jnp.mean(v * v, axis=-1, keepdims=True) + NORM_EPS)


def rms_back(v, inv, g):
    return inv * g - v * (inv * inv * inv * jnp.mean(g * v, axis=-1, keepdims=True))


def turn(place, dest_core, d1, d2):
    along_x = dest_core == 0
    return jnp.where(along_x, d2, d1), jnp.where(along_x, d1, d2)


def block_offset(i, place):
    side = place.side
    d1, dc = i // (2 * side), lax.rem(i // side, 2)
    d2 = lax.rem(i // 2, 2) + 2 * lax.rem(i, 2)
    dy, dx = turn(place, lax.rem(place.core + dc, 2), d1, d2)
    return dy, dx, dc


def layer_kernel(group, experts, cap, x_ref, idst_ref, dy_ref, wq_ref, wk_ref, wv_ref, wo_ref, wr_ref, wg_in, wu_in, wd_in,
                 y_ref, gx_ref, gg_ref, gu_ref, gd_ref,
                 w_full, u_all, dy_all, ids_all, g_all, m_s, r_s, pick_s, ru_s, rdy_s, ag_s, au_s, mid_s, dag_s, dau_s,
                 wg_ref, wu_ref, wd_ref, relay, sums, total, small, smalls, prob_s, q_s, k_s, v_s, o_s, hid_s, place_s, gg_s, gu_s, gd_s, y_s,
                 lsem, ssem, rsem):
    place = Place(group)
    me = place.me
    toks, d_model = x_ref.shape
    choices = idst_ref.shape[0]
    local, _, ff = wg_in.shape
    depth = wq_ref.shape[0]
    per = 2 * place.side
    groups = group // per
    sems = Sems(ssem, rsem)

    def rows_of(d):
        return pl.ds(pl.multiple_of(d * depth, depth), depth)

    own_w = [pltpu.make_async_copy(w, w_full.at[i, rows_of(me)], lsem.at[i]) for i, w in enumerate((wq_ref, wk_ref, wv_ref, wo_ref))]
    experts_in = [pltpu.make_async_copy(src, dst, lsem.at[4 + i])
                  for i, (src, dst) in enumerate(((wg_in, wg_ref), (wu_in, wu_ref), (wd_in, wd_ref)))]
    for copy in own_w + experts_in:
        copy.start()
    sem = pltpu.get_barrier_semaphore()
    peers = near_peers(place)
    for peer in peers:
        pl.semaphore_signal(sem, inc=1, device_id={AXIS: peer}, device_id_type=pl.DeviceIdType.MESH)

    dy_all[me] = dy_ref[...]
    idst = idst_ref[...].astype(F32)
    ids_all[me] = idst
    lane_e = iota((2 * experts, toks), 0).astype(F32)
    chosen_t = jnp.zeros((2 * experts, toks), F32)
    for j in range(choices):
        chosen_t += jnp.where(idst[j:j + 1, :] == lane_e, 1.0, 0.0)
    chosen = jnp.transpose(chosen_t)[:, :experts]
    before = (iota((toks, toks), 0) > iota((toks, toks), 1)).astype(F32).astype(BF16)
    x = x_ref[...].astype(F32)
    x_inv = inv_rms(x)
    a = (x * x_inv).astype(BF16)

    for copy in own_w:
        copy.wait()
    pl.semaphore_wait(sem, len(peers))
    quarter = toks // 4
    two = ((0, 0, 2), (1, 2, 2))
    w_steps = gather_steps(place, sems, lambda d, lo, num: w_full.at[pl.ds(lo, num), rows_of(d)],
                           lambda n: w_full.at[:, pl.ds(0, n * depth)], False, two)
    ids_steps = gather_steps(place, sems, lambda d, lo, num: ids_all.at[d], lambda n: ids_all.at[pl.ds(0, n)], False, ((0, 0, 1),), True)
    dy_steps = gather_steps(place, sems, lambda d, lo, num: dy_all.at[d, pl.ds(lo * quarter, num * quarter)],
                            lambda n: dy_all.at[pl.ds(0, n)], True, two)
    next(w_steps)
    next(ids_steps)
    next(dy_steps)
    for _ in range(3):
        next(w_steps)
        next(ids_steps)
    next(dy_steps)
    next(dy_steps)
    finish(w_steps)
    next(ids_steps)

    q_s[...] = mm(a, w_full[0]).astype(BF16)
    k_s[...] = mm(a, w_full[1]).astype(BF16)
    v_s[...] = mm(a, w_full[2]).astype(BF16)
    next(dy_steps, None)
    causal = iota((toks, toks), 0) >= iota((toks, toks), 1)
    low = iota((toks, 2 * HEAD_DIM), 1) < HEAD_DIM
    zero_b = jnp.zeros((toks, 2 * HEAD_DIM), BF16)
    pairs = d_model // (2 * HEAD_DIM)
    scale = HEAD_DIM ** -0.5

    def half(v, side):
        return jnp.where(low, v, zero_b) if side == 0 else jnp.where(low, zero_b, v)

    for pair in range(pairs):
        lanes = pl.ds(pair * 2 * HEAD_DIM, 2 * HEAD_DIM)
        qp, kp, vp = q_s[:, lanes], k_s[:, lanes], v_s[:, lanes]
        outs = []
        for hf in range(2):
            s = jnp.where(causal, mm(half(qp, hf), kp, NT) * scale, -1e30)
            e = jnp.exp(s - jnp.max(s, axis=-1, keepdims=True))
            p = e / jnp.sum(e, axis=-1, keepdims=True)
            prob_s[2 * pair + hf] = p
            outs.append(mm(p.astype(BF16), vp))
        o_s[:, lanes] = jnp.where(low, outs[0], outs[1]).astype(BF16)
        if pair >= 3:
            next(dy_steps, None)

    hid = (x + mm(o_s[...], w_full[3])).astype(BF16)
    hid_s[...] = hid
    h = hid.astype(F32)
    h_inv = inv_rms(h)
    n = h * h_inv
    u_all[me] = n.astype(BF16)
    logits = mm(n, wr_ref[...], NT, EXACT)
    top = jnp.max(jnp.where(chosen > 0.0, logits, -3e38), axis=-1, keepdims=True)
    expd = jnp.where(chosen > 0.0, jnp.exp(logits - top), 0.0)
    gates = expd / jnp.sum(expd, axis=-1, keepdims=True)
    gates_t = jnp.transpose(jnp.concatenate([gates, jnp.zeros_like(gates)], axis=-1))
    for j in range(choices):
        g_all[me, j:j + 1, :] = jnp.sum(jnp.where(idst[j:j + 1, :] == lane_e, gates_t, 0.0), axis=0, keepdims=True)

    u_steps = gather_steps(place, sems, lambda d, lo, num: u_all.at[d, pl.ds(lo * quarter, num * quarter)],
                           lambda n: u_all.at[pl.ds(0, n)], True, two)
    g_steps = gather_steps(place, sems, lambda d, lo, num: g_all.at[d], lambda n: g_all.at[pl.ds(0, n)], False, ((0, 0, 1),), True)
    next(g_steps)
    next(u_steps)
    finish(ids_steps)

    first_e = (me * local).astype(F32)
    row8 = iota((8, toks), 0)

    def find(i, _):
        ids = ids_all[place.at(*block_offset(i, place))]
        m = jnp.zeros((8, toks), F32)
        for e in range(local):
            hit = jnp.sum(jnp.where(ids == first_e + e, 1.0, 0.0), axis=0, keepdims=True)
            m = jnp.where(row8 == e, hit, m)
        m_s[i] = m
        return 0

    lax.fori_loop(0, group, find, 0)
    next(u_steps)
    for _ in range(3):
        next(g_steps)
    next(dy_steps, None)
    next(dy_steps, None)
    m_flat = m_s[...].reshape(group * 8, toks)
    after = (iota((toks, toks), 0) < iota((toks, toks), 1)).astype(F32).astype(BF16)
    r_flat = jnp.where(m_flat > 0.0, mm(m_flat.astype(BF16), after), -1.0)
    r_s[...] = r_flat.reshape(group, 8, toks)
    next(u_steps)
    next(dy_steps, None)
    slot = iota((cap, toks), 0).astype(F32)

    def build(i, _):
        r = r_s[i]
        for e in range(local):
            pick_s[i, pl.ds(e * cap, cap), :] = jnp.where(slot == r[e:e + 1, :], 1.0, 0.0).astype(BF16)
        return 0

    lax.fori_loop(0, group, build, 0)

    def take_rows(i, source, dest):
        rows = mm(pick_s[i], source[place.at(*block_offset(i, place))]).astype(BF16)
        for e in range(local):
            at = i * cap
            dest[e, pl.ds(pl.multiple_of(at, cap), cap), :] = rows[e * cap:(e + 1) * cap]

    def take_dy(g, _):
        for b in range(per):
            take_rows(g * per + b, dy_all, rdy_s)
        return 0

    for _ in range(9):
        next(u_steps)
        next(dy_steps, None)
        next(dy_steps, None)
    for copy in experts_in:
        copy.wait()

    span = per * cap
    side = place.side
    both = local * cap
    k_first, k_second, k_small = sems.new_recv(4), sems.new_recv(2), sems.new_recv()
    k_rows, k_sums, k_smalls = [sems.new_send() for _ in range(2)], [sems.new_send() for _ in range(2)], sems.new_send()

    def first_hop(part, d1, dc, p):
        core = lax.rem(place.core + dc, 2)
        relay_dc = (dc + p) % 2
        src = u_all.at[pl.ds(d1 * per + dc * side + 2 * p, 2), pl.ds(part * both, both)]
        return sems.copy(src, relay.at[part, p, :, 2 * d1 + relay_dc], k_rows[part], k_first + 2 * part + p,
                         place.at(*turn(place, core, d1, 0), relay_dc))

    def first_done(part, p):
        at = relay.at[part, p, :, pl.ds(1, per - 1)]
        return sems.copy(at, at, k_rows[part], k_first + 2 * part + p, me)

    def dest_of(p, j):
        core = lax.rem(place.core + p, 2)
        return place.at(*turn(place, core, 0, p + 2 * j), p)

    def second_hop(part, p, j):
        return sems.copy(sums.at[part, 2 * j + p - 1], total.at[part, 2 * j + p], k_sums[part], k_second + part, dest_of(p, j))

    def small_hop(p, j):
        return sems.copy(small.at[2 * j + p - 1], smalls.at[2 * j + p], k_smalls, k_small, dest_of(p, j))

    def put(part, e, g, rows):
        for b in range(per):
            u_all[g * per + b, pl.ds(part * both + e * cap, cap), :] = rows[b * cap:(b + 1) * cap]

    def start_group(part, g):
        @pl.when(g > 0)
        def _():
            for dc in range(2):
                for p in range(2):
                    first_hop(part, g, dc, p).start()

        @pl.when(g == 0)
        def _():
            for p in range(2):
                first_hop(part, 0, 1 - p, p).start()
                for j in range(2):
                    relay[part, p, j, 0] = u_all[p * side + 2 * p + j, pl.ds(part * both, both), :]

    def take_u(dc):
        def body(g, _):
            for b in range(2):
                for d2 in range(side):
                    take_rows((2 * g + b) * per + dc * side + d2, u_all, ru_s)
            return 0
        lax.fori_loop(0, side // 2, body, 0)

    take_u(0)
    next(u_steps)
    next(dy_steps, None)
    take_u(1)
    finish(u_steps)

    def forward(step, _):
        g = lax.rem(step + side // 2, side)
        rows = pl.ds(pl.multiple_of(g * span, span), span)
        for e in range(local):
            ru = ru_s[e, rows, :]
            ag = mm(ru, wg_ref[e])
            au = mm(ru, wu_ref[e])
            mid = (ag * jax.nn.sigmoid(ag) * au).astype(BF16)
            ag_s[e, rows, :] = ag
            au_s[e, rows, :] = au
            mid_s[e, rows, :] = mid
            put(0, e, g, mm(mid, wd_ref[e]).astype(BF16))
        start_group(0, g)
        return 0

    lax.fori_loop(0, groups, forward, 0)

    def weigh(q, _):
        for i in [q * side + b for b in range(side)]:
            d = place.at(*block_offset(i, place))
            ids, gts = ids_all[d], g_all[d]
            for e in range(local):
                gate = jnp.sum(jnp.where(ids == first_e + e, gts, 0.0), axis=0, keepdims=True)
                col = jnp.sum(pick_s[i, pl.ds(e * cap, cap), :].astype(F32) * gate, axis=-1, keepdims=True)
                at = pl.ds(pl.multiple_of(i * cap, cap), cap)
                rdy_s[e, at, :] = (col * rdy_s[e, at, :].astype(F32)).astype(BF16)
        return 0

    finish(g_steps, dy_steps)
    lax.fori_loop(0, groups, take_dy, 0)
    lax.fori_loop(0, group // side, weigh, 0)

    def backward(step, _):
        g = lax.rem(step + side // 2, side)
        rows = pl.ds(pl.multiple_of(g * span, span), span)
        for e in range(local):
            gm = mm(rdy_s[e, rows, :], wd_ref[e], NT)
            ag, au = ag_s[e, rows, :], au_s[e, rows, :]
            sg = jax.nn.sigmoid(ag)
            dag = (gm * au * sg * (1.0 + ag * (1.0 - sg))).astype(BF16)
            dau = (gm * ag * sg).astype(BF16)
            dag_s[e, rows, :] = dag
            dau_s[e, rows, :] = dau
            put(1, e, g, (mm(dag, wg_ref[e], NT) + mm(dau, wu_ref[e], NT)).astype(BF16))
        start_group(1, g)
        return 0

    lax.fori_loop(0, groups, backward, 0)

    def weights(e, _):
        gd_s[e] = mm(mid_s[e], rdy_s[e], TN).astype(BF16)
        gg_s[e] = mm(ru_s[e], dag_s[e], TN).astype(BF16)
        gu_s[e] = mm(ru_s[e], dau_s[e], TN).astype(BF16)
        return 0

    lax.fori_loop(0, local, weights, 0)
    grads_out = [pltpu.make_async_copy(src, dst, lsem.at[i])
                 for i, (src, dst) in enumerate(((gg_s, gg_ref), (gu_s, gu_ref), (gd_s, gd_ref), (y_s, y_ref)))]
    for copy in grads_out[:3]:
        copy.start()

    wide = per * both
    blocks = wide // cap
    col = iota((1, wide), 1)
    colmod = col
    for _ in range(1, blocks):
        colmod = jnp.where(colmod >= cap, colmod - cap, colmod)
    colmod = colmod.astype(F32)
    e_row = iota((experts, wide), 0).astype(F32)
    blk = iota((blocks, wide), 0) * cap
    blk_col = iota((blocks, wide), 1)
    block_of = jnp.where((blk_col >= blk) & (blk_col < blk + cap), 1.0, 0.0).astype(BF16)

    def owner_at(core, p, d1, dc, d2, e):
        dy, dx = turn(place, core, -d1, -d2)
        return (place.at(dy, dx, p + dc) * local + e).astype(F32)

    def relay_z(q, _):
        p, j = q % 2, q // 2
        core = lax.rem(place.core + p, 2)
        dest = dest_of(p, j)
        owner = jnp.zeros((1, wide), F32)
        for b in range(blocks):
            s, e = b // local, b % local
            owner = jnp.where((col >= b * cap) & (col < (b + 1) * cap), owner_at(core, 0, s // 2, s % 2, 0, e), owner)
        spread = jnp.where(e_row == owner, 1.0, 0.0).astype(BF16)
        ids, gts = ids_all[dest], g_all[dest]
        e_in = iota((2 * experts, toks), 0)
        e_id = jnp.where(e_in >= experts, e_in - experts, e_in).astype(F32)
        both_t = jnp.zeros((2 * experts, toks), F32)
        for c in range(choices):
            both_t += jnp.where(ids[c:c + 1, :] == e_id, jnp.where(e_in >= experts, gts[c:c + 1, :], 1.0), 0.0)
        both_v = jnp.transpose(both_t)
        chose, weight = both_v[:, :experts], both_v[:, experts:]
        ranks = jnp.where(chose > 0.0, mm(before, chose.astype(BF16)), -1.0).astype(BF16)
        z = relay[0, p, j].reshape(wide, d_model)
        here = mm(ranks, spread) == colmod
        place_s[q] = jnp.where(here, 1.0, 0.0).astype(BF16)
        y_sum = jnp.zeros((toks, d_model), F32)
        for piece in three(weight):
            y_sum += mm(jnp.where(here, mm(piece, spread), 0.0).astype(BF16), z)
        gg_sum = jnp.zeros((blocks, toks), F32)
        for piece in three(jnp.where(here, mm(dy_all[dest], z, NT), 0.0)):
            gg_sum += mm(block_of, piece, NT)

        @pl.when(q == 0)
        def _():
            total[0, 0] = y_sum
            smalls[0] = gg_sum

        @pl.when(q > 0)
        def _():
            sums[0, q - 1] = y_sum
            small[q - 1] = gg_sum
            second_hop(0, p, j).start()
            small_hop(p, j).start()
        return 0

    for p in range(2):
        first_done(0, p).wait_recv()
    lax.fori_loop(0, side, lambda t, _: relay_z(lax.rem(t + 2, side), 0), 0)
    for p in range(2):
        first_done(1, p).wait_recv()

    def relay_d(q, _):
        p, j = q % 2, q // 2
        sums_d = mm(place_s[q], relay[1, p, j].reshape(wide, d_model))

        @pl.when(q == 0)
        def _():
            total[1, 0] = sums_d

        @pl.when(q > 0)
        def _():
            sums[1, q - 1] = sums_d
            second_hop(1, p, j).start()
        return 0

    lax.fori_loop(0, side, lambda t, _: relay_d(lax.rem(t + 2, side), 0), 0)

    rest = pl.ds(1, side - 1)
    sems.copy(total.at[0, rest], total.at[0, rest], k_sums[0], k_second, me).wait_recv()
    sems.copy(smalls.at[rest], smalls.at[rest], k_smalls, k_small, me).wait_recv()
    dyv = dy_ref[...]
    y_s[...] = (hid_s[...].astype(F32) + ((total[0, 0] + total[0, 1]) + (total[0, 2] + total[0, 3]))).astype(BF16)
    grads_out[3].start()
    m_col = iota((experts, 1), 0)
    owner = jnp.zeros((experts, 1), F32)
    for m in range(experts):
        d2, s, e = m // blocks, (m % blocks) // local, m % local
        owner = jnp.where(m_col == m, owner_at(place.core, d2 % 2, s // 2, s % 2, d2, e), owner)
    perm = jnp.where(owner == iota((experts, experts), 1).astype(F32), 1.0, 0.0).astype(BF16)
    g_gates = jnp.zeros((toks, experts), F32)
    for piece in three(smalls[...].reshape(experts, toks)):
        g_gates += mm(piece, perm, TN)
    g_logits = gates * (g_gates - jnp.sum(gates * g_gates, axis=-1, keepdims=True))
    g_hnorm = mm(g_logits, wr_ref[...], NN, EXACT)
    sems.copy(total.at[1, rest], total.at[1, rest], k_sums[1], k_second + 1, me).wait_recv()
    gn = g_hnorm + ((total[1, 0] + total[1, 1]) + (total[1, 2] + total[1, 3]))
    h = hid_s[...].astype(F32)
    h_inv = inv_rms(h)
    g_hid = (dyv.astype(F32) + rms_back(h, h_inv, gn)).astype(BF16)
    o_s[...] = mm(g_hid, w_full[3], NT).astype(BF16)
    g_xn = jnp.zeros((toks, d_model), F32)
    for pair in range(pairs):
        lanes = pl.ds(pair * 2 * HEAD_DIM, 2 * HEAD_DIM)
        qp, kp, vp, dop = q_s[:, lanes], k_s[:, lanes], v_s[:, lanes], o_s[:, lanes]
        dq, dk, dv = [], [], []
        for hf in range(2):
            p = prob_s[2 * pair + hf]
            dp = mm(half(dop, hf), vp, NT)
            ds = (p * (dp - jnp.sum(dp * p, axis=-1, keepdims=True)) * scale).astype(BF16)
            dq.append(mm(ds, kp))
            dk.append(mm(ds, qp, TN))
            dv.append(mm(p.astype(BF16), dop, TN))
        for i, parts in enumerate((dq, dk, dv)):
            grad = jnp.where(low, parts[0], parts[1]).astype(BF16)
            g_xn += mm(grad, w_full[i, :, lanes], NT)
    x = x_ref[...].astype(F32)
    gx_ref[...] = (g_hid.astype(F32) + rms_back(x, inv_rms(x), g_xn)).astype(BF16)

    for copy in grads_out:
        copy.wait()
    for part in range(2):
        at = relay.at[part, :, :, pl.ds(1, per - 1)]
        sems.copy(at, at, k_rows[part], k_first, me).wait_send()
        sems.copy(sums.at[part], sums.at[part], k_sums[part], k_second, me).wait_send()
    sems.copy(small, small, k_smalls, k_small, me).wait_send()
    assert (sems.n_send, sems.n_recv) == (N_SEND, N_RECV)


def settle_kernel(*refs):
    n = (len(refs) - 2) // 3
    ins, outs, held, lsem, ssem = refs[:n], refs[n:2 * n], refs[2 * n:3 * n], refs[-2], refs[-1]
    loads = [pltpu.make_async_copy(a, h, lsem.at[i]) for i, (a, h) in enumerate(zip(ins, held))]
    stores = [pltpu.make_async_copy(h, o, ssem.at[i]) for i, (h, o) in enumerate(zip(held, outs))]
    for copy in loads:
        copy.start()
    for load, store in zip(loads, stores):
        load.wait()
        store.start()
    for copy in stores:
        copy.wait()


def settle(*arrays):
    n = len(arrays)
    hbm = pl.BlockSpec(memory_space=pl.ANY)
    return pl.pallas_call(
        settle_kernel, out_shape=[jax.ShapeDtypeStruct(a.shape, a.dtype) for a in arrays],
        in_specs=[hbm] * n, out_specs=[hbm] * n,
        scratch_shapes=[pltpu.VMEM(a.shape, a.dtype) for a in arrays] + [pltpu.SemaphoreType.DMA((n,))] * 2,
        name='settle')(*arrays)


def solution(mesh):
    group = mesh.shape[AXIS]
    tok_spec = P(('dp', 'ep'), None)
    fsdp_spec = P('ep', None)
    expert_spec = P('ep', None, None)
    grad_spec = P(('dp', 'ep'), None, None)

    def device_step(x_tokens, expert_ids, grad_y, w_q, w_k, w_v, w_o, w_router, w_gate, w_up, w_down):
        toks, d_model = x_tokens.shape
        choices = expert_ids.shape[1]
        experts = w_router.shape[1]
        local, _, ff = w_gate.shape
        avg_load = toks * choices // experts
        cap = avg_load + avg_load // 2
        assert toks == SEQ_LEN
        heads = w_q.shape[1] // HEAD_DIM
        shape, vm = jax.ShapeDtypeStruct, pltpu.VMEM
        rows = group * cap
        side = math.isqrt(group // 2)
        per = 2 * side
        assert local == 2
        in_vmem = pl.BlockSpec(memory_space=pltpu.VMEM)
        in_hbm = pl.BlockSpec(memory_space=pl.ANY)
        square = vm((toks, d_model), BF16)
        outs = pl.pallas_call(
            functools.partial(layer_kernel, group, experts, cap),
            out_shape=[shape(x_tokens.shape, BF16), shape(x_tokens.shape, BF16), shape(w_gate.shape, BF16),
                       shape(w_up.shape, BF16), shape(w_down.shape, BF16)],
            in_specs=[in_vmem] * 3 + [in_hbm] * 4 + [in_vmem] + [in_hbm] * 3,
            out_specs=[in_hbm, in_vmem] + [in_hbm] * 3,
            scratch_shapes=[
                vm((4, group * w_q.shape[0], d_model), BF16), vm((group, toks, d_model), BF16), vm((group, toks, d_model), BF16),
                vm((group, choices, toks), F32), vm((group, choices, toks), F32), vm((group, 8, toks), F32), vm((group, 8, toks), F32),
                vm((group, local * cap, toks), BF16), vm((local, rows, d_model), BF16), vm((local, rows, d_model), BF16),
                vm((local, rows, ff), F32), vm((local, rows, ff), F32),
                vm((local, rows, ff), BF16), vm((local, rows, ff), BF16), vm((local, rows, ff), BF16),
                vm(w_gate.shape, BF16), vm(w_up.shape, BF16), vm(w_down.shape, BF16), vm((2, 2, 2, per, local * cap, d_model), BF16),
                vm((2, side - 1, toks, d_model), F32), vm((2, side, toks, d_model), F32),
                vm((side - 1, experts // side, toks), F32), vm((side, experts // side, toks), F32),
                vm((heads, toks, toks), F32), square, square, square, square, square,
                vm((group // per, toks, per * local * cap), BF16),
                vm(w_gate.shape, BF16), vm(w_up.shape, BF16), vm(w_down.shape, BF16), square,
                pltpu.SemaphoreType.DMA((7,)), pltpu.SemaphoreType.DMA((N_SEND,)), pltpu.SemaphoreType.DMA((N_RECV,))],
            compiler_params=pltpu.CompilerParams(collective_id=1, has_side_effects=True, vmem_limit_bytes=67043328),
            name='layer')(x_tokens, expert_ids.T, grad_y, w_q, w_k, w_v, w_o, w_router.T, w_gate, w_up, w_down)
        return settle(*outs)

    return jax.shard_map(
        device_step, mesh=mesh,
        in_specs=(tok_spec, tok_spec, tok_spec, fsdp_spec, fsdp_spec, fsdp_spec, fsdp_spec,
                  P(None, None), expert_spec, expert_spec, expert_spec),
        out_specs=(tok_spec, tok_spec, grad_spec, grad_spec, grad_spec),
        check_vma=False)
```

```python
import functools
import math

import jax
import jax.numpy as jnp
from jax import lax
from jax.experimental import pallas as pl
from jax.experimental.pallas import tpu as pltpu
from jax.sharding import PartitionSpec as P

NORM_EPS = 1e-6
SEQ_LEN = 256
HEAD_DIM = 64
AXIS = 'ep'
N_SEND = 10
N_RECV = 110
F32 = jnp.float32
BF16 = jnp.bfloat16


class Place:
    def __init__(self, group):
        self.group = group
        self.side = math.isqrt(group // 2)
        self.me = lax.axis_index(AXIS)
        self.core = lax.rem(self.me, 2)
        self.x = lax.rem(self.me // 2, self.side)
        self.y = self.me // (2 * self.side)

    def wrap(self, v):
        return lax.rem(v + self.side, self.side)

    def at(self, dy, dx, dc=0):
        return (self.wrap(self.y + dy) * self.side + self.wrap(self.x + dx)) * 2 + lax.rem(self.core + dc, 2)


def near_peers(pl_):
    return [pl_.at(0, 1), pl_.at(0, -1), pl_.at(1, 0), pl_.at(-1, 0), pl_.at(0, 2), pl_.at(2, 0), pl_.at(0, 0, 1)]


class Sems:
    def __init__(self, ssem, rsem):
        self.ssem, self.rsem, self.n_send, self.n_recv = ssem, rsem, 0, 0

    def new_send(self):
        self.n_send += 1
        return self.n_send - 1

    def new_recv(self, count=1):
        self.n_recv += count
        return self.n_recv - count

    def copy(self, src, dst, ks, kr, target):
        return pltpu.make_async_remote_copy(
            src_ref=src, dst_ref=dst, send_sem=self.ssem.at[ks], recv_sem=self.rsem.at[kr],
            device_id={AXIS: target}, device_id_type=pl.DeviceIdType.MESH)


def gather_steps(place, sems, region, most, relay, halves, merge=False):
    partner = place.at(0, 0, 1)
    chips = place.side * place.side
    ks, k_pass = sems.new_send(), sems.new_recv()
    k_second = sems.new_recv() if merge else None

    def dev(h, a, b, dc=0):
        return place.at(b, a, dc) if h == 0 else place.at(a, b, dc)

    def send(h, a, b, lo, num, target, kr=None):
        where = region(dev(h, a, b), lo, num)
        kr = sems.new_recv() if kr is None else kr
        sems.copy(where, where, ks, kr, target).start()
        return kr

    def wait(kr, h, a, b, lo, num):
        where = region(dev(h, a, b), lo, num)
        sems.copy(where, where, ks, kr, partner).wait_recv()

    def wait_most(kr, n):
        sems.copy(most(n), most(n), ks, kr, partner).wait_recv()

    def pass_on(h, a, b, lo, num):
        send(h, a, b, lo, num, partner, k_pass)

    first, second, rel1, rel2 = {}, {}, {}, {}
    shifts = (1, -1) if relay else (1, -1, 2)

    def go_second(h, a, lo, num):
        for s in shifts:
            second[h, a, s] = send(h, a, 0, lo, num, dev(h, 0, s), k_second)

    for h, lo, num in halves:
        for s in shifts:
            first[h, s] = send(h, 0, 0, lo, num, dev(h, s, 0))
    for h, lo, num in halves:
        go_second(h, 0, lo, num)
    for h, lo, num in halves:
        pass_on(h, 0, 0, lo, num)
    yield
    if not relay:
        for s in shifts:
            for h, lo, num in halves:
                wait(first[h, s], h, -s, 0, lo, num)
                go_second(h, -s, lo, num)
                pass_on(h, -s, 0, lo, num)
            yield
        if merge:
            wait_most(k_second, chips - place.side)
        for a in (0, -1, 1, -2):
            for s in shifts:
                for h, lo, num in halves:
                    if not merge:
                        wait(second[h, a, s], h, a, -s, lo, num)
                    pass_on(h, a, -s, lo, num)
            yield
    else:
        def relay_on(kr, h, a, b, lo, s, ta, tb):
            part = lo + (s == -1)
            return send(h, a, b, part, 1, dev(h, ta, tb), kr)

        for s in shifts:
            for h, lo, num in halves:
                wait(first[h, s], h, -s, 0, lo, num)
                rel1[h] = relay_on(rel1.get(h), h, -s, 0, lo, s, s, 0)
                go_second(h, -s, lo, num)
                pass_on(h, -s, 0, lo, num)
            yield

        def relay2(h, lo, num, a, s):
            wait(second[h, a, s], h, a, -s, lo, num)
            rel2[h, a] = relay_on(rel2.get((h, a)), h, a, -s, lo, s, 0, s)
            pass_on(h, a, -s, lo, num)

        for h, lo, num in halves:
            for s in shifts:
                relay2(h, lo, num, 0, s)
        yield
        for h, lo, num in halves:
            wait(rel1[h], h, 2, 0, lo, num)
            go_second(h, 2, lo, num)
            pass_on(h, 2, 0, lo, num)
        yield
        for a in (-1, 1, 2):
            for s in shifts:
                for h, lo, num in halves:
                    relay2(h, lo, num, a, s)
            yield
        for a in (0, -1, 1, 2):
            for h, lo, num in halves:
                wait(rel2[h, a], h, a, 2, lo, num)
                pass_on(h, a, 2, lo, num)
            yield
    wait_most(k_pass, chips)
    yield
    sems.copy(most(2 * chips - 1), most(2 * chips - 1), ks, k_pass, partner).wait_send()
    yield


def finish(*gens):
    gens = list(gens)
    while gens:
        gens = [g for g in gens if next(g, gens) is not gens]


NN = (((1,), (0,)), ((), ()))
NT = (((1,), (1,)), ((), ()))
TN = (((0,), (0,)), ((), ()))
EXACT = lax.Precision.HIGHEST


def mm(a, b, dims=NN, precision=None):
    return lax.dot_general(a, b, dims, precision=precision, preferred_element_type=F32)


def three(v):
    a = v.astype(BF16)
    v = v - a.astype(F32)
    b = v.astype(BF16)
    return a, b, (v - b.astype(F32)).astype(BF16)


def iota(shape, dim):
    return lax.broadcasted_iota(jnp.int32, shape, dim)


def inv_rms(v):
    return lax.rsqrt(jnp.mean(v * v, axis=-1, keepdims=True) + NORM_EPS)


def rms_back(v, inv, g):
    return inv * g - v * (inv * inv * inv * jnp.mean(g * v, axis=-1, keepdims=True))


def turn(place, dest_core, d1, d2):
    along_x = dest_core == 0
    return jnp.where(along_x, d2, d1), jnp.where(along_x, d1, d2)


def block_offset(i, place):
    side = place.side
    d1, dc = i // (2 * side), lax.rem(i // side, 2)
    d2 = lax.rem(i // 2, 2) + 2 * lax.rem(i, 2)
    dy, dx = turn(place, lax.rem(place.core + dc, 2), d1, d2)
    return dy, dx, dc


def layer_kernel(group, experts, cap, x_in, idst_in, dy_in, wq_ref, wk_ref, wv_ref, wo_ref, wr_in, wg_in, wu_in, wd_in,
                 y_ref, gx_ref, gg_ref, gu_ref, gd_ref,
                 w_full, u_all, dy_all, ids_all, g_all, m_s, pick_s, ru_s, rdy_s, ag_s, au_s, mid_s, dag_s, dau_s,
                 x_ref, idst_ref, dy_ref, wr_ref, wg_ref, wu_ref, wd_ref, relay, sums, total, small, smalls, prob_s, q_s, k_s, v_s, o_s, hid_s, place_s, gd_s,
                 lsem, ssem, rsem):
    place = Place(group)
    me = place.me
    toks, d_model = x_ref.shape
    choices = idst_ref.shape[0]
    local, _, ff = wg_in.shape
    depth = wq_ref.shape[0]
    per = 2 * place.side
    groups = group // per
    sems = Sems(ssem, rsem)

    def rows_of(d):
        return pl.ds(pl.multiple_of(d * depth, depth), depth)

    own_w = [pltpu.make_async_copy(w, w_full.at[i, rows_of(me)], lsem.at[i]) for i, w in enumerate((wq_ref, wk_ref, wv_ref, wo_ref))]
    experts_in = [pltpu.make_async_copy(src, dst, lsem.at[4 + i])
                  for i, (src, dst) in enumerate(((wg_in, wg_ref), (wu_in, wu_ref), (wd_in, wd_ref)))]
    sem = pltpu.get_barrier_semaphore()
    peers = near_peers(place)
    for peer in peers:
        pl.semaphore_signal(sem, inc=1, device_id={AXIS: peer}, device_id_type=pl.DeviceIdType.MESH)

    tokens_in = [pltpu.make_async_copy(src, dst, lsem.at[7 + i])
                 for i, (src, dst) in enumerate(((idst_in, idst_ref), (x_in, x_ref), (dy_in, dy_ref), (wr_in, wr_ref)))]
    for copy in tokens_in + own_w + experts_in:
        copy.start()

    for copy in tokens_in:
        copy.wait()
    dy_all[me] = dy_ref[...]
    idst = idst_ref[...].astype(F32)
    ids_all[me] = idst
    lane_e = iota((2 * experts, toks), 0).astype(F32)
    chosen_t = jnp.zeros((2 * experts, toks), F32)
    for j in range(choices):
        chosen_t += jnp.where(idst[j:j + 1, :] == lane_e, 1.0, 0.0)
    chosen = jnp.transpose(chosen_t)[:, :experts]
    before = (iota((toks, toks), 0) > iota((toks, toks), 1)).astype(F32).astype(BF16)
    x = x_ref[...].astype(F32)
    x_inv = inv_rms(x)
    a = (x * x_inv).astype(BF16)

    for copy in own_w:
        copy.wait()
    pl.semaphore_wait(sem, len(peers))
    quarter = toks // 4
    two = ((0, 0, 2), (1, 2, 2))
    w_steps = gather_steps(place, sems, lambda d, lo, num: w_full.at[pl.ds(lo, num), rows_of(d)],
                           lambda n: w_full.at[:, pl.ds(0, n * depth)], False, two)
    ids_steps = gather_steps(place, sems, lambda d, lo, num: ids_all.at[d], lambda n: ids_all.at[pl.ds(0, n)], False, ((0, 0, 1),), True)
    dy_steps = gather_steps(place, sems, lambda d, lo, num: dy_all.at[d, pl.ds(lo * quarter, num * quarter)],
                            lambda n: dy_all.at[pl.ds(0, n)], True, two)
    next(w_steps)
    next(ids_steps)
    next(dy_steps)
    for _ in range(3):
        next(w_steps)
        next(ids_steps)
    next(dy_steps)
    next(dy_steps)
    finish(w_steps)
    next(ids_steps)

    q_s[...] = mm(a, w_full[0]).astype(BF16)
    k_s[...] = mm(a, w_full[1]).astype(BF16)
    v_s[...] = mm(a, w_full[2]).astype(BF16)
    next(dy_steps, None)
    causal = iota((toks, toks), 0) >= iota((toks, toks), 1)
    low = iota((toks, 2 * HEAD_DIM), 1) < HEAD_DIM
    zero_b = jnp.zeros((toks, 2 * HEAD_DIM), BF16)
    pairs = d_model // (2 * HEAD_DIM)
    scale = HEAD_DIM ** -0.5

    def half(v, side):
        return jnp.where(low, v, zero_b) if side == 0 else jnp.where(low, zero_b, v)

    for pair in range(pairs):
        lanes = pl.ds(pair * 2 * HEAD_DIM, 2 * HEAD_DIM)
        qp, kp, vp = q_s[:, lanes], k_s[:, lanes], v_s[:, lanes]
        outs = []
        for hf in range(2):
            s = jnp.where(causal, mm(half(qp, hf), kp, NT) * scale, -1e30)
            e = jnp.exp(s - jnp.max(s, axis=-1, keepdims=True))
            p = e / jnp.sum(e, axis=-1, keepdims=True)
            prob_s[2 * pair + hf] = jnp.transpose(p)
            outs.append(mm(p.astype(BF16), vp))
        o_s[:, lanes] = jnp.where(low, outs[0], outs[1]).astype(BF16)
        if pair >= 3:
            next(dy_steps, None)

    hid = (x + mm(o_s[...], w_full[3])).astype(BF16)
    hid_s[...] = hid
    h = hid.astype(F32)
    h_inv = inv_rms(h)
    n = h * h_inv
    u_all[me] = n.astype(BF16)
    logits = mm(n, wr_ref[...], NT, EXACT)
    top = jnp.max(jnp.where(chosen > 0.0, logits, -3e38), axis=-1, keepdims=True)
    expd = jnp.where(chosen > 0.0, jnp.exp(logits - top), 0.0)
    gates = expd / jnp.sum(expd, axis=-1, keepdims=True)
    gates_t = jnp.transpose(jnp.concatenate([gates, jnp.zeros_like(gates)], axis=-1))
    for j in range(choices):
        g_all[me, j:j + 1, :] = jnp.sum(jnp.where(idst[j:j + 1, :] == lane_e, gates_t, 0.0), axis=0, keepdims=True)

    u_steps = gather_steps(place, sems, lambda d, lo, num: u_all.at[d, pl.ds(lo * quarter, num * quarter)],
                           lambda n: u_all.at[pl.ds(0, n)], True, two)
    g_steps = gather_steps(place, sems, lambda d, lo, num: g_all.at[d], lambda n: g_all.at[pl.ds(0, n)], False, ((0, 0, 1),), True)
    next(g_steps)
    next(u_steps)
    finish(ids_steps)

    first_e = (me * local).astype(F32)
    row8 = iota((8, toks), 0)

    def find(i, _):
        ids = ids_all[place.at(*block_offset(i, place))]
        m = jnp.zeros((8, toks), F32)
        for e in range(local):
            hit = jnp.sum(jnp.where(ids == first_e + e, 1.0, 0.0), axis=0, keepdims=True)
            m = jnp.where(row8 == e, hit, m)
        m_s[i] = m
        return 0

    lax.fori_loop(0, group, find, 0)
    next(u_steps)
    for _ in range(3):
        next(g_steps)
    next(dy_steps, None)
    next(dy_steps, None)
    m_flat = m_s[...].reshape(group * 8, toks)
    after = (iota((toks, toks), 0) < iota((toks, toks), 1)).astype(F32).astype(BF16)
    r_flat = jnp.where(m_flat > 0.0, mm(m_flat.astype(BF16), after), -1.0)
    m_s[...] = r_flat.reshape(group, 8, toks)
    next(u_steps)
    next(dy_steps, None)
    slot = iota((cap, toks), 0).astype(F32)

    def build(i, _):
        r = m_s[i]
        for e in range(local):
            pick_s[i, pl.ds(e * cap, cap), :] = jnp.where(slot == r[e:e + 1, :], 1.0, 0.0).astype(BF16)
        return 0

    lax.fori_loop(0, group, build, 0)

    def take_rows(i, source, dest):
        rows = mm(pick_s[i], source[place.at(*block_offset(i, place))]).astype(BF16)
        for e in range(local):
            at = i * cap
            dest[e, pl.ds(pl.multiple_of(at, cap), cap), :] = rows[e * cap:(e + 1) * cap]

    def take_dy(g, _):
        for b in range(per):
            take_rows(g * per + b, dy_all, rdy_s)
        return 0

    for _ in range(9):
        next(u_steps)
        next(dy_steps, None)
        next(dy_steps, None)
    for copy in experts_in:
        copy.wait()

    span = per * cap
    side = place.side
    both = local * cap
    k_first, k_second, k_small = sems.new_recv(4), sems.new_recv(2), sems.new_recv()
    k_rows, k_sums, k_smalls = [sems.new_send() for _ in range(2)], [sems.new_send() for _ in range(2)], sems.new_send()

    def first_hop(part, d1, dc, p):
        core = lax.rem(place.core + dc, 2)
        relay_dc = (dc + p) % 2
        src = u_all.at[pl.ds(d1 * per + dc * side + 2 * p, 2), pl.ds(part * both, both)]
        return sems.copy(src, relay.at[part, p, :, 2 * d1 + relay_dc], k_rows[part], k_first + 2 * part + p,
                         place.at(*turn(place, core, d1, 0), relay_dc))

    def first_done(part, p):
        at = relay.at[part, p, :, pl.ds(1, per - 1)]
        return sems.copy(at, at, k_rows[part], k_first + 2 * part + p, me)

    def dest_of(p, j):
        core = lax.rem(place.core + p, 2)
        return place.at(*turn(place, core, 0, p + 2 * j), p)

    def second_hop(part, p, j):
        return sems.copy(sums.at[part, 2 * j + p - 1], total.at[part, 2 * j + p], k_sums[part], k_second + part, dest_of(p, j))

    def small_hop(p, j):
        return sems.copy(small.at[2 * j + p - 1], smalls.at[2 * j + p], k_smalls, k_small, dest_of(p, j))

    def put(part, e, g, rows):
        for b in range(per):
            u_all[g * per + b, pl.ds(part * both + e * cap, cap), :] = rows[b * cap:(b + 1) * cap]

    def start_group(part, g):
        @pl.when(g > 0)
        def _():
            for dc in range(2):
                for p in range(2):
                    first_hop(part, g, dc, p).start()

        @pl.when(g == 0)
        def _():
            for p in range(2):
                first_hop(part, 0, 1 - p, p).start()
                for j in range(2):
                    relay[part, p, j, 0] = u_all[p * side + 2 * p + j, pl.ds(part * both, both), :]

    def take_u(dc):
        def body(g, _):
            for b in range(2):
                for d2 in range(side):
                    take_rows((2 * g + b) * per + dc * side + d2, u_all, ru_s)
            return 0
        lax.fori_loop(0, side // 2, body, 0)

    take_u(0)
    next(u_steps)
    next(dy_steps, None)
    take_u(1)
    finish(u_steps)

    def forward(step, _):
        g = lax.rem(step + side // 2, side)
        rows = pl.ds(pl.multiple_of(g * span, span), span)
        for e in range(local):
            ru = ru_s[e, rows, :]
            ag = mm(ru, wg_ref[e])
            au = mm(ru, wu_ref[e])
            mid = (ag * jax.nn.sigmoid(ag) * au).astype(BF16)
            ag_s[e, rows, :] = ag
            au_s[e, rows, :] = au
            mid_s[e, rows, :] = mid
            put(0, e, g, mm(mid, wd_ref[e]).astype(BF16))
        start_group(0, g)
        return 0

    lax.fori_loop(0, groups, forward, 0)

    def weigh(q, _):
        for i in [q * side + b for b in range(side)]:
            d = place.at(*block_offset(i, place))
            ids, gts = ids_all[d], g_all[d]
            for e in range(local):
                gate = jnp.sum(jnp.where(ids == first_e + e, gts, 0.0), axis=0, keepdims=True)
                col = jnp.sum(pick_s[i, pl.ds(e * cap, cap), :].astype(F32) * gate, axis=-1, keepdims=True)
                at = pl.ds(pl.multiple_of(i * cap, cap), cap)
                rdy_s[e, at, :] = (col * rdy_s[e, at, :].astype(F32)).astype(BF16)
        return 0

    finish(g_steps, dy_steps)
    lax.fori_loop(0, groups, take_dy, 0)
    lax.fori_loop(0, group // side, weigh, 0)

    def backward(step, _):
        g = lax.rem(step + side // 2, side)
        rows = pl.ds(pl.multiple_of(g * span, span), span)
        for e in range(local):
            gm = mm(rdy_s[e, rows, :], wd_ref[e], NT)
            ag, au = ag_s[e, rows, :], au_s[e, rows, :]
            sg = jax.nn.sigmoid(ag)
            dag = (gm * au * sg * (1.0 + ag * (1.0 - sg))).astype(BF16)
            dau = (gm * ag * sg).astype(BF16)
            dag_s[e, rows, :] = dag
            dau_s[e, rows, :] = dau
            put(1, e, g, (mm(dag, wg_ref[e], NT) + mm(dau, wu_ref[e], NT)).astype(BF16))
        start_group(1, g)
        return 0

    lax.fori_loop(0, groups, backward, 0)

    def weights(e, _):
        gd_s[e] = mm(mid_s[e], rdy_s[e], TN).astype(BF16)
        mid_s[e, pl.ds(0, d_model), :] = mm(ru_s[e], dag_s[e], TN).astype(BF16)
        dag_s[e, pl.ds(0, d_model), :] = mm(ru_s[e], dau_s[e], TN).astype(BF16)
        return 0

    lax.fori_loop(0, local, weights, 0)
    grads_out = [pltpu.make_async_copy(src, dst, lsem.at[i])
                 for i, (src, dst) in enumerate(((mid_s.at[:, pl.ds(0, d_model)], gg_ref), (dag_s.at[:, pl.ds(0, d_model)], gu_ref), (gd_s, gd_ref), (o_s, y_ref)))]
    for copy in grads_out[:3]:
        copy.start()

    wide = per * both
    blocks = wide // cap
    col = iota((1, wide), 1)
    colmod = col
    for _ in range(1, blocks):
        colmod = jnp.where(colmod >= cap, colmod - cap, colmod)
    colmod = colmod.astype(F32)
    e_row = iota((experts, wide), 0).astype(F32)
    blk = iota((blocks, wide), 0) * cap
    blk_col = iota((blocks, wide), 1)
    block_of = jnp.where((blk_col >= blk) & (blk_col < blk + cap), 1.0, 0.0).astype(BF16)

    def owner_at(core, p, d1, dc, d2, e):
        dy, dx = turn(place, core, -d1, -d2)
        return (place.at(dy, dx, p + dc) * local + e).astype(F32)

    def relay_z(q, _):
        p, j = q % 2, q // 2
        core = lax.rem(place.core + p, 2)
        dest = dest_of(p, j)
        owner = jnp.zeros((1, wide), F32)
        for b in range(blocks):
            s, e = b // local, b % local
            owner = jnp.where((col >= b * cap) & (col < (b + 1) * cap), owner_at(core, 0, s // 2, s % 2, 0, e), owner)
        spread = jnp.where(e_row == owner, 1.0, 0.0).astype(BF16)
        ids, gts = ids_all[dest], g_all[dest]
        e_in = iota((2 * experts, toks), 0)
        e_id = jnp.where(e_in >= experts, e_in - experts, e_in).astype(F32)
        both_t = jnp.zeros((2 * experts, toks), F32)
        for c in range(choices):
            both_t += jnp.where(ids[c:c + 1, :] == e_id, jnp.where(e_in >= experts, gts[c:c + 1, :], 1.0), 0.0)
        both_v = jnp.transpose(both_t)
        chose, weight = both_v[:, :experts], both_v[:, experts:]
        ranks = jnp.where(chose > 0.0, mm(before, chose.astype(BF16)), -1.0).astype(BF16)
        z = relay[0, p, j].reshape(wide, d_model)
        here = mm(ranks, spread) == colmod
        place_s[q] = jnp.where(here, 1.0, 0.0).astype(BF16)
        y_sum = jnp.zeros((toks, d_model), F32)
        for piece in three(weight):
            y_sum += mm(jnp.where(here, mm(piece, spread), 0.0).astype(BF16), z)
        gg_sum = jnp.zeros((blocks, toks), F32)
        for piece in three(jnp.where(here, mm(dy_all[dest], z, NT), 0.0)):
            gg_sum += mm(block_of, piece, NT)

        @pl.when(q == 0)
        def _():
            total[0, 0] = y_sum
            smalls[0] = gg_sum

        @pl.when(q > 0)
        def _():
            sums[0, q - 1] = y_sum
            small[q - 1] = gg_sum
            second_hop(0, p, j).start()
            small_hop(p, j).start()
        return 0

    for p in range(2):
        first_done(0, p).wait_recv()
    lax.fori_loop(0, side, lambda t, _: relay_z(lax.rem(t + 2, side), 0), 0)
    for p in range(2):
        first_done(1, p).wait_recv()

    def relay_d(q, _):
        p, j = q % 2, q // 2
        sums_d = mm(place_s[q], relay[1, p, j].reshape(wide, d_model))

        @pl.when(q == 0)
        def _():
            total[1, 0] = sums_d

        @pl.when(q > 0)
        def _():
            sums[1, q - 1] = sums_d
            second_hop(1, p, j).start()
        return 0

    lax.fori_loop(0, side, lambda t, _: relay_d(lax.rem(t + 2, side), 0), 0)

    rest = pl.ds(1, side - 1)
    sems.copy(total.at[0, rest], total.at[0, rest], k_sums[0], k_second, me).wait_recv()
    sems.copy(smalls.at[rest], smalls.at[rest], k_smalls, k_small, me).wait_recv()
    dyv = dy_ref[...]
    o_s[...] = (hid_s[...].astype(F32) + ((total[0, 0] + total[0, 1]) + (total[0, 2] + total[0, 3]))).astype(BF16)
    grads_out[3].start()
    m_col = iota((experts, 1), 0)
    owner = jnp.zeros((experts, 1), F32)
    for m in range(experts):
        d2, s, e = m // blocks, (m % blocks) // local, m % local
        owner = jnp.where(m_col == m, owner_at(place.core, d2 % 2, s // 2, s % 2, d2, e), owner)
    perm = jnp.where(owner == iota((experts, experts), 1).astype(F32), 1.0, 0.0).astype(BF16)
    g_gates = jnp.zeros((toks, experts), F32)
    for piece in three(smalls[...].reshape(experts, toks)):
        g_gates += mm(piece, perm, TN)
    g_logits = gates * (g_gates - jnp.sum(gates * g_gates, axis=-1, keepdims=True))
    g_hnorm = mm(g_logits, wr_ref[...], NN, EXACT)
    sems.copy(total.at[1, rest], total.at[1, rest], k_sums[1], k_second + 1, me).wait_recv()
    gn = g_hnorm + ((total[1, 0] + total[1, 1]) + (total[1, 2] + total[1, 3]))
    h = hid_s[...].astype(F32)
    h_inv = inv_rms(h)
    g_hid = (dyv.astype(F32) + rms_back(h, h_inv, gn)).astype(BF16)
    grads_out[3].wait()
    o_s[...] = mm(g_hid, w_full[3], NT).astype(BF16)
    g_xn = jnp.zeros((toks, d_model), F32)
    for pair in range(pairs):
        lanes = pl.ds(pair * 2 * HEAD_DIM, 2 * HEAD_DIM)
        qp, kp, vp, dop = q_s[:, lanes], k_s[:, lanes], v_s[:, lanes], o_s[:, lanes]
        dq, dk, dv = [], [], []
        for hf in range(2):
            p_t = prob_s[2 * pair + hf]
            dp_t = mm(vp, half(dop, hf), NT)
            ds_t = (p_t * (dp_t - jnp.sum(dp_t * p_t, axis=0, keepdims=True)) * scale).astype(BF16)
            dq.append(mm(ds_t, kp, TN))
            dk.append(mm(ds_t, qp))
            dv.append(mm(p_t.astype(BF16), dop))
        for i, parts in enumerate((dq, dk, dv)):
            grad = jnp.where(low, parts[0], parts[1]).astype(BF16)
            g_xn += mm(grad, w_full[i, :, lanes], NT)
    x = x_ref[...].astype(F32)
    gx_ref[...] = (g_hid.astype(F32) + rms_back(x, inv_rms(x), g_xn)).astype(BF16)

    for copy in grads_out[:3]:
        copy.wait()
    for part in range(2):
        at = relay.at[part, :, :, pl.ds(1, per - 1)]
        sems.copy(at, at, k_rows[part], k_first, me).wait_send()
        sems.copy(sums.at[part], sums.at[part], k_sums[part], k_second, me).wait_send()
    sems.copy(small, small, k_smalls, k_small, me).wait_send()
    assert (sems.n_send, sems.n_recv) == (N_SEND, N_RECV)


def settle_kernel(*refs):
    n = (len(refs) - 2) // 3
    ins, outs, held, lsem, ssem = refs[:n], refs[n:2 * n], refs[2 * n:3 * n], refs[-2], refs[-1]
    loads = [pltpu.make_async_copy(a, h, lsem.at[i]) for i, (a, h) in enumerate(zip(ins, held))]
    stores = [pltpu.make_async_copy(h, o, ssem.at[i]) for i, (h, o) in enumerate(zip(held, outs))]
    for copy in loads:
        copy.start()
    for load, store in zip(loads, stores):
        load.wait()
        store.start()
    for copy in stores:
        copy.wait()


def settle(*arrays):
    n = len(arrays)
    hbm = pl.BlockSpec(memory_space=pl.ANY)
    return pl.pallas_call(
        settle_kernel, out_shape=[jax.ShapeDtypeStruct(a.shape, a.dtype) for a in arrays],
        in_specs=[hbm] * n, out_specs=[hbm] * n,
        scratch_shapes=[pltpu.VMEM(a.shape, a.dtype) for a in arrays] + [pltpu.SemaphoreType.DMA((n,))] * 2,
        name='settle')(*arrays)


def solution(mesh):
    group = mesh.shape[AXIS]
    tok_spec = P(('dp', 'ep'), None)
    fsdp_spec = P('ep', None)
    expert_spec = P('ep', None, None)
    grad_spec = P(('dp', 'ep'), None, None)

    def device_step(x_tokens, expert_ids, grad_y, w_q, w_k, w_v, w_o, w_router, w_gate, w_up, w_down):
        toks, d_model = x_tokens.shape
        choices = expert_ids.shape[1]
        experts = w_router.shape[1]
        local, _, ff = w_gate.shape
        avg_load = toks * choices // experts
        cap = avg_load + avg_load // 2
        assert toks == SEQ_LEN
        heads = w_q.shape[1] // HEAD_DIM
        shape, vm = jax.ShapeDtypeStruct, pltpu.VMEM
        rows = group * cap
        side = math.isqrt(group // 2)
        per = 2 * side
        assert local == 2
        in_vmem = pl.BlockSpec(memory_space=pltpu.VMEM)
        in_hbm = pl.BlockSpec(memory_space=pl.ANY)
        square = vm((toks, d_model), BF16)
        outs = pl.pallas_call(
            functools.partial(layer_kernel, group, experts, cap),
            out_shape=[shape(x_tokens.shape, BF16), shape(x_tokens.shape, BF16), shape(w_gate.shape, BF16),
                       shape(w_up.shape, BF16), shape(w_down.shape, BF16)],
            in_specs=[in_hbm] * 11,
            out_specs=[in_hbm, in_vmem] + [in_hbm] * 3,
            scratch_shapes=[
                vm((4, group * w_q.shape[0], d_model), BF16), vm((group, toks, d_model), BF16), vm((group, toks, d_model), BF16),
                vm((group, choices, toks), F32), vm((group, choices, toks), F32), vm((group, 8, toks), F32),
                vm((group, local * cap, toks), BF16), vm((local, rows, d_model), BF16), vm((local, rows, d_model), BF16),
                vm((local, rows, ff), F32), vm((local, rows, ff), F32),
                vm((local, rows, ff), BF16), vm((local, rows, ff), BF16), vm((local, rows, ff), BF16),
                square, vm((choices, toks), jnp.int32), square, vm((experts, d_model), F32),
                vm(w_gate.shape, BF16), vm(w_up.shape, BF16), vm(w_down.shape, BF16), vm((2, 2, 2, per, local * cap, d_model), BF16),
                vm((2, side - 1, toks, d_model), F32), vm((2, side, toks, d_model), F32),
                vm((side - 1, experts // side, toks), F32), vm((side, experts // side, toks), F32),
                vm((heads, toks, toks), F32), square, square, square, square, square,
                vm((group // per, toks, per * local * cap), BF16),
                vm(w_down.shape, BF16),
                pltpu.SemaphoreType.DMA((11,)), pltpu.SemaphoreType.DMA((N_SEND,)), pltpu.SemaphoreType.DMA((N_RECV,))],
            compiler_params=pltpu.CompilerParams(collective_id=1, has_side_effects=True, vmem_limit_bytes=67043328),
            name='layer')(x_tokens, expert_ids.T, grad_y, w_q, w_k, w_v, w_o, w_router.T, w_gate, w_up, w_down)
        return settle(*outs)

    return jax.shard_map(
        device_step, mesh=mesh,
        in_specs=(tok_spec, tok_spec, tok_spec, fsdp_spec, fsdp_spec, fsdp_spec, fsdp_spec,
                  P(None, None), expert_spec, expert_spec, expert_spec),
        out_specs=(tok_spec, tok_spec, grad_spec, grad_spec, grad_spec),
        check_vma=False)
```

```python
import functools
import math

import jax
import jax.numpy as jnp
from jax import lax
from jax.experimental import pallas as pl
from jax.experimental.pallas import tpu as pltpu
from jax.sharding import PartitionSpec as P

NORM_EPS = 1e-6
SEQ_LEN = 256
HEAD_DIM = 64
AXIS = 'ep'
N_SEND = 10
N_RECV = 110
F32 = jnp.float32
BF16 = jnp.bfloat16


class Place:
    def __init__(self, group):
        self.group = group
        self.side = math.isqrt(group // 2)
        self.me = lax.axis_index(AXIS)
        self.core = lax.rem(self.me, 2)
        self.x = lax.rem(self.me // 2, self.side)
        self.y = self.me // (2 * self.side)

    def wrap(self, v):
        return lax.rem(v + self.side, self.side)

    def at(self, dy, dx, dc=0):
        return (self.wrap(self.y + dy) * self.side + self.wrap(self.x + dx)) * 2 + lax.rem(self.core + dc, 2)


def near_peers(pl_):
    return [pl_.at(0, 1), pl_.at(0, -1), pl_.at(1, 0), pl_.at(-1, 0), pl_.at(0, 2), pl_.at(2, 0), pl_.at(0, 0, 1)]


class Sems:
    def __init__(self, ssem, rsem):
        self.ssem, self.rsem, self.n_send, self.n_recv = ssem, rsem, 0, 0

    def new_send(self):
        self.n_send += 1
        return self.n_send - 1

    def new_recv(self, count=1):
        self.n_recv += count
        return self.n_recv - count

    def copy(self, src, dst, ks, kr, target):
        return pltpu.make_async_remote_copy(
            src_ref=src, dst_ref=dst, send_sem=self.ssem.at[ks], recv_sem=self.rsem.at[kr],
            device_id={AXIS: target}, device_id_type=pl.DeviceIdType.MESH)


def gather_steps(place, sems, region, most, relay, halves, merge=False):
    partner = place.at(0, 0, 1)
    chips = place.side * place.side
    ks, k_pass = sems.new_send(), sems.new_recv()
    k_second = sems.new_recv() if merge else None

    def dev(h, a, b, dc=0):
        return place.at(b, a, dc) if h == 0 else place.at(a, b, dc)

    def send(h, a, b, lo, num, target, kr=None):
        where = region(dev(h, a, b), lo, num)
        kr = sems.new_recv() if kr is None else kr
        sems.copy(where, where, ks, kr, target).start()
        return kr

    def wait(kr, h, a, b, lo, num):
        where = region(dev(h, a, b), lo, num)
        sems.copy(where, where, ks, kr, partner).wait_recv()

    def wait_most(kr, n):
        sems.copy(most(n), most(n), ks, kr, partner).wait_recv()

    def pass_on(h, a, b, lo, num):
        send(h, a, b, lo, num, partner, k_pass)

    first, second, rel1, rel2 = {}, {}, {}, {}
    shifts = (1, -1) if relay else (1, -1, 2)

    def go_second(h, a, lo, num):
        for s in shifts:
            second[h, a, s] = send(h, a, 0, lo, num, dev(h, 0, s), k_second)

    for h, lo, num in halves:
        for s in shifts:
            first[h, s] = send(h, 0, 0, lo, num, dev(h, s, 0))
    for h, lo, num in halves:
        go_second(h, 0, lo, num)
    for h, lo, num in halves:
        pass_on(h, 0, 0, lo, num)
    yield
    if not relay:
        for s in shifts:
            for h, lo, num in halves:
                wait(first[h, s], h, -s, 0, lo, num)
                go_second(h, -s, lo, num)
                pass_on(h, -s, 0, lo, num)
            yield
        if merge:
            wait_most(k_second, chips - place.side)
        for a in (0, -1, 1, -2):
            for s in shifts:
                for h, lo, num in halves:
                    if not merge:
                        wait(second[h, a, s], h, a, -s, lo, num)
                    pass_on(h, a, -s, lo, num)
            yield
    else:
        def relay_on(kr, h, a, b, lo, s, ta, tb):
            part = lo + (s == -1)
            return send(h, a, b, part, 1, dev(h, ta, tb), kr)

        for s in shifts:
            for h, lo, num in halves:
                wait(first[h, s], h, -s, 0, lo, num)
                rel1[h] = relay_on(rel1.get(h), h, -s, 0, lo, s, s, 0)
                go_second(h, -s, lo, num)
                pass_on(h, -s, 0, lo, num)
            yield

        def relay2(h, lo, num, a, s):
            wait(second[h, a, s], h, a, -s, lo, num)
            rel2[h, a] = relay_on(rel2.get((h, a)), h, a, -s, lo, s, 0, s)
            pass_on(h, a, -s, lo, num)

        for h, lo, num in halves:
            for s in shifts:
                relay2(h, lo, num, 0, s)
        yield
        for h, lo, num in halves:
            wait(rel1[h], h, 2, 0, lo, num)
            go_second(h, 2, lo, num)
            pass_on(h, 2, 0, lo, num)
        yield
        for a in (-1, 1, 2):
            for s in shifts:
                for h, lo, num in halves:
                    relay2(h, lo, num, a, s)
            yield
        for a in (0, -1, 1, 2):
            for h, lo, num in halves:
                wait(rel2[h, a], h, a, 2, lo, num)
                pass_on(h, a, 2, lo, num)
            yield
    wait_most(k_pass, chips)
    yield
    sems.copy(most(2 * chips - 1), most(2 * chips - 1), ks, k_pass, partner).wait_send()
    yield


def finish(*gens):
    gens = list(gens)
    while gens:
        gens = [g for g in gens if next(g, gens) is not gens]


NN = (((1,), (0,)), ((), ()))
NT = (((1,), (1,)), ((), ()))
TN = (((0,), (0,)), ((), ()))
EXACT = lax.Precision.HIGHEST


def mm(a, b, dims=NN, precision=None):
    return lax.dot_general(a, b, dims, precision=precision, preferred_element_type=F32)


def three(v):
    a = v.astype(BF16)
    v = v - a.astype(F32)
    b = v.astype(BF16)
    return a, b, (v - b.astype(F32)).astype(BF16)


def iota(shape, dim):
    return lax.broadcasted_iota(jnp.int32, shape, dim)


def inv_rms(v):
    return lax.rsqrt(jnp.mean(v * v, axis=-1, keepdims=True) + NORM_EPS)


def rms_back(v, inv, g):
    return inv * g - v * (inv * inv * inv * jnp.mean(g * v, axis=-1, keepdims=True))


def turn(place, dest_core, d1, d2):
    along_x = dest_core == 0
    return jnp.where(along_x, d2, d1), jnp.where(along_x, d1, d2)


def block_offset(i, place):
    side = place.side
    d1, dc = i // (2 * side), lax.rem(i // side, 2)
    d2 = lax.rem(i // 2, 2) + 2 * lax.rem(i, 2)
    dy, dx = turn(place, lax.rem(place.core + dc, 2), d1, d2)
    return dy, dx, dc


def layer_kernel(group, experts, cap, x_in, idst_in, dy_in, wq_ref, wk_ref, wv_ref, wo_ref, wr_in, wg_in, wu_in, wd_in,
                 y_ref, gx_ref, gg_ref, gu_ref, gd_ref,
                 w_full, u_all, dy_all, ids_all, g_all, m_s, pick_s, ru_s, rdy_s, ag_s, au_s, mid_s, dag_s, dau_s,
                 x_ref, idst_ref, dy_ref, wr_ref, wg_ref, wu_ref, wd_ref, relay, sums, total, small, smalls, prob_s, q_s, k_s, v_s, o_s, hid_s, place_s, gd_s,
                 lsem, ssem, rsem):
    place = Place(group)
    me = place.me
    toks, d_model = x_ref.shape
    choices = idst_ref.shape[0]
    local, _, ff = wg_in.shape
    depth = wq_ref.shape[0]
    per = 2 * place.side
    groups = group // per
    sems = Sems(ssem, rsem)

    def rows_of(d):
        return pl.ds(pl.multiple_of(d * depth, depth), depth)

    own_w = [pltpu.make_async_copy(w, w_full.at[i, rows_of(me)], lsem.at[i]) for i, w in enumerate((wq_ref, wk_ref, wv_ref, wo_ref))]
    experts_in = [pltpu.make_async_copy(src, dst, lsem.at[4 + i])
                  for i, (src, dst) in enumerate(((wg_in, wg_ref), (wu_in, wu_ref), (wd_in, wd_ref)))]
    sem = pltpu.get_barrier_semaphore()
    peers = near_peers(place)
    for peer in peers:
        pl.semaphore_signal(sem, inc=1, device_id={AXIS: peer}, device_id_type=pl.DeviceIdType.MESH)

    tokens_in = [pltpu.make_async_copy(src, dst, lsem.at[7 + i])
                 for i, (src, dst) in enumerate(((idst_in, idst_ref), (x_in, x_ref), (dy_in, dy_ref), (wr_in, wr_ref)))]
    for copy in tokens_in + own_w + experts_in:
        copy.start()

    for copy in tokens_in:
        copy.wait()
    dy_all[me] = dy_ref[...]
    idst = idst_ref[...].astype(F32)
    ids_all[me] = idst
    lane_e = iota((2 * experts, toks), 0).astype(F32)
    chosen_t = jnp.zeros((2 * experts, toks), F32)
    for j in range(choices):
        chosen_t += jnp.where(idst[j:j + 1, :] == lane_e, 1.0, 0.0)
    chosen = jnp.transpose(chosen_t)[:, :experts]
    before = (iota((toks, toks), 0) > iota((toks, toks), 1)).astype(F32).astype(BF16)
    x = x_ref[...].astype(F32)
    x_inv = inv_rms(x)
    a = (x * x_inv).astype(BF16)

    for copy in own_w:
        copy.wait()
    pl.semaphore_wait(sem, len(peers))
    quarter = toks // 4
    two = ((0, 0, 2), (1, 2, 2))
    w_steps = gather_steps(place, sems, lambda d, lo, num: w_full.at[pl.ds(lo, num), rows_of(d)],
                           lambda n: w_full.at[:, pl.ds(0, n * depth)], False, two)
    ids_steps = gather_steps(place, sems, lambda d, lo, num: ids_all.at[d], lambda n: ids_all.at[pl.ds(0, n)], False, ((0, 0, 1),), True)
    dy_steps = gather_steps(place, sems, lambda d, lo, num: dy_all.at[d, pl.ds(lo * quarter, num * quarter)],
                            lambda n: dy_all.at[pl.ds(0, n)], True, two)
    next(w_steps)
    next(ids_steps)
    next(dy_steps)
    for _ in range(3):
        next(w_steps)
        next(ids_steps)
    next(dy_steps)
    next(dy_steps)
    finish(w_steps)
    next(ids_steps)

    q_s[...] = mm(a, w_full[0]).astype(BF16)
    k_s[...] = mm(a, w_full[1]).astype(BF16)
    v_s[...] = mm(a, w_full[2]).astype(BF16)
    next(dy_steps, None)
    causal = iota((toks, toks), 0) >= iota((toks, toks), 1)
    low = iota((toks, 2 * HEAD_DIM), 1) < HEAD_DIM
    zero_b = jnp.zeros((toks, 2 * HEAD_DIM), BF16)
    pairs = d_model // (2 * HEAD_DIM)
    scale = HEAD_DIM ** -0.5

    def half(v, side):
        return jnp.where(low, v, zero_b) if side == 0 else jnp.where(low, zero_b, v)

    for pair in range(pairs):
        lanes = pl.ds(pair * 2 * HEAD_DIM, 2 * HEAD_DIM)
        qp, kp, vp = q_s[:, lanes], k_s[:, lanes], v_s[:, lanes]
        outs = []
        for hf in range(2):
            s = jnp.where(causal, mm(half(qp, hf), kp, NT) * scale, -1e30)
            e = jnp.exp(s - jnp.max(s, axis=-1, keepdims=True))
            p = e / jnp.sum(e, axis=-1, keepdims=True)
            prob_s[2 * pair + hf] = jnp.transpose(p)
            outs.append(mm(p.astype(BF16), vp))
        o_s[:, lanes] = jnp.where(low, outs[0], outs[1]).astype(BF16)
        if pair >= 3:
            next(dy_steps, None)

    hid = (x + mm(o_s[...], w_full[3])).astype(BF16)
    hid_s[...] = hid
    h = hid.astype(F32)
    h_inv = inv_rms(h)
    n = h * h_inv
    u_all[me] = n.astype(BF16)
    logits = mm(n, wr_ref[...], NT, EXACT)
    top = jnp.max(jnp.where(chosen > 0.0, logits, -3e38), axis=-1, keepdims=True)
    expd = jnp.where(chosen > 0.0, jnp.exp(logits - top), 0.0)
    gates = expd / jnp.sum(expd, axis=-1, keepdims=True)
    gates_t = jnp.transpose(jnp.concatenate([gates, jnp.zeros_like(gates)], axis=-1))
    for j in range(choices):
        g_all[me, j:j + 1, :] = jnp.sum(jnp.where(idst[j:j + 1, :] == lane_e, gates_t, 0.0), axis=0, keepdims=True)

    u_steps = gather_steps(place, sems, lambda d, lo, num: u_all.at[d, pl.ds(lo * quarter, num * quarter)],
                           lambda n: u_all.at[pl.ds(0, n)], True, two)
    g_steps = gather_steps(place, sems, lambda d, lo, num: g_all.at[d], lambda n: g_all.at[pl.ds(0, n)], False, ((0, 0, 1),), True)
    next(g_steps)
    next(u_steps)
    finish(ids_steps)

    first_e = (me * local).astype(F32)
    row8 = iota((8, toks), 0)

    def find(i, _):
        ids = ids_all[place.at(*block_offset(i, place))]
        m = jnp.zeros((8, toks), F32)
        for e in range(local):
            hit = jnp.sum(jnp.where(ids == first_e + e, 1.0, 0.0), axis=0, keepdims=True)
            m = jnp.where(row8 == e, hit, m)
        m_s[i] = m
        return 0

    lax.fori_loop(0, group, find, 0)
    next(u_steps)
    for _ in range(3):
        next(g_steps)
    next(dy_steps, None)
    next(dy_steps, None)
    m_flat = m_s[...].reshape(group * 8, toks)
    after = (iota((toks, toks), 0) < iota((toks, toks), 1)).astype(F32).astype(BF16)
    r_flat = jnp.where(m_flat > 0.0, mm(m_flat.astype(BF16), after), -1.0)
    m_s[...] = r_flat.reshape(group, 8, toks)
    next(u_steps)
    next(dy_steps, None)
    slot = iota((cap, toks), 0).astype(F32)

    def build(i, _):
        r = m_s[i]
        for e in range(local):
            pick_s[i, pl.ds(e * cap, cap), :] = jnp.where(slot == r[e:e + 1, :], 1.0, 0.0).astype(BF16)
        return 0

    lax.fori_loop(0, group, build, 0)

    def take_rows(i, source, dest):
        rows = mm(pick_s[i], source[place.at(*block_offset(i, place))]).astype(BF16)
        for e in range(local):
            at = i * cap
            dest[e, pl.ds(pl.multiple_of(at, cap), cap), :] = rows[e * cap:(e + 1) * cap]

    def take_dy(g, _):
        for b in range(per):
            take_rows(g * per + b, dy_all, rdy_s)
        return 0

    for _ in range(9):
        next(u_steps)
        next(dy_steps, None)
        next(dy_steps, None)
    for copy in experts_in:
        copy.wait()

    span = per * cap
    side = place.side
    both = local * cap
    k_first, k_second, k_small = sems.new_recv(4), sems.new_recv(2), sems.new_recv()
    k_rows, k_sums, k_smalls = [sems.new_send() for _ in range(2)], [sems.new_send() for _ in range(2)], sems.new_send()

    def first_hop(part, d1, dc, p):
        core = lax.rem(place.core + dc, 2)
        relay_dc = (dc + p) % 2
        src = u_all.at[pl.ds(d1 * per + dc * side + 2 * p, 2), pl.ds(part * both, both)]
        return sems.copy(src, relay.at[part, p, :, 2 * d1 + relay_dc], k_rows[part], k_first + 2 * part + p,
                         place.at(*turn(place, core, d1, 0), relay_dc))

    def first_done(part, p):
        at = relay.at[part, p, :, pl.ds(1, per - 1)]
        return sems.copy(at, at, k_rows[part], k_first + 2 * part + p, me)

    def dest_of(p, j):
        core = lax.rem(place.core + p, 2)
        return place.at(*turn(place, core, 0, p + 2 * j), p)

    def second_hop(part, p, j):
        return sems.copy(sums.at[part, 2 * j + p - 1], total.at[part, 2 * j + p], k_sums[part], k_second + part, dest_of(p, j))

    def small_hop(p, j):
        return sems.copy(small.at[2 * j + p - 1], smalls.at[2 * j + p], k_smalls, k_small, dest_of(p, j))

    def put(part, e, g, rows):
        for b in range(per):
            u_all[g * per + b, pl.ds(part * both + e * cap, cap), :] = rows[b * cap:(b + 1) * cap]

    def start_group(part, g):
        @pl.when(g > 0)
        def _():
            for dc in range(2):
                for p in range(2):
                    first_hop(part, g, dc, p).start()

        @pl.when(g == 0)
        def _():
            for p in range(2):
                first_hop(part, 0, 1 - p, p).start()
                for j in range(2):
                    relay[part, p, j, 0] = u_all[p * side + 2 * p + j, pl.ds(part * both, both), :]

    def take_u(dc):
        def body(g, _):
            for b in range(2):
                for d2 in range(side):
                    take_rows((2 * g + b) * per + dc * side + d2, u_all, ru_s)
            return 0
        lax.fori_loop(0, side // 2, body, 0)

    take_u(0)
    next(u_steps)
    next(dy_steps, None)
    take_u(1)
    finish(u_steps)

    def forward(step, _):
        g = lax.rem(step + side // 2, side)
        rows = pl.ds(pl.multiple_of(g * span, span), span)
        for e in range(local):
            ru = ru_s[e, rows, :]
            ag = mm(ru, wg_ref[e])
            au = mm(ru, wu_ref[e])
            mid = (ag * jax.nn.sigmoid(ag) * au).astype(BF16)
            ag_s[e, rows, :] = ag
            au_s[e, rows, :] = au
            mid_s[e, rows, :] = mid
            put(0, e, g, mm(mid, wd_ref[e]).astype(BF16))
        start_group(0, g)
        return 0

    lax.fori_loop(0, groups, forward, 0)

    def weigh(q, _):
        for i in [q * side + b for b in range(side)]:
            d = place.at(*block_offset(i, place))
            ids, gts = ids_all[d], g_all[d]
            for e in range(local):
                gate = jnp.sum(jnp.where(ids == first_e + e, gts, 0.0), axis=0, keepdims=True)
                col = jnp.sum(pick_s[i, pl.ds(e * cap, cap), :].astype(F32) * gate, axis=-1, keepdims=True)
                at = pl.ds(pl.multiple_of(i * cap, cap), cap)
                rdy_s[e, at, :] = (col * rdy_s[e, at, :].astype(F32)).astype(BF16)
        return 0

    finish(g_steps, dy_steps)
    lax.fori_loop(0, groups, take_dy, 0)
    lax.fori_loop(0, group // side, weigh, 0)

    def backward(step, _):
        g = lax.rem(step + side // 2, side)
        rows = pl.ds(pl.multiple_of(g * span, span), span)
        for e in range(local):
            gm = mm(rdy_s[e, rows, :], wd_ref[e], NT)
            ag, au = ag_s[e, rows, :], au_s[e, rows, :]
            sg = jax.nn.sigmoid(ag)
            dag = (gm * au * sg * (1.0 + ag * (1.0 - sg))).astype(BF16)
            dau = (gm * ag * sg).astype(BF16)
            dag_s[e, rows, :] = dag
            dau_s[e, rows, :] = dau
            put(1, e, g, (mm(dag, wg_ref[e], NT) + mm(dau, wu_ref[e], NT)).astype(BF16))
        start_group(1, g)
        return 0

    lax.fori_loop(0, groups, backward, 0)

    def weights(e, _):
        gd_s[e] = mm(mid_s[e], rdy_s[e], TN).astype(BF16)
        mid_s[e, pl.ds(0, d_model), :] = mm(ru_s[e], dag_s[e], TN).astype(BF16)
        dag_s[e, pl.ds(0, d_model), :] = mm(ru_s[e], dau_s[e], TN).astype(BF16)
        return 0

    lax.fori_loop(0, local, weights, 0)
    grads_out = [pltpu.make_async_copy(src, dst, lsem.at[i])
                 for i, (src, dst) in enumerate(((mid_s.at[:, pl.ds(0, d_model)], gg_ref), (dag_s.at[:, pl.ds(0, d_model)], gu_ref), (gd_s, gd_ref), (o_s, y_ref)))]
    for copy in grads_out[:3]:
        copy.start()

    wide = per * both
    blocks = wide // cap
    col = iota((1, wide), 1)
    colmod = col
    for _ in range(1, blocks):
        colmod = jnp.where(colmod >= cap, colmod - cap, colmod)
    colmod = colmod.astype(F32)
    e_row = iota((experts, wide), 0).astype(F32)
    blk = iota((blocks, wide), 0) * cap
    blk_col = iota((blocks, wide), 1)
    block_of = jnp.where((blk_col >= blk) & (blk_col < blk + cap), 1.0, 0.0).astype(BF16)

    def owner_at(core, p, d1, dc, d2, e):
        dy, dx = turn(place, core, -d1, -d2)
        return (place.at(dy, dx, p + dc) * local + e).astype(F32)

    def relay_z(q, _):
        p, j = q % 2, q // 2
        core = lax.rem(place.core + p, 2)
        dest = dest_of(p, j)
        owner = jnp.zeros((1, wide), F32)
        for b in range(blocks):
            s, e = b // local, b % local
            owner = jnp.where((col >= b * cap) & (col < (b + 1) * cap), owner_at(core, 0, s // 2, s % 2, 0, e), owner)
        spread = jnp.where(e_row == owner, 1.0, 0.0).astype(BF16)
        ids, gts = ids_all[dest], g_all[dest]
        e_in = iota((2 * experts, toks), 0)
        e_id = jnp.where(e_in >= experts, e_in - experts, e_in).astype(F32)
        both_t = jnp.zeros((2 * experts, toks), F32)
        for c in range(choices):
            both_t += jnp.where(ids[c:c + 1, :] == e_id, jnp.where(e_in >= experts, gts[c:c + 1, :], 1.0), 0.0)
        both_v = jnp.transpose(both_t)
        chose, weight = both_v[:, :experts], both_v[:, experts:]
        ranks = jnp.where(chose > 0.0, mm(before, chose.astype(BF16)), -1.0).astype(BF16)
        z = relay[0, p, j].reshape(wide, d_model)
        here = mm(ranks, spread) == colmod
        place_s[q] = jnp.where(here, 1.0, 0.0).astype(BF16)
        y_sum = jnp.zeros((toks, d_model), F32)
        for piece in three(weight):
            y_sum += mm(jnp.where(here, mm(piece, spread), 0.0).astype(BF16), z)
        gg_sum = jnp.zeros((blocks, toks), F32)
        for piece in three(jnp.where(here, mm(dy_all[dest], z, NT), 0.0)):
            gg_sum += mm(block_of, piece, NT)

        @pl.when(q == 0)
        def _():
            total[0, 0] = y_sum
            smalls[0] = gg_sum

        @pl.when(q > 0)
        def _():
            sums[0, q - 1] = y_sum
            small[q - 1] = gg_sum
            second_hop(0, p, j).start()
            small_hop(p, j).start()
        return 0

    for p in range(2):
        first_done(0, p).wait_recv()
    lax.fori_loop(0, side, lambda t, _: relay_z(lax.rem(t + 2, side), 0), 0)
    for p in range(2):
        first_done(1, p).wait_recv()

    def relay_d(q, _):
        p, j = q % 2, q // 2
        sums_d = mm(place_s[q], relay[1, p, j].reshape(wide, d_model))

        @pl.when(q == 0)
        def _():
            total[1, 0] = sums_d

        @pl.when(q > 0)
        def _():
            sums[1, q - 1] = sums_d
            second_hop(1, p, j).start()
        return 0

    lax.fori_loop(0, side, lambda t, _: relay_d(lax.rem(t + 2, side), 0), 0)

    rest = pl.ds(1, side - 1)
    sems.copy(total.at[0, rest], total.at[0, rest], k_sums[0], k_second, me).wait_recv()
    sems.copy(smalls.at[rest], smalls.at[rest], k_smalls, k_small, me).wait_recv()
    dyv = dy_ref[...]
    o_s[...] = (hid_s[...].astype(F32) + ((total[0, 0] + total[0, 1]) + (total[0, 2] + total[0, 3]))).astype(BF16)
    grads_out[3].start()
    m_col = iota((experts, 1), 0)
    owner = jnp.zeros((experts, 1), F32)
    for m in range(experts):
        d2, s, e = m // blocks, (m % blocks) // local, m % local
        owner = jnp.where(m_col == m, owner_at(place.core, d2 % 2, s // 2, s % 2, d2, e), owner)
    perm = jnp.where(owner == iota((experts, experts), 1).astype(F32), 1.0, 0.0).astype(BF16)
    g_gates = jnp.zeros((toks, experts), F32)
    for piece in three(smalls[...].reshape(experts, toks)):
        g_gates += mm(piece, perm, TN)
    g_logits = gates * (g_gates - jnp.sum(gates * g_gates, axis=-1, keepdims=True))
    g_hnorm = mm(g_logits, wr_ref[...], NN, EXACT)
    sems.copy(total.at[1, rest], total.at[1, rest], k_sums[1], k_second + 1, me).wait_recv()
    gn = g_hnorm + ((total[1, 0] + total[1, 1]) + (total[1, 2] + total[1, 3]))
    h = hid_s[...].astype(F32)
    h_inv = inv_rms(h)
    g_hid = (dyv.astype(F32) + rms_back(h, h_inv, gn)).astype(BF16)
    grads_out[3].wait()
    o_s[...] = mm(g_hid, w_full[3], NT).astype(BF16)
    g_xn = jnp.zeros((toks, d_model), F32)
    for pair in range(pairs):
        lanes = pl.ds(pair * 2 * HEAD_DIM, 2 * HEAD_DIM)
        qp, kp, vp, dop = q_s[:, lanes], k_s[:, lanes], v_s[:, lanes], o_s[:, lanes]
        dq, dk, dv = [], [], []
        for hf in range(2):
            p_t = prob_s[2 * pair + hf]
            dp_t = mm(vp, half(dop, hf), NT)
            ds_t = (p_t * (dp_t - jnp.sum(dp_t * p_t, axis=0, keepdims=True)) * scale).astype(BF16)
            dq.append(mm(ds_t, kp, TN))
            dk.append(mm(ds_t, qp))
            dv.append(mm(p_t.astype(BF16), dop))
        for i, parts in enumerate((dq, dk, dv)):
            grad = jnp.where(low, parts[0], parts[1]).astype(BF16)
            g_xn += mm(grad, w_full[i, :, lanes], NT)
    x = x_ref[...].astype(F32)
    hid_s[...] = (g_hid.astype(F32) + rms_back(x, inv_rms(x), g_xn)).astype(BF16)
    gx_out = pltpu.make_async_copy(hid_s, gx_ref, lsem.at[4])
    gx_out.start()

    for copy in grads_out[:3] + [gx_out]:
        copy.wait()
    for part in range(2):
        at = relay.at[part, :, :, pl.ds(1, per - 1)]
        sems.copy(at, at, k_rows[part], k_first, me).wait_send()
        sems.copy(sums.at[part], sums.at[part], k_sums[part], k_second, me).wait_send()
    sems.copy(small, small, k_smalls, k_small, me).wait_send()
    assert (sems.n_send, sems.n_recv) == (N_SEND, N_RECV)


def settle_kernel(*refs):
    n = (len(refs) - 2) // 3
    ins, outs, held, lsem, ssem = refs[:n], refs[n:2 * n], refs[2 * n:3 * n], refs[-2], refs[-1]
    loads = [pltpu.make_async_copy(a, h, lsem.at[i]) for i, (a, h) in enumerate(zip(ins, held))]
    stores = [pltpu.make_async_copy(h, o, ssem.at[i]) for i, (h, o) in enumerate(zip(held, outs))]
    for copy in loads:
        copy.start()
    for load, store in zip(loads, stores):
        load.wait()
        store.start()
    for copy in stores:
        copy.wait()


def settle(*arrays):
    n = len(arrays)
    hbm = pl.BlockSpec(memory_space=pl.ANY)
    return pl.pallas_call(
        settle_kernel, out_shape=[jax.ShapeDtypeStruct(a.shape, a.dtype) for a in arrays],
        in_specs=[hbm] * n, out_specs=[hbm] * n,
        scratch_shapes=[pltpu.VMEM(a.shape, a.dtype) for a in arrays] + [pltpu.SemaphoreType.DMA((n,))] * 2,
        name='settle')(*arrays)


def solution(mesh):
    group = mesh.shape[AXIS]
    tok_spec = P(('dp', 'ep'), None)
    fsdp_spec = P('ep', None)
    expert_spec = P('ep', None, None)
    grad_spec = P(('dp', 'ep'), None, None)

    def device_step(x_tokens, expert_ids, grad_y, w_q, w_k, w_v, w_o, w_router, w_gate, w_up, w_down):
        toks, d_model = x_tokens.shape
        choices = expert_ids.shape[1]
        experts = w_router.shape[1]
        local, _, ff = w_gate.shape
        avg_load = toks * choices // experts
        cap = avg_load + avg_load // 2
        assert toks == SEQ_LEN
        heads = w_q.shape[1] // HEAD_DIM
        shape, vm = jax.ShapeDtypeStruct, pltpu.VMEM
        rows = group * cap
        side = math.isqrt(group // 2)
        per = 2 * side
        assert local == 2
        in_vmem = pl.BlockSpec(memory_space=pltpu.VMEM)
        in_hbm = pl.BlockSpec(memory_space=pl.ANY)
        square = vm((toks, d_model), BF16)
        outs = pl.pallas_call(
            functools.partial(layer_kernel, group, experts, cap),
            out_shape=[shape(x_tokens.shape, BF16), shape(x_tokens.shape, BF16), shape(w_gate.shape, BF16),
                       shape(w_up.shape, BF16), shape(w_down.shape, BF16)],
            in_specs=[in_hbm] * 11,
            out_specs=[in_hbm] * 5,
            scratch_shapes=[
                vm((4, group * w_q.shape[0], d_model), BF16), vm((group, toks, d_model), BF16), vm((group, toks, d_model), BF16),
                vm((group, choices, toks), F32), vm((group, choices, toks), F32), vm((group, 8, toks), F32),
                vm((group, local * cap, toks), BF16), vm((local, rows, d_model), BF16), vm((local, rows, d_model), BF16),
                vm((local, rows, ff), F32), vm((local, rows, ff), F32),
                vm((local, rows, ff), BF16), vm((local, rows, ff), BF16), vm((local, rows, ff), BF16),
                square, vm((choices, toks), jnp.int32), square, vm((experts, d_model), F32),
                vm(w_gate.shape, BF16), vm(w_up.shape, BF16), vm(w_down.shape, BF16), vm((2, 2, 2, per, local * cap, d_model), BF16),
                vm((2, side - 1, toks, d_model), F32), vm((2, side, toks, d_model), F32),
                vm((side - 1, experts // side, toks), F32), vm((side, experts // side, toks), F32),
                vm((heads, toks, toks), F32), square, square, square, square, square,
                vm((group // per, toks, per * local * cap), BF16),
                vm(w_down.shape, BF16),
                pltpu.SemaphoreType.DMA((11,)), pltpu.SemaphoreType.DMA((N_SEND,)), pltpu.SemaphoreType.DMA((N_RECV,))],
            compiler_params=pltpu.CompilerParams(collective_id=1, has_side_effects=True, vmem_limit_bytes=67043328),
            name='layer')(x_tokens, expert_ids.T, grad_y, w_q, w_k, w_v, w_o, w_router.T, w_gate, w_up, w_down)
        return settle(*outs)

    return jax.shard_map(
        device_step, mesh=mesh,
        in_specs=(tok_spec, tok_spec, tok_spec, fsdp_spec, fsdp_spec, fsdp_spec, fsdp_spec,
                  P(None, None), expert_spec, expert_spec, expert_spec),
        out_specs=(tok_spec, tok_spec, grad_spec, grad_spec, grad_spec),
        check_vma=False)
```
